32 devices in a mesh: pb: 8 (over y, x, core), ga: 4 (over z).
Axes of the slice: x: 2, y: 2, z: 4, core: 2. Of those that a mesh axis runs over, the one named last changes fastest.
Arguments:
- query_points: float32 [3, 32768], P(None, 'pb'), may hold values from 0 to 1
- cotangent: bfloat16 [64, 32768], P(None, 'pb'), may hold values from -6 to 6
- slab_ids: int32 [8, 32768], P(None, 'pb'), may hold values from -1 to 3
- rel_cells: int32 [8, 32768], P(None, 'pb'), may hold values from 0 to 511
- offsets: int32 [4, 256], P('ga', 'pb'), may hold values from 0 to 15872
- latent: bfloat16 [4, 64, 16384], P('ga', None, 'pb'), may hold values from -6 to 6
- w_in: float32 [80, 6], replicated, may hold values from -2.5 to 2.5
- b_in: float32 [80], replicated, may hold values from -3 to 3
- w_out: bfloat16 [64, 80], replicated, may hold values from -0.625 to 0.625
- b_out: float32 [64], replicated, may hold values from -3 to 3
Outputs:
- grid_grad: float32 [4, 64, 16384], P('ga', None, 'pb')
- w_in_grad: float32 [80, 6], replicated
- b_in_grad: float32 [80], replicated
- w_out_grad: float32 [64, 80], replicated
- b_out_grad: float32 [64], replicated
The draws below stay inside these ranges and needn't reach their ends.
Inputs may be any that keep to these rules, and one draw needn't show every extreme that they name: `slab_ids`: -1 marks a padding slot; otherwise the slab that holds the neighbour cell.
All inputs are finite; a program needn't handle non-finite values.
Results may differ from the reference program's by a relative error of at most 0.0085.
Values may be sent and summed in bfloat16 or wider, within the bound.
A program may use at most 64 MiB of HBM per device.

```python
import math
import jax
import jax.numpy as jnp
from jax import lax

CH = 64
HID = 80
KN = 8
TILE = 128
WIN = 512
GX = 64
ZS = 4
SLAB_CELLS = 16384
QUERIES = 32768
TILES = 256
N_GA = 4


def with_ends(array, rng, low, high):
    extent = array.shape
    spot = [jax.random.randint(jax.random.fold_in(rng, axis), (), 0, extent[axis]) for axis in range(len(extent))]
    array = array.at[tuple(spot)].set(low)
    longest = extent.index(max(extent))
    spot[longest] = (spot[longest] + 1) % extent[longest]
    return array.at[tuple(spot)].set(high)


def block_levels(rng, extent, split, least, top_value):
    loudness = 1.0
    for dim, blocks in split:
        draws = jax.random.uniform(jax.random.fold_in(jax.random.fold_in(rng, 6), dim), (blocks,), jnp.float32, least / len(split), top_value / len(split))
        loudness = loudness * jnp.repeat(jnp.exp(draws), extent[dim] // blocks).reshape((-1,) + (1,) * (len(extent) - 1 - dim))
    return loudness


def gaussian(rng, shape, deviation, bound, cuts=(), kind=jnp.bfloat16):
    drawn = jax.random.normal(rng, shape, jnp.float32) * deviation
    if len(cuts) > 0:
        drawn = block_levels(rng, shape, cuts, -0.22, 0.18) * drawn
    return jnp.clip(drawn, min=-bound, max=bound).astype(kind)


def setup_inputs(seed: int = 0) -> dict:
    key_list = jax.random.split(jax.random.key(seed), 11)
    return {
        "query_points": jnp.clip(1.0 * jax.random.uniform(key_list[0], (3, QUERIES), jnp.float32) ** block_levels(key_list[0], (3, QUERIES), ((1, 8),), -0.2, 0.2), 0.0, 1.0),
        "cotangent": gaussian(key_list[1], (CH, QUERIES), 1.0, 6.0, ((1, 8),)),
        "slab_ids": with_ends(jax.random.randint(key_list[2], (KN, QUERIES), -1, N_GA), jax.random.fold_in(key_list[2], 1), -1, N_GA - 1).astype(jnp.int32),
        "rel_cells": with_ends(jax.random.randint(key_list[3], (KN, QUERIES), 0, WIN), jax.random.fold_in(key_list[3], 1), 0, WIN - 1).astype(jnp.int32),
        "offsets": with_ends(jax.random.randint(key_list[4], (N_GA, TILES), 0, SLAB_CELLS - WIN + 1), jax.random.fold_in(key_list[4], 1), 0, SLAB_CELLS - WIN).astype(jnp.int32),
        "latent": gaussian(key_list[5], (N_GA, CH, SLAB_CELLS), 1.0, 6.0, ((0, 4), (2, 8))),
        "w_in": gaussian(key_list[6], (HID, 6), 6 ** -0.5, 2.5, (), jnp.float32),
        "b_in": gaussian(key_list[7], (HID,), 0.5, 3.0, (), jnp.float32),
        "w_out": gaussian(key_list[8], (CH, HID), HID ** -0.5, 0.625),
        "b_out": gaussian(key_list[9], (CH,), 0.5, 3.0, (), jnp.float32),
    }


def gelu_exact(values):
    return jax.nn.gelu(values, approximate=False)

def cell_centres(cell, slab):
    along_x = cell // (GX * ZS)
    along_y = cell // ZS % GX
    along_z = cell % ZS + slab * ZS
    return jnp.stack([(along_x.astype(jnp.float32) + 0.5) / GX, (along_y.astype(jnp.float32) + 0.5) / GX, (along_z.astype(jnp.float32) + 0.5) / GX], 0)

def reference(query_points, cotangent, slab_ids, rel_cells, offsets, latent, w_in, b_in, w_out, b_out):
    cells_slab = GX * GX * ZS
    latent_flat = jnp.transpose(latent, (1, 0, 2)).reshape(CH, N_GA * cells_slab)
    per_block = TILE * math.gcd(TILES, 64)
    count = QUERIES // per_block

    def reshape_blocks(values):
        return values.reshape(values.shape[0], count, per_block).transpose(1, 0, 2)

    def advance(running, inputs_block):
        grid_sum, totals = running
        number, points, cot_cols, slabs, rels = inputs_block
        tile_ids = (number * per_block + jnp.arange(per_block, dtype=jnp.int32)) // TILE
        slab_safe = jnp.maximum(slabs, 0)
        cell = offsets[slab_safe, tile_ids[None, :]] + rels
        flat_index = (slab_safe * cells_slab + cell).reshape(-1).astype(jnp.int32)
        mask_flat = (slabs >= 0).reshape(-1).astype(jnp.float32)
        centres = cell_centres(cell.reshape(-1), slab_safe.reshape(-1))
        features_in = jnp.concatenate([jnp.tile(points, (1, KN)), centres], 0)
        cot_flat = jnp.tile(cot_cols.astype(jnp.float32), (1, KN))
        feats = jnp.take(latent_flat, flat_index, axis=1).astype(jnp.float32)
        preact = jnp.dot(w_in, features_in, precision=lax.Precision.HIGHEST, preferred_element_type=jnp.float32) + b_in[:, None]
        hidden = gelu_exact(preact).astype(jnp.bfloat16)
        kernel = jnp.dot(w_out, hidden, preferred_element_type=jnp.float32) + b_out[:, None]
        grad_cell = (kernel * cot_flat * mask_flat).astype(jnp.bfloat16)
        grad_kernel = (feats * cot_flat * mask_flat).astype(jnp.bfloat16)
        grid_sum = grid_sum.at[:, flat_index].add(grad_cell.astype(jnp.float32))
        grad_w_out = lax.dot_general(grad_kernel, hidden, (((1,), (1,)), ((), ())), preferred_element_type=jnp.float32)
        grad_b_out = lax.optimization_barrier(jnp.sum(grad_kernel.astype(jnp.float32), 1))
        grad_hidden = lax.dot_general(w_out, grad_kernel, (((0,), (0,)), ((), ())), preferred_element_type=jnp.float32)
        grad_pre = jax.vjp(gelu_exact, preact)[1](grad_hidden)[0]
        grad_w_in = lax.dot_general(grad_pre, features_in, (((1,), (1,)), ((), ())), precision=lax.Precision.HIGHEST, preferred_element_type=jnp.float32)
        grad_b_in = lax.optimization_barrier(jnp.sum(grad_pre, 1))
        parts = (grad_w_in, grad_b_in, grad_w_out, grad_b_out)
        totals = tuple((old + new for old, new in zip(totals, parts)))
        return ((grid_sum, totals), None)
    start_totals = (jnp.zeros((HID, 6), jnp.float32), jnp.zeros((HID,), jnp.float32), jnp.zeros((CH, HID), jnp.float32), jnp.zeros((CH,), jnp.float32))
    start_grid = jnp.zeros((CH, N_GA * cells_slab), jnp.float32)
    inputs_all = (jnp.arange(count, dtype=jnp.int32), reshape_blocks(query_points), reshape_blocks(cotangent), reshape_blocks(slab_ids), reshape_blocks(rel_cells))
    (grid_sum, totals), _ = lax.scan(advance, (start_grid, start_totals), inputs_all)
    scale = float(QUERIES) ** (-0.5)
    grid_grad = grid_sum.reshape(CH, N_GA, cells_slab).transpose(1, 0, 2)
    return (grid_grad, totals[0] * scale, totals[1] * scale, totals[2] * scale, totals[3] * scale)
```

```python
import functools
import math

import jax
import jax.numpy as jnp
from jax import lax
from jax.experimental import pallas as pl
from jax.experimental.pallas import tpu as pltpu
from jax.sharding import PartitionSpec as P

KN = 8
TILE = 128
WIN = 512
GX = 64
ZS = 4
LANES = 128
SPAN = WIN // LANES + 1
CAP = 256
XR = 48
F32 = jnp.float32
BF16 = jnp.bfloat16
I32 = jnp.int32
MESH = pl.DeviceIdType.MESH
HIGHEST = lax.Precision.HIGHEST


def dot(a, b):
    return jnp.dot(a, b, preferred_element_type=F32)


def dot_nt(a, b):
    return lax.dot_general(a, b, (((1,), (1,)), ((), ())), preferred_element_type=F32)


def exact(a, b):
    return jnp.dot(a, b, preferred_element_type=F32, precision=HIGHEST)


def exact_nt(a, b):
    return lax.dot_general(a, b, (((1,), (1,)), ((), ())), preferred_element_type=F32, precision=HIGHEST)


def rows_of(shape):
    return lax.broadcasted_iota(I32, shape, 0)


def cols_of(shape):
    return lax.broadcasted_iota(I32, shape, 1)


def gelu_parts(x):
    z = jnp.abs(x) * (2.0**-0.5)
    t = 1.0 / (1.0 + 0.3275911 * z)
    e = jnp.exp(-0.5 * x * x)
    poly = ((((1.061405429 * t - 1.453152027) * t + 1.421413741) * t - 0.284496736) * t + 0.254829592) * t
    tail = 0.5 * poly * e
    cdf = jnp.where(x < 0, tail, 1.0 - tail)
    return x * cdf, cdf + x * e * ((2.0 * math.pi) ** -0.5)


def mask_of(cond):
    return jnp.where(cond, 1.0, 0.0).astype(BF16)


def split3(v):
    a = v.astype(BF16)
    r = v - a.astype(F32)
    b = r.astype(BF16)
    return a, b, (r - b.astype(F32)).astype(BF16)


def weights(win_ref, bin_ref, wout_ref, bout_ref, pad_ref, w1_ref, w2_ref, w2t_ref):
    hid, channels = win_ref.shape[0], wout_ref.shape[0]
    pad_ref[...] = jnp.zeros_like(pad_ref)
    pad_ref[:hid, : win_ref.shape[1]] = win_ref[...]
    wide = pad_ref[:hid, :]
    w_hi = wide.astype(BF16)
    w_lo = (wide - w_hi.astype(F32)).astype(BF16)
    k, col = rows_of((LANES, LANES)), cols_of((LANES, LANES))
    s_hi = mask_of(((k < 3) & ((col == k) | (col == k + 8))) | ((k >= 3) & (k < 6) & (col == k + 13)))
    s_lo = mask_of(((k < 3) & (col == k + 24)) | ((k >= 3) & (k < 6) & (col == k + 29)))
    w1 = dot(w_hi, s_hi) + dot(w_lo, s_lo)
    pad_ref[0:1, :hid] = bin_ref[...]
    diag = jnp.where(rows_of((hid, LANES)) == cols_of((hid, LANES)), pad_ref[0:1, :], 0.0)
    for i, part in enumerate(split3(diag)):
        w1 += dot(part, mask_of(col == 3 + i))
    w1_ref[...] = w1.astype(BF16)

    pad_ref[0:channels, :hid] = wout_ref[...].astype(F32)
    pad_ref[0:channels, hid:] = jnp.zeros((channels, LANES - hid), F32)
    w_out = pad_ref[0:channels, :].astype(BF16)
    w2 = dot(w_out, mask_of(k == col))
    eye = mask_of(rows_of((hid, LANES)) == cols_of((hid, LANES)))
    w2t_ref[...] = dot_nt(eye, w_out).astype(BF16)
    pad_ref[0:1, :channels] = bout_ref[...]
    diag = jnp.where(rows_of((channels, LANES)) == cols_of((channels, LANES)), pad_ref[0:1, :], 0.0)
    for i, part in enumerate(split3(diag)):
        w2 += dot(part, mask_of(col == hid + 3 + i))
    w2_ref[...] = w2.astype(BF16)


def order_parts(tiles, limit, offv_ref, table_ref):
    pairs = SPAN * tiles
    lanes = -(-pairs // LANES) * LANES
    base_row = jnp.minimum(lax.shift_right_logical(offv_ref[...], 7), limit)
    wide = jnp.concatenate([base_row, jnp.zeros((1, LANES - tiles), I32)], 1)
    pick = rows_of((tiles, LANES)) == cols_of((tiles, LANES))
    column = jnp.sum(jnp.where(pick, wide.astype(F32), 0.0), 1, keepdims=True)
    key = jnp.concatenate([column + float(j) for j in range(SPAN)], 0)
    key = jnp.broadcast_to(key, (pairs, lanes))
    p, q = rows_of((pairs, lanes)), cols_of((pairs, lanes))
    key_row = jnp.sum(jnp.where(p == q, key, 0.0), 0, keepdims=True)
    key_row = jnp.where(q[:1] < pairs, key_row, 1.0e6)
    ahead = (key_row == key) & (q < p)
    rank = jnp.sum(jnp.where((key_row < key) | ahead, 1.0, 0.0), 1, keepdims=True)
    again = jnp.sum(jnp.where(ahead, 1.0, 0.0), 1, keepdims=True)
    here = rank == q.astype(F32)
    order = jnp.sum(jnp.where(here, p.astype(F32), 0.0), 0, keepdims=True)
    keep = jnp.sum(jnp.where(here & (again > 0), 1.0, 0.0), 0, keepdims=True)
    upto = jnp.sum(jnp.where(key <= q.astype(F32), 1.0, 0.0), 0, keepdims=True)
    some = jnp.sum(jnp.where(key == q.astype(F32), 1.0, 0.0), 0, keepdims=True)
    some = jnp.minimum(some, 1.0)
    last = jnp.maximum(upto - 1.0, 0.0)
    rows = jnp.concatenate([order, keep, last, some, jnp.zeros((4, lanes), F32)], 0)
    table_ref[...] = rows.astype(I32)


def kernel(
    n_pb, n_ga, scale,
    step_ref, offs_ref, offv_ref, qp_ref, cot_ref, ids_ref, rel_ref, latent_ref, win_ref, bin_ref, wout_ref, bout_ref,
    grid_ref, gwin_ref, gbin_ref, gwout_ref, gbout_ref, more_ref,
    pts_ref, pos_ref, from_ref, upto_ref, pad_ref, w1_ref, w2_ref, w2t_ref, tablev_ref, table_ref,
    cots_ref, hid_ref, slope_ref, x_ref, spot_ref, parts_ref, sums_ref, feats_ref,
    near_ref, nearin_ref, far_ref, farin_ref, own_ref, acc_ref,
    ar_ref, arin_ref, gaall_ref, fin_ref,
    table_sem, gsend, grecv, fsend, nsend, nrecv, rsend, rrecv, asend, arecv, bsend, brecv, csend, crecv,
):
    me, slab = lax.axis_index("pb"), lax.axis_index("ga")
    chips = n_pb // 2
    chip, core = me // 2, me % 2
    sibling = chip * 2 + 1 - core
    tiles = cot_ref.shape[1] // TILE
    channels, hid = cot_ref.shape[0], win_ref.shape[0]
    blocks = latent_ref.shape[2] // LANES
    limit = blocks * n_pb - SPAN
    group = math.gcd(tiles, 4)

    def send(src, dst, ssem, rsem, where):
        return pltpu.make_async_remote_copy(
            src_ref=src, dst_ref=dst, send_sem=ssem, recv_sem=rsem, device_id=where, device_id_type=MESH
        )

    def peer(m):
        return lax.rem(chip + m, chips) * 2 + core

    def peer_back(m):
        return lax.rem(chip + chips - m, chips) * 2 + core

    barrier = pltpu.get_barrier_semaphore()
    for m in range(1, n_pb):
        pl.semaphore_signal(barrier, inc=1, device_id={"pb": lax.rem(me + m, n_pb)}, device_id_type=MESH)
    for m in range(1, n_ga):
        pl.semaphore_signal(barrier, inc=1, device_id={"ga": lax.rem(slab + m, n_ga)}, device_id_type=MESH)

    mine = me * blocks
    for b in range(blocks):
        feats_ref[mine + b] = latent_ref[0, :, b * LANES : (b + 1) * LANES]
    pts_ref[...] = jnp.ones_like(pts_ref)
    pts_ref[0:3, :] = qp_ref[...]
    order_parts(tiles, limit, offv_ref, tablev_ref)
    weights(win_ref, bin_ref, wout_ref, bout_ref, pad_ref, w1_ref, w2_ref, w2t_ref)

    pl.semaphore_wait(barrier, n_pb - 1 + n_ga - 1)

    def feats_of(d):
        return feats_ref.at[pl.ds(d * blocks, blocks)]

    out = []
    for m in range(1, chips):
        out.append(send(feats_of(me), feats_of(me), gsend.at[m], grecv.at[me], {"pb": peer(m)}))
    out.append(send(feats_of(me), feats_of(me), gsend.at[0], grecv.at[me], {"pb": sibling}))
    for copy in out:
        copy.start()
    table_copy = pltpu.make_async_copy(tablev_ref, table_ref, table_sem)
    table_copy.start()

    lives = [jnp.where(ids_ref[:, t * TILE : (t + 1) * TILE] == slab, 1.0, 0.0) for t in range(tiles)]
    live = jnp.concatenate(lives, 0)
    rows = tiles * KN
    packed = live.astype(BF16)
    before = dot(packed, mask_of(rows_of((TILE, TILE)) < cols_of((TILE, TILE))))
    total = dot(packed, jnp.ones((TILE, TILE), BF16))
    r, c = rows_of((rows, rows)), cols_of((rows, rows))
    start = dot(mask_of((r // KN == c // KN) & (c < r)), total.astype(BF16))
    skip = (step_ref[0] * CAP).astype(F32)
    pos_ref[...] = jnp.where(live > 0, before + start - skip, -1.0e6)
    from_ref[...] = start - skip
    upto_ref[...] = start + total - skip
    left = jnp.max(start + total - skip - float(CAP), axis=0, keepdims=True)
    left = jnp.max(left, axis=1, keepdims=True)

    def tile_base(t):
        return jnp.minimum(lax.shift_right_logical(offs_ref[0, t], 7), limit)

    def query_side(t):
        cols = pl.ds(pl.multiple_of(t * TILE, TILE), TILE)
        lines = pl.ds(pl.multiple_of(t * KN, KN), KN)
        base = tile_base(t)
        pos = pos_ref[lines, :].astype(BF16)
        place = rows_of((CAP, TILE)).astype(F32).astype(BF16)
        pick = jnp.zeros((CAP, TILE), BF16)
        one = jnp.ones((CAP, TILE), BF16)
        for k in range(KN):
            pick = jnp.where(pos[k : k + 1, :] == place, one, pick)
        relp = rel_ref[:, cols] + (offs_ref[0, t] - base * LANES)
        low = (relp & (LANES - 1)).astype(F32)
        high = lax.shift_right_logical(relp, 7).astype(F32)
        points = pts_ref[:, cols]
        p_hi = points.astype(BF16).astype(F32)
        small = jnp.concatenate([p_hi, points - p_hi, low, high], 0).astype(BF16)
        data = jnp.concatenate([cot_ref[:, cols], small], 0)
        drawn = dot_nt(data, pick)
        cot = drawn[:channels]
        head = drawn[channels : channels + 16]
        wide_from = jnp.concatenate([from_ref[lines, :]] * (CAP // TILE), 1)
        wide_upto = jnp.concatenate([upto_ref[lines, :]] * (CAP // TILE), 1)
        index = cols_of((KN, CAP)).astype(F32)
        which = (index >= wide_from) & (index < wide_upto)
        lo = jnp.sum(jnp.where(which, drawn[channels + 16 : channels + 24], 0.0), 0, keepdims=True)
        hi = jnp.sum(jnp.where(which, drawn[channels + 24 : channels + 32], 0.0), 0, keepdims=True)
        lo = jnp.broadcast_to(lo, (8, CAP))
        hi = jnp.broadcast_to(hi, (8, CAP))
        cell = (base + hi.astype(I32)) * LANES + lo.astype(I32)
        row = rows_of((8, CAP))
        along = jnp.where(
            row == 0,
            lax.shift_right_logical(cell, int(math.log2(GX * ZS))),
            jnp.where(
                row == 1,
                lax.shift_right_logical(cell, int(math.log2(ZS))) & (GX - 1),
                (cell & (ZS - 1)) + slab * ZS,
            ),
        )
        centre = jnp.where(row < 3, (along.astype(F32) + 0.5) / GX, 0.0)
        x = jnp.concatenate([head, centre, head[:8], centre, jnp.zeros((8, CAP), F32)], 0).astype(BF16)
        hidden, slope = gelu_parts(dot(w1_ref[:, :XR], x))
        hidden = hidden.astype(BF16)
        kern = dot(w2_ref[...], jnp.concatenate([hidden, x], 0))
        grad = (kern * cot).astype(BF16)
        part = dot_nt(spread(hi, grad), lane_onehot(lo))
        return cot.astype(BF16), hidden, slope, x, jnp.where(row < 4, lo, hi), part

    def lane_onehot(lo):
        row = jnp.broadcast_to(lo[:1], (LANES, CAP)).astype(BF16)
        return jnp.where(
            rows_of((LANES, CAP)).astype(F32).astype(BF16) == row, jnp.ones((LANES, CAP), BF16), jnp.zeros((LANES, CAP), BF16)
        )

    def spread(hi, grad):
        full = jnp.concatenate([hi, hi], 0)
        pieces = []
        for j in range(SPAN):
            on = jnp.where(full == float(j), 1.0, 0.0).astype(BF16)
            pieces.append(grad * jnp.concatenate([on] * (channels // 16), 0))
        return jnp.concatenate(pieces, 0)

    def first(i, carry):
        done = [(i * group + u, query_side(i * group + u)) for u in range(group)]
        for t, (cot, hidden, slope, x, spot, part) in done:
            cots_ref[t] = cot
            hid_ref[t] = hidden
            slope_ref[t] = slope
            x_ref[t] = x
            spot_ref[t] = spot
            for j in range(SPAN):
                parts_ref[j * tiles + t] = part[j * channels : (j + 1) * channels]
        return carry

    lax.fori_loop(0, tiles // group, first, 0)

    table_copy.wait()

    def pair_at(line, b):
        return jnp.clip(table_ref[line, b], 0, SPAN * tiles - 1)

    def run(i, acc):
        for u in range(group):
            at = i * group + u
            acc = acc * table_ref[1, at].astype(F32) + parts_ref[pair_at(0, at)]
            sums_ref[at] = acc
        return acc

    lax.fori_loop(0, SPAN * tiles // group, run, jnp.zeros((channels, LANES), F32))

    def block(b):
        return sums_ref[pair_at(2, b)] * table_ref[3, b].astype(F32)

    def near_copy(m):
        return send(near_ref.at[m], nearin_ref.at[m], nsend.at[m], nrecv.at[m], {"pb": sibling})

    pair = math.gcd(blocks, 4)
    order = [m % chips for m in range(1, chips + 1)]
    for i, m in enumerate(order):
        owner = lax.rem(chip + m, chips) * 2 + 1 - core

        def fill(b, carry, m=m, owner=owner):
            for u in range(pair):
                near_ref[m, b * pair + u] = block(owner * blocks + b * pair + u).astype(BF16)
            return carry

        lax.fori_loop(0, blocks // pair, fill, 0)
        if i > 0:
            near_copy(order[i - 1]).start()
    forwards = []
    for m in range(1, chips):
        d = peer_back(m)
        send(feats_of(d), feats_of(d), gsend.at[m], grecv.at[d], {"pb": d}).wait_recv()
        copy = send(feats_of(d), feats_of(d), fsend.at[m - 1], grecv.at[d], {"pb": sibling})
        copy.start()
        forwards.append(copy)
        if m == 1:
            near_copy(order[-1]).start()

    def far_copy(m):
        return send(far_ref.at[m - 1], farin_ref.at[m - 1], rsend.at[m - 1], rrecv.at[m - 1], {"pb": peer(m)})

    for i, m in enumerate(order):
        owner = lax.rem(chip + m, chips) * 2 + core
        near_copy(m).wait_recv()

        def join(b, carry, m=m, owner=owner):
            for u in range(pair):
                at = b * pair + u
                value = block(owner * blocks + at) + nearin_ref[m, at].astype(F32)
                if m:
                    far_ref[m - 1, at] = value.astype(BF16)
                else:
                    own_ref[at] = value
            return carry

        lax.fori_loop(0, blocks // pair, join, 0)
        if i > 0:
            far_copy(order[i - 1]).start()

    for m in range(chips):
        d = lax.rem(chip + m, chips) * 2 + 1 - core
        send(feats_of(d), feats_of(d), gsend.at[0], grecv.at[d], {"pb": sibling}).wait_recv()

    acc_ref[...] = jnp.zeros_like(acc_ref)

    def feature_side(t):
        spot = spot_ref[t]
        hi = jnp.broadcast_to(spot[4:5], (8, CAP))
        window = feats_ref[pl.ds(tile_base(t), SPAN)].reshape(SPAN * channels, LANES)
        drawn = dot(window, lane_onehot(spot))
        tall = jnp.concatenate([hi] * (channels // 8), 0)
        feats = drawn[:channels]
        for j in range(1, SPAN):
            feats = jnp.where(tall == float(j), drawn[j * channels : (j + 1) * channels], feats)
        grad_kernel = (feats * cots_ref[t].astype(F32)).astype(BF16)
        grad_pre = (dot(w2t_ref[...], grad_kernel) * slope_ref[t]).astype(BF16)
        return dot_nt(jnp.concatenate([grad_kernel, grad_pre], 0), jnp.concatenate([hid_ref[t], x_ref[t]], 0))

    def second(i, carry):
        acc_ref[...] += functools.reduce(lambda a, b: a + b, [feature_side(i * group + u) for u in range(group)])
        return carry

    lax.fori_loop(0, tiles // group, second, 0)

    k, l = rows_of((LANES, LANES)), cols_of((LANES, LANES))

    def gathered(shift):
        a = (l - shift >= 0) & (l - shift < 4) & ((k == hid + l - shift) | ((k == hid + 8 + l - shift) & (l - shift < 3)))
        b = (l - shift >= 4) & (l - shift < 7) & (k == hid + 16 + l - shift - 4)
        return jnp.where(a | b, 1.0, 0.0)

    top = jnp.where(cols_of((channels, LANES)) < 112, acc_ref[:channels], 0.0)
    tail = hid - channels
    top += exact(acc_ref[channels : 2 * channels], gathered(112))
    rest = exact(acc_ref[2 * channels : 2 * channels + tail], gathered(120))
    flag = jnp.where(left > 0, 1.0, 0.0)
    corner = (rows_of((tail, LANES)) == 0) & (cols_of((tail, LANES)) == 119)
    rest = jnp.where(corner, flag, rest)
    top = jnp.concatenate([top[:tail] + rest, top[tail:]], 0)
    slices = channels // n_pb
    ar_ref[...] = top.reshape(n_pb, slices, LANES)
    arin_ref[pl.ds(me, 1)] = ar_ref[pl.ds(me, 1)]
    first_hop = []
    for m in range(1, n_pb):
        to = lax.rem(me + m, n_pb)
        copy = send(ar_ref.at[to], arin_ref.at[me], asend.at[m - 1], arecv.at[me], {"pb": to})
        copy.start()
        first_hop.append(copy)
    for m in range(1, n_pb):
        d = lax.rem(me + m, n_pb)
        send(ar_ref.at[d], arin_ref.at[d], asend.at[m - 1], arecv.at[d], {"pb": d}).wait_recv()
    gaall_ref[pl.ds(slab, 1)] = jnp.sum(arin_ref[...], 0, keepdims=True)
    second_hop = []
    for m in range(1, n_ga):
        to = lax.rem(slab + m, n_ga)
        copy = send(gaall_ref.at[slab], gaall_ref.at[slab], bsend.at[m - 1], brecv.at[slab], {"ga": to})
        copy.start()
        second_hop.append(copy)
    for m in range(1, n_ga):
        d = lax.rem(slab + m, n_ga)
        send(gaall_ref.at[d], gaall_ref.at[d], bsend.at[m - 1], brecv.at[d], {"ga": d}).wait_recv()
    fin_ref[pl.ds(me, 1)] = jnp.sum(gaall_ref[...], 0, keepdims=True)
    third_hop = []
    for m in range(1, n_pb):
        to = lax.rem(me + m, n_pb)
        copy = send(fin_ref.at[me], fin_ref.at[me], csend.at[m - 1], crecv.at[me], {"pb": to})
        copy.start()
        third_hop.append(copy)

    for m in range(1, chips):
        far_copy(m).wait_recv()
    for b in range(blocks):
        value = own_ref[b]
        for m in range(1, chips):
            value += farin_ref[m - 1, b].astype(F32)
        grid_ref[0, :, b * LANES : (b + 1) * LANES] = value

    for m in range(1, n_pb):
        d = lax.rem(me + m, n_pb)
        send(fin_ref.at[d], fin_ref.at[d], csend.at[m - 1], crecv.at[d], {"pb": d}).wait_recv()
    final = fin_ref[...].reshape(channels, LANES)
    gwout_ref[...] = final[:, :hid] * scale
    more_ref[...] = jnp.broadcast_to(final[0:1, :], more_ref.shape)

    def chosen(shift):
        return jnp.where(((l < 3) & (k == shift + l)) | ((l >= 3) & (l < 6) & (k == shift + 1 + l)) | ((l == 6) & (k == shift + 3)), scale, 0.0)

    taken = jnp.concatenate([exact(final, chosen(112)), exact(final[:tail], chosen(120))], 0)
    gwin_ref[...] = taken[:, : gwin_ref.shape[1]]
    pick6 = jnp.where(cols_of((8, LANES)) == 6, 1.0, 0.0)
    gbin_ref[...] = exact_nt(pick6, taken)[0:1]
    pickb = jnp.where(cols_of((8, LANES)) == hid + 3, scale, 0.0)
    gbout_ref[...] = exact_nt(pickb, final)[0:1]

    for copy in out + forwards + first_hop + second_hop + third_hop:
        copy.wait_send()
    for m in range(chips):
        near_copy(m).wait_send()
    for m in range(1, chips):
        far_copy(m).wait_send()


def call(step, collective_id, query_points, cotangent, slab_ids, rel_cells, offsets, latent, w_in, b_in, w_out, b_out):
    n_pb, n_ga = lax.axis_size("pb"), lax.axis_size("ga")
    channels, owned = latent.shape[1], latent.shape[2]
    hid = w_in.shape[0]
    queries = query_points.shape[1]
    tiles = queries // TILE
    chips = n_pb // 2
    blocks = owned // LANES
    pairs = SPAN * tiles
    lanes = -(-pairs // LANES) * LANES
    vmem = pl.BlockSpec(memory_space=pltpu.VMEM)
    smem = pl.BlockSpec(memory_space=pltpu.SMEM)
    dma = pltpu.SemaphoreType.DMA
    slices = channels // n_pb
    return pl.pallas_call(
        functools.partial(kernel, n_pb, n_ga, float(queries * n_pb) ** (-0.5)),
        out_shape=[
            jax.ShapeDtypeStruct((1, channels, owned), F32),
            jax.ShapeDtypeStruct(w_in.shape, F32),
            jax.ShapeDtypeStruct((1, hid), F32),
            jax.ShapeDtypeStruct(w_out.shape, F32),
            jax.ShapeDtypeStruct((1, channels), F32),
            jax.ShapeDtypeStruct((8, LANES), F32),
        ],
        in_specs=[smem, smem] + [vmem] * 10,
        out_specs=[vmem] * 6,
        scratch_shapes=[
            pltpu.VMEM((8, queries), F32),
            pltpu.VMEM((tiles * KN, TILE), F32),
            pltpu.VMEM((tiles * KN, TILE), F32),
            pltpu.VMEM((tiles * KN, TILE), F32),
            pltpu.VMEM((LANES, LANES), F32),
            pltpu.VMEM((hid, LANES), BF16),
            pltpu.VMEM((channels, LANES), BF16),
            pltpu.VMEM((hid, channels), BF16),
            pltpu.VMEM((8, lanes), I32),
            pltpu.SMEM((8, lanes), I32),
            pltpu.VMEM((tiles, channels, CAP), BF16),
            pltpu.VMEM((tiles, hid, CAP), BF16),
            pltpu.VMEM((tiles, hid, CAP), F32),
            pltpu.VMEM((tiles, XR, CAP), BF16),
            pltpu.VMEM((tiles, 8, CAP), F32),
            pltpu.VMEM((pairs, channels, LANES), F32),
            pltpu.VMEM((pairs, channels, LANES), F32),
            pltpu.VMEM((n_pb * blocks, channels, LANES), BF16),
            pltpu.VMEM((chips, blocks, channels, LANES), BF16),
            pltpu.VMEM((chips, blocks, channels, LANES), BF16),
            pltpu.VMEM((chips - 1, blocks, channels, LANES), BF16),
            pltpu.VMEM((chips - 1, blocks, channels, LANES), BF16),
            pltpu.VMEM((blocks, channels, LANES), F32),
            pltpu.VMEM((channels + hid, LANES), F32),
            pltpu.VMEM((n_pb, slices, LANES), F32),
            pltpu.VMEM((n_pb, slices, LANES), F32),
            pltpu.VMEM((n_ga, slices, LANES), F32),
            pltpu.VMEM((n_pb, slices, LANES), F32),
            dma,
            dma((chips,)),
            dma((n_pb,)),
            dma((chips,)),
            dma((chips,)),
            dma((chips,)),
            dma((chips,)),
            dma((chips,)),
            dma((n_pb,)),
            dma((n_pb,)),
            dma((n_ga,)),
            dma((n_ga,)),
            dma((n_pb,)),
            dma((n_pb,)),
        ],
        compiler_params=pltpu.CompilerParams(
            vmem_limit_bytes=60 * 2**20, collective_id=collective_id, has_side_effects=True
        ),
        name="whole",
    )(step, offsets, offsets, query_points, cotangent, slab_ids, rel_cells, latent, w_in, b_in[None], w_out, b_out[None])


def shards(*args):
    def run(step, collective_id):
        return tuple(call(step, collective_id, *args))

    def left(state):
        return state[1][5][0, 119] > 0

    def again(state):
        step, sums = state
        new = run(step, 1)
        return step + 1, tuple(a + b for a, b in zip(sums[:5], new[:5])) + (new[5],)

    sums = run(jnp.zeros((1,), I32), 0)
    _, sums = lax.while_loop(left, again, (jnp.ones((1,), I32), sums))
    return sums[0], sums[1], sums[2][0], sums[3], sums[4][0]


def solution(mesh):
    return jax.shard_map(
        shards,
        mesh=mesh,
        in_specs=(
            P(None, "pb"),
            P(None, "pb"),
            P(None, "pb"),
            P(None, "pb"),
            P("ga", "pb"),
            P("ga", None, "pb"),
            P(),
            P(),
            P(),
            P(),
        ),
        out_specs=(P("ga", None, "pb"), P(), P(), P(), P()),
        check_vma=False,
    )
```

```python
import functools
import math

import jax
import jax.numpy as jnp
from jax import lax
from jax.experimental import pallas as pl
from jax.experimental.pallas import tpu as pltpu
from jax.sharding import PartitionSpec as P

KN = 8
TILE = 128
WIN = 512
GX = 64
ZS = 4
LANES = 128
SPAN = WIN // LANES + 1
CAP = 256
XR = 48
F32 = jnp.float32
BF16 = jnp.bfloat16
I32 = jnp.int32
MESH = pl.DeviceIdType.MESH
HIGHEST = lax.Precision.HIGHEST


def dot(a, b):
    return jnp.dot(a, b, preferred_element_type=F32)


def dot_nt(a, b):
    return lax.dot_general(a, b, (((1,), (1,)), ((), ())), preferred_element_type=F32)


def exact(a, b):
    return jnp.dot(a, b, preferred_element_type=F32, precision=HIGHEST)


def exact_nt(a, b):
    return lax.dot_general(a, b, (((1,), (1,)), ((), ())), preferred_element_type=F32, precision=HIGHEST)


def rows_of(shape):
    return lax.broadcasted_iota(I32, shape, 0)


def cols_of(shape):
    return lax.broadcasted_iota(I32, shape, 1)


def gelu_parts(x):
    z = jnp.abs(x) * (2.0**-0.5)
    t = 1.0 / (1.0 + 0.3275911 * z)
    e = jnp.exp(-0.5 * x * x)
    poly = ((((1.061405429 * t - 1.453152027) * t + 1.421413741) * t - 0.284496736) * t + 0.254829592) * t
    tail = 0.5 * poly * e
    cdf = jnp.where(x < 0, tail, 1.0 - tail)
    return x * cdf, cdf + x * e * ((2.0 * math.pi) ** -0.5)


def mask_of(cond):
    return jnp.where(cond, 1.0, 0.0).astype(BF16)


def split3(v):
    a = v.astype(BF16)
    r = v - a.astype(F32)
    b = r.astype(BF16)
    return a, b, (r - b.astype(F32)).astype(BF16)


def weights(win_ref, bin_ref, wout_ref, bout_ref, pad_ref, w1_ref, w2_ref, w2t_ref):
    hid, channels = win_ref.shape[1], wout_ref.shape[0]
    pad_ref[...] = jnp.zeros_like(pad_ref)
    pad_ref[: win_ref.shape[0], :hid] = win_ref[...]
    wide = pad_ref[...].T[:hid]
    w_hi = wide.astype(BF16)
    w_lo = (wide - w_hi.astype(F32)).astype(BF16)
    k, col = rows_of((LANES, LANES)), cols_of((LANES, LANES))
    s_hi = mask_of(((k < 3) & ((col == k) | (col == k + 8))) | ((k >= 3) & (k < 6) & (col == k + 13)))
    s_lo = mask_of(((k < 3) & (col == k + 24)) | ((k >= 3) & (k < 6) & (col == k + 29)))
    w1 = dot(w_hi, s_hi) + dot(w_lo, s_lo)
    pad_ref[0:1, :hid] = bin_ref[...]
    pad_ref[0:1, hid:] = jnp.zeros((1, LANES - hid), F32)
    diag = jnp.where(rows_of((hid, LANES)) == cols_of((hid, LANES)), pad_ref[0:1, :], 0.0)
    for i, part in enumerate(split3(diag)):
        w1 += dot(part, mask_of(col == 3 + i))
    w1_ref[...] = w1.astype(BF16)

    pad_ref[0:channels, :hid] = wout_ref[...].astype(F32)
    pad_ref[0:channels, hid:] = jnp.zeros((channels, LANES - hid), F32)
    w_out = pad_ref[0:channels, :].astype(BF16)
    w2 = dot(w_out, mask_of(k == col))
    eye = mask_of(rows_of((hid, LANES)) == cols_of((hid, LANES)))
    w2t_ref[...] = dot_nt(eye, w_out).astype(BF16)
    pad_ref[0:1, :channels] = bout_ref[...]
    diag = jnp.where(rows_of((channels, LANES)) == cols_of((channels, LANES)), pad_ref[0:1, :], 0.0)
    for i, part in enumerate(split3(diag)):
        w2 += dot(part, mask_of(col == hid + 3 + i))
    w2_ref[...] = w2.astype(BF16)


def order_parts(tiles, limit, offv_ref, table_ref):
    pairs = SPAN * tiles
    lanes = -(-pairs // LANES) * LANES
    base_row = jnp.minimum(lax.shift_right_logical(offv_ref[...], 7), limit)
    wide = jnp.concatenate([base_row, jnp.zeros((1, LANES - tiles), I32)], 1)
    pick = rows_of((tiles, LANES)) == cols_of((tiles, LANES))
    column = jnp.sum(jnp.where(pick, wide.astype(F32), 0.0), 1, keepdims=True)
    key = jnp.concatenate([column + float(j) for j in range(SPAN)], 0)
    key = jnp.broadcast_to(key, (pairs, lanes))
    p, q = rows_of((pairs, lanes)), cols_of((pairs, lanes))
    key_row = jnp.sum(jnp.where(p == q, key, 0.0), 0, keepdims=True)
    key_row = jnp.where(q[:1] < pairs, key_row, 1.0e6)
    ahead = (key_row == key) & (q < p)
    rank = jnp.sum(jnp.where((key_row < key) | ahead, 1.0, 0.0), 1, keepdims=True)
    again = jnp.sum(jnp.where(ahead, 1.0, 0.0), 1, keepdims=True)
    here = rank == q.astype(F32)
    order = jnp.sum(jnp.where(here, p.astype(F32), 0.0), 0, keepdims=True)
    keep = jnp.sum(jnp.where(here & (again > 0), 1.0, 0.0), 0, keepdims=True)
    upto = jnp.sum(jnp.where(key <= q.astype(F32), 1.0, 0.0), 0, keepdims=True)
    some = jnp.sum(jnp.where(key == q.astype(F32), 1.0, 0.0), 0, keepdims=True)
    some = jnp.minimum(some, 1.0)
    last = jnp.maximum(upto - 1.0, 0.0)
    rows = jnp.concatenate([order, keep, last, some, jnp.zeros((4, lanes), F32)], 0)
    table_ref[...] = rows.astype(I32)


def kernel(
    n_pb, n_ga,
    n_ins, latent_in, *rest,
):
    ins, rest = rest[:n_ins], rest[n_ins:]
    outs, rest = rest[:3], rest[3:]
    held, rest = rest[:n_ins], rest[n_ins:]
    ready, rest = rest[:3], rest[3:]
    body(n_pb, n_ga, latent_in, ins, outs, held, ready, *rest)


def body(
    n_pb, n_ga, latent_in, ins, outs, held, ready,
    pts_ref, pos_ref, from_ref, upto_ref, pad_ref, w1_ref, w2_ref, w2t_ref, tablev_ref, table_ref,
    cots_ref, hid_ref, slope_ref, x_ref, spot_ref, parts_ref, sums_ref, feats_ref,
    near_ref, nearin_ref, far_ref, farin_ref, own_ref, acc_ref,
    ar_ref, arin_ref, gaall_ref, fin_ref,
    in_sem, latent_sem, out_sem, table_sem, gsend, grecv, fsend, nsend, nrecv, rsend, rrecv, asend, arecv, bsend, brecv, csend, crecv,
):
    offs_ref, offv_ref, win_ref, bin_ref, wout_ref, bout_ref, ids_ref, qp_ref, rel_ref, cot_ref = held[:10]
    gridv_ref, final_ref, more_ref = ready
    me, slab = lax.axis_index("pb"), lax.axis_index("ga")
    chips = n_pb // 2
    chip, core = me // 2, me % 2
    sibling = chip * 2 + 1 - core
    tiles = cot_ref.shape[1] // TILE
    channels, hid = cot_ref.shape[0], win_ref.shape[1]
    blocks = latent_in.shape[2] // LANES
    limit = blocks * n_pb - SPAN
    group = math.gcd(tiles, 4)

    def send(src, dst, ssem, rsem, where):
        return pltpu.make_async_remote_copy(
            src_ref=src, dst_ref=dst, send_sem=ssem, recv_sem=rsem, device_id=where, device_id_type=MESH
        )

    def peer(m):
        return lax.rem(chip + m, chips) * 2 + core

    def peer_back(m):
        return lax.rem(chip + chips - m, chips) * 2 + core

    barrier = pltpu.get_barrier_semaphore()
    mine = me * blocks
    latent_copies = [
        pltpu.make_async_copy(latent_in.at[0, :, pl.ds(b * LANES, LANES)], feats_ref.at[mine + b], latent_sem.at[b])
        for b in range(blocks)
    ]
    loads = [pltpu.make_async_copy(src, dst, in_sem.at[i]) for i, (src, dst) in enumerate(zip(ins, held))]
    for copy in latent_copies + loads:
        copy.start()
    for m in range(1, n_pb):
        pl.semaphore_signal(barrier, inc=1, device_id={"pb": lax.rem(me + m, n_pb)}, device_id_type=MESH)
    for m in range(1, n_ga):
        pl.semaphore_signal(barrier, inc=1, device_id={"ga": lax.rem(slab + m, n_ga)}, device_id_type=MESH)

    def feats_of(d):
        return feats_ref.at[pl.ds(d * blocks, blocks)]

    for copy in latent_copies:
        copy.wait()
    pl.semaphore_wait(barrier, n_pb - 1 + n_ga - 1)
    out = []
    for m in range(1, chips):
        out.append(send(feats_of(me), feats_of(me), gsend.at[m], grecv.at[me], {"pb": peer(m)}))
    out.append(send(feats_of(me), feats_of(me), gsend.at[0], grecv.at[me], {"pb": sibling}))
    for copy in out:
        copy.start()

    for copy in loads:
        copy.wait()
    pts_ref[...] = jnp.ones_like(pts_ref)
    pts_ref[0:3, :] = qp_ref[...]
    order_parts(tiles, limit, offv_ref, tablev_ref)
    weights(win_ref, bin_ref, wout_ref, bout_ref, pad_ref, w1_ref, w2_ref, w2t_ref)
    table_copy = pltpu.make_async_copy(tablev_ref, table_ref, table_sem)
    table_copy.start()

    lives = [jnp.where(ids_ref[:, t * TILE : (t + 1) * TILE] == slab, 1.0, 0.0) for t in range(tiles)]
    live = jnp.concatenate(lives, 0)
    rows = tiles * KN
    packed = live.astype(BF16)
    before = dot(packed, mask_of(rows_of((TILE, TILE)) < cols_of((TILE, TILE))))
    total = dot(packed, jnp.ones((TILE, TILE), BF16))
    r, c = rows_of((rows, rows)), cols_of((rows, rows))
    start = dot(mask_of((r // KN == c // KN) & (c < r)), total.astype(BF16))
    skip = (held[10][0] * CAP).astype(F32) if len(held) > 10 else 0.0
    pos_ref[...] = jnp.where(live > 0, before + start - skip, -1.0e6)
    from_ref[...] = start - skip
    upto_ref[...] = start + total - skip
    left = jnp.max(start + total - skip - float(CAP), axis=0, keepdims=True)
    left = jnp.max(left, axis=1, keepdims=True)

    def tile_base(t):
        return jnp.minimum(lax.shift_right_logical(offs_ref[0, t], 7), limit)

    def draw(t):
        cols = pl.ds(pl.multiple_of(t * TILE, TILE), TILE)
        lines = pl.ds(pl.multiple_of(t * KN, KN), KN)
        base = tile_base(t)
        pos = pos_ref[lines, :].astype(BF16)
        place = rows_of((CAP, TILE)).astype(F32).astype(BF16)
        pick = jnp.zeros((CAP, TILE), BF16)
        one = jnp.ones((CAP, TILE), BF16)
        for k in range(KN):
            pick = jnp.where(pos[k : k + 1, :] == place, one, pick)
        relp = rel_ref[:, cols] + (offs_ref[0, t] - base * LANES)
        low = (relp & (LANES - 1)).astype(F32)
        high = lax.shift_right_logical(relp, 7).astype(F32)
        points = pts_ref[:, cols]
        p_hi = points.astype(BF16).astype(F32)
        small = jnp.concatenate([p_hi, points - p_hi, low, high], 0).astype(BF16)
        data = jnp.concatenate([cot_ref[:, cols], small], 0)
        return dot_nt(data, pick)

    def place_inputs(t, drawn):
        lines = pl.ds(pl.multiple_of(t * KN, KN), KN)
        base = tile_base(t)
        head = drawn[channels : channels + 16]
        wide_from = jnp.concatenate([from_ref[lines, :]] * (CAP // TILE), 1)
        wide_upto = jnp.concatenate([upto_ref[lines, :]] * (CAP // TILE), 1)
        index = cols_of((KN, CAP)).astype(F32)
        which = (index >= wide_from) & (index < wide_upto)
        lo = jnp.sum(jnp.where(which, drawn[channels + 16 : channels + 24], 0.0), 0, keepdims=True)
        hi = jnp.sum(jnp.where(which, drawn[channels + 24 : channels + 32], 0.0), 0, keepdims=True)
        lo = jnp.broadcast_to(lo, (8, CAP))
        hi = jnp.broadcast_to(hi, (8, CAP))
        cell = (base + hi.astype(I32)) * LANES + lo.astype(I32)
        row = rows_of((8, CAP))
        along = jnp.where(
            row == 0,
            lax.shift_right_logical(cell, int(math.log2(GX * ZS))),
            jnp.where(
                row == 1,
                lax.shift_right_logical(cell, int(math.log2(ZS))) & (GX - 1),
                (cell & (ZS - 1)) + slab * ZS,
            ),
        )
        centre = jnp.where(row < 3, (along.astype(F32) + 0.5) / GX, 0.0)
        x = jnp.concatenate([head, centre, head[:8], centre, jnp.zeros((8, CAP), F32)], 0).astype(BF16)
        return x, lo, hi

    def lane_onehot(lo):
        row = jnp.broadcast_to(lo[:1], (LANES, CAP)).astype(BF16)
        return jnp.where(
            rows_of((LANES, CAP)).astype(F32).astype(BF16) == row, jnp.ones((LANES, CAP), BF16), jnp.zeros((LANES, CAP), BF16)
        )

    def spread(hi, grad):
        full = jnp.concatenate([hi, hi], 0)
        pieces = []
        for j in range(SPAN):
            on = jnp.where(full == float(j), 1.0, 0.0).astype(BF16)
            pieces.append(grad * jnp.concatenate([on] * (channels // 16), 0))
        return jnp.concatenate(pieces, 0)

    def first(i, carry):
        ts = [i * group + u for u in range(group)]
        drawn = [draw(t) for t in ts]
        placed = [place_inputs(t, d) for t, d in zip(ts, drawn)]
        cots = [d[:channels].astype(BF16) for d in drawn]
        pres = [dot(w1_ref[:, :XR], x) for x, _, _ in placed]
        kerns = []
        for t, pre, cot, (x, lo, hi) in zip(ts, pres, cots, placed):
            hidden, slope = gelu_parts(pre)
            hidden = hidden.astype(BF16)
            kerns.append(dot(w2_ref[...], jnp.concatenate([hidden, x], 0)))
            hid_ref[t] = hidden
            slope_ref[t] = slope
            cots_ref[t] = cot
            x_ref[t] = x
            spot_ref[t] = jnp.where(rows_of((8, CAP)) < 4, lo, hi)
        parts = []
        for kern, cot, (x, lo, hi) in zip(kerns, cots, placed):
            grad = (kern * cot.astype(F32)).astype(BF16)
            parts.append(dot_nt(spread(hi, grad), lane_onehot(lo)))
        for t, part in zip(ts, parts):
            for j in range(SPAN):
                parts_ref[j * tiles + t] = part[j * channels : (j + 1) * channels]
        return carry

    lax.fori_loop(0, tiles // group, first, 0)

    table_copy.wait()

    def pair_at(line, b):
        return jnp.clip(table_ref[line, b], 0, SPAN * tiles - 1)

    def run(i, acc):
        for u in range(group):
            at = i * group + u
            acc = acc * table_ref[1, at].astype(F32) + parts_ref[pair_at(0, at)]
            sums_ref[at] = acc
        return acc

    lax.fori_loop(0, SPAN * tiles // group, run, jnp.zeros((channels, LANES), F32))

    def block(b):
        return sums_ref[pair_at(2, b)] * table_ref[3, b].astype(F32)

    def near_copy(m):
        return send(near_ref.at[m], nearin_ref.at[m], nsend.at[m], nrecv.at[m], {"pb": sibling})

    pair = math.gcd(blocks, 4)
    order = [m % chips for m in range(1, chips + 1)]
    for i, m in enumerate(order):
        owner = lax.rem(chip + m, chips) * 2 + 1 - core

        def fill(b, carry, m=m, owner=owner):
            for u in range(pair):
                near_ref[m, b * pair + u] = block(owner * blocks + b * pair + u).astype(BF16)
            return carry

        lax.fori_loop(0, blocks // pair, fill, 0)
        if i > 0:
            near_copy(order[i - 1]).start()
    forwards = []
    for m in range(1, chips):
        d = peer_back(m)
        send(feats_of(d), feats_of(d), gsend.at[m], grecv.at[d], {"pb": d}).wait_recv()
        copy = send(feats_of(d), feats_of(d), fsend.at[m - 1], grecv.at[d], {"pb": sibling})
        copy.start()
        forwards.append(copy)
        if m == 1:
            near_copy(order[-1]).start()

    def far_copy(m):
        return send(far_ref.at[m - 1], farin_ref.at[m - 1], rsend.at[m - 1], rrecv.at[m - 1], {"pb": peer(m)})

    for i, m in enumerate(order):
        owner = lax.rem(chip + m, chips) * 2 + core
        near_copy(m).wait_recv()

        def join(b, carry, m=m, owner=owner):
            for u in range(pair):
                at = b * pair + u
                value = block(owner * blocks + at) + nearin_ref[m, at].astype(F32)
                if m:
                    far_ref[m - 1, at] = value.astype(BF16)
                else:
                    own_ref[at] = value
            return carry

        lax.fori_loop(0, blocks // pair, join, 0)
        if i > 0:
            far_copy(order[i - 1]).start()

    for m in range(chips):
        d = lax.rem(chip + m, chips) * 2 + 1 - core
        send(feats_of(d), feats_of(d), gsend.at[0], grecv.at[d], {"pb": sibling}).wait_recv()

    acc_ref[...] = jnp.zeros_like(acc_ref)

    def draw_feats(t):
        window = feats_ref[pl.ds(tile_base(t), SPAN)].reshape(SPAN * channels, LANES)
        return dot(window, lane_onehot(spot_ref[t]))

    def feats_grad(t, drawn):
        tall = jnp.broadcast_to(spot_ref[t][4:5], (channels, CAP))
        feats = drawn[:channels]
        for j in range(1, SPAN):
            feats = jnp.where(tall == float(j), drawn[j * channels : (j + 1) * channels], feats)
        return (feats * cots_ref[t].astype(F32)).astype(BF16)

    def second(i, carry):
        ts = [i * group + u for u in range(group)]
        drawn = [draw_feats(t) for t in ts]
        grads = [feats_grad(t, d) for t, d in zip(ts, drawn)]
        pres = [dot(w2t_ref[...], g) for g in grads]
        sums = []
        for t, g, p in zip(ts, grads, pres):
            both = jnp.concatenate([g, (p * slope_ref[t]).astype(BF16)], 0)
            sums.append(dot_nt(both, jnp.concatenate([hid_ref[t], x_ref[t]], 0)))
        acc_ref[...] += functools.reduce(lambda a, b: a + b, sums)
        return carry

    lax.fori_loop(0, tiles // group, second, 0)

    k, l = rows_of((LANES, LANES)), cols_of((LANES, LANES))

    def gathered(shift):
        a = (l - shift >= 0) & (l - shift < 4) & ((k == hid + l - shift) | ((k == hid + 8 + l - shift) & (l - shift < 3)))
        b = (l - shift >= 4) & (l - shift < 7) & (k == hid + 16 + l - shift - 4)
        return jnp.where(a | b, 1.0, 0.0)

    top = jnp.where(cols_of((channels, LANES)) < 112, acc_ref[:channels], 0.0)
    tail = hid - channels
    top += exact(acc_ref[channels : 2 * channels], gathered(112))
    rest = exact(acc_ref[2 * channels : 2 * channels + tail], gathered(120))
    flag = jnp.where(left > 0, 1.0, 0.0)
    corner = (rows_of((tail, LANES)) == 0) & (cols_of((tail, LANES)) == 119)
    rest = jnp.where(corner, flag, rest)
    top = jnp.concatenate([top[:tail] + rest, top[tail:]], 0)
    slices = channels // n_pb
    ar_ref[...] = top.reshape(n_pb, slices, LANES)
    arin_ref[pl.ds(me, 1)] = ar_ref[pl.ds(me, 1)]
    first_hop = []
    for m in range(1, n_pb):
        to = lax.rem(me + m, n_pb)
        copy = send(ar_ref.at[to], arin_ref.at[me], asend.at[m - 1], arecv.at[me], {"pb": to})
        copy.start()
        first_hop.append(copy)
    for m in range(1, n_pb):
        d = lax.rem(me + m, n_pb)
        send(ar_ref.at[d], arin_ref.at[d], asend.at[m - 1], arecv.at[d], {"pb": d}).wait_recv()
    gaall_ref[pl.ds(slab, 1)] = jnp.sum(arin_ref[...], 0, keepdims=True)
    second_hop = []
    for m in range(1, n_ga):
        to = lax.rem(slab + m, n_ga)
        copy = send(gaall_ref.at[slab], gaall_ref.at[slab], bsend.at[m - 1], brecv.at[slab], {"ga": to})
        copy.start()
        second_hop.append(copy)
    for m in range(1, n_ga):
        d = lax.rem(slab + m, n_ga)
        send(gaall_ref.at[d], gaall_ref.at[d], bsend.at[m - 1], brecv.at[d], {"ga": d}).wait_recv()
    fin_ref[pl.ds(me, 1)] = jnp.sum(gaall_ref[...], 0, keepdims=True)
    third_hop = []
    for m in range(1, n_pb):
        to = lax.rem(me + m, n_pb)
        copy = send(fin_ref.at[me], fin_ref.at[me], csend.at[m - 1], crecv.at[me], {"pb": to})
        copy.start()
        third_hop.append(copy)

    for m in range(1, chips):
        far_copy(m).wait_recv()
    for b in range(blocks):
        value = own_ref[b]
        for m in range(1, chips):
            value += farin_ref[m - 1, b].astype(F32)
        gridv_ref[0, :, b * LANES : (b + 1) * LANES] = value
    stores = [pltpu.make_async_copy(src, dst, out_sem.at[i]) for i, (src, dst) in enumerate(zip(ready, outs))]
    stores[0].start()

    for m in range(1, n_pb):
        d = lax.rem(me + m, n_pb)
        send(fin_ref.at[d], fin_ref.at[d], csend.at[m - 1], crecv.at[d], {"pb": d}).wait_recv()
    final = fin_ref[...].reshape(channels, LANES)
    final_ref[...] = final
    flags = jnp.where(cols_of((1, LANES)) == 119, final[0:1], 0.0)
    more_ref[0] = jnp.sum(flags).astype(I32)
    for copy in stores[1:]:
        copy.start()
    for copy in stores:
        copy.wait()
    for copy in out + forwards + first_hop + second_hop + third_hop:
        copy.wait_send()
    for m in range(chips):
        near_copy(m).wait_send()
    for m in range(1, chips):
        far_copy(m).wait_send()


def call(step, collective_id, query_points, cotangent, slab_ids, rel_cells, offsets, latent, w_in, b_in, w_out, b_out):
    n_pb, n_ga = lax.axis_size("pb"), lax.axis_size("ga")
    channels, owned = latent.shape[1], latent.shape[2]
    hid = w_in.shape[0]
    queries = query_points.shape[1]
    tiles = queries // TILE
    chips = n_pb // 2
    blocks = owned // LANES
    pairs = SPAN * tiles
    lanes = -(-pairs // LANES) * LANES
    hbm = pl.BlockSpec(memory_space=pltpu.HBM)
    dma = pltpu.SemaphoreType.DMA
    slices = channels // n_pb
    ins = (offsets, offsets, w_in.T, b_in[None], w_out, b_out[None], slab_ids, query_points, rel_cells, cotangent)
    ins += () if step is None else (step,)
    outs = [
        ((1, channels, owned), F32),
        ((channels, LANES), F32),
        ((1,), I32),
    ]
    return pl.pallas_call(
        functools.partial(kernel, n_pb, n_ga, len(ins)),
        out_shape=[jax.ShapeDtypeStruct(*o) for o in outs],
        in_specs=[hbm] * (1 + len(ins)),
        out_specs=[hbm] * len(outs),
        scratch_shapes=[(pltpu.SMEM if i in (0, 10) else pltpu.VMEM)(a.shape, a.dtype) for i, a in enumerate(ins)]
        + [pltpu.VMEM(*outs[0]), pltpu.VMEM(*outs[1]), pltpu.SMEM(*outs[2])]
        + [
            pltpu.VMEM((8, queries), F32),
            pltpu.VMEM((tiles * KN, TILE), F32),
            pltpu.VMEM((tiles * KN, TILE), F32),
            pltpu.VMEM((tiles * KN, TILE), F32),
            pltpu.VMEM((LANES, LANES), F32),
            pltpu.VMEM((hid, LANES), BF16),
            pltpu.VMEM((channels, LANES), BF16),
            pltpu.VMEM((hid, channels), BF16),
            pltpu.VMEM((8, lanes), I32),
            pltpu.SMEM((8, lanes), I32),
            pltpu.VMEM((tiles, channels, CAP), BF16),
            pltpu.VMEM((tiles, hid, CAP), BF16),
            pltpu.VMEM((tiles, hid, CAP), F32),
            pltpu.VMEM((tiles, XR, CAP), BF16),
            pltpu.VMEM((tiles, 8, CAP), F32),
            pltpu.VMEM((pairs, channels, LANES), F32),
            pltpu.VMEM((pairs, channels, LANES), F32),
            pltpu.VMEM((n_pb * blocks, channels, LANES), BF16),
            pltpu.VMEM((chips, blocks, channels, LANES), BF16),
            pltpu.VMEM((chips, blocks, channels, LANES), BF16),
            pltpu.VMEM((chips - 1, blocks, channels, LANES), BF16),
            pltpu.VMEM((chips - 1, blocks, channels, LANES), BF16),
            pltpu.VMEM((blocks, channels, LANES), F32),
            pltpu.VMEM((channels + hid, LANES), F32),
            pltpu.VMEM((n_pb, slices, LANES), F32),
            pltpu.VMEM((n_pb, slices, LANES), F32),
            pltpu.VMEM((n_ga, slices, LANES), F32),
            pltpu.VMEM((n_pb, slices, LANES), F32),
            dma((len(ins),)),
            dma((blocks,)),
            dma((len(outs),)),
            dma,
            dma((chips,)),
            dma((n_pb,)),
            dma((chips,)),
            dma((chips,)),
            dma((chips,)),
            dma((chips,)),
            dma((chips,)),
            dma((n_pb,)),
            dma((n_pb,)),
            dma((n_ga,)),
            dma((n_ga,)),
            dma((n_pb,)),
            dma((n_pb,)),
        ],
        compiler_params=pltpu.CompilerParams(
            vmem_limit_bytes=67043328, collective_id=collective_id, has_side_effects=True
        ),
        name="whole",
    )(latent, *ins)


def settle(scale, grid_in, final_in, grid_ref, *rest):
    smalls, (final_ref, hold_ref), ready = rest[:4], rest[4:6], rest[6:10]
    load_sem, in_sem, out_sem, small_sem = rest[10:]
    gwin_ref, gbin_ref, gwout_ref, gbout_ref = ready
    load = pltpu.make_async_copy(final_in, final_ref, load_sem)
    load.start()
    parts = out_sem.shape[0]
    wide = grid_ref.shape[2] // parts
    arrive, leave = [], []
    for i in range(parts):
        at = (0, slice(None), pl.ds(i * wide, wide))
        arrive.append(pltpu.make_async_copy(grid_in.at[at], hold_ref.at[at], in_sem.at[i]))
        leave.append(pltpu.make_async_copy(hold_ref.at[at], grid_ref.at[at], out_sem.at[i]))
        arrive[-1].start()
    load.wait()
    channels, hid = gwout_ref.shape
    final = final_ref[...]
    k, l = rows_of((LANES, LANES)), cols_of((LANES, LANES))

    def chosen(shift):
        along = (l < 3) & (k == shift + l)
        cells = (l >= 3) & (l < 6) & (k == shift + 1 + l)
        return jnp.where(along | cells | ((l == 6) & (k == shift + 3)), scale, 0.0)

    gwout_ref[...] = final[:, :hid] * scale
    taken = jnp.concatenate([exact(final, chosen(112)), exact(final[: hid - channels], chosen(120))], 0)
    turned = exact_nt(jnp.where(rows_of((8, LANES)) == cols_of((8, LANES)), 1.0, 0.0), taken)
    gwin_ref[...] = turned[: gwin_ref.shape[0]]
    gbin_ref[...] = turned[6:7]
    gbout_ref[...] = exact_nt(jnp.where(cols_of((8, LANES)) == hid + 3, scale, 0.0), final)[0:1]
    for i in range(parts):
        arrive[i].wait()
        leave[i].start()
    stores = [pltpu.make_async_copy(src, dst, small_sem.at[i]) for i, (src, dst) in enumerate(zip(ready, smalls))]
    for copy in stores:
        copy.start()
    for copy in leave + stores:
        copy.wait()


def shards(*args):
    def again(state):
        step, _, sums = state
        grid, final, more = call(step, 1, *args)
        return step + 1, more, (sums[0] + grid, sums[1] + final)

    grid, final, more = call(None, 0, *args)
    first = (jnp.ones((1,), I32), more, (grid, final))
    grid, final = lax.while_loop(lambda state: state[1][0] > 0, again, first)[2]
    hid, channels = args[6].shape[0], args[8].shape[0]
    queries = args[0].shape[1] * lax.axis_size("pb")
    hbm = pl.BlockSpec(memory_space=pltpu.HBM)
    dma = pltpu.SemaphoreType.DMA
    parts = math.gcd(grid.shape[2] // LANES, 4)
    shapes = [args[6].shape[::-1], (1, hid), (channels, hid), (1, channels)]
    grid, gwin, gbin, gwout, gbout = pl.pallas_call(
        functools.partial(settle, float(queries) ** (-0.5)),
        out_shape=[jax.ShapeDtypeStruct(v, F32) for v in [grid.shape] + shapes],
        in_specs=[hbm] * 2,
        out_specs=[hbm] * 5,
        scratch_shapes=[pltpu.VMEM(v, F32) for v in [final.shape, grid.shape] + shapes]
        + [dma, dma((parts,)), dma((parts,)), dma((4,))],
        name="settle",
    )(grid, final)
    return grid, gwin.T, gbin[0], gwout, gbout[0]


def solution(mesh):
    return jax.shard_map(
        shards,
        mesh=mesh,
        in_specs=(
            P(None, "pb"),
            P(None, "pb"),
            P(None, "pb"),
            P(None, "pb"),
            P("ga", "pb"),
            P("ga", None, "pb"),
            P(),
            P(),
            P(),
            P(),
        ),
        out_specs=(P("ga", None, "pb"), P(), P(), P(), P()),
        check_vma=False,
    )
```

```python
import functools
import math

import jax
import jax.numpy as jnp
from jax import lax
from jax.experimental import pallas as pl
from jax.experimental.pallas import tpu as pltpu
from jax.sharding import PartitionSpec as P

KN = 8
TILE = 128
WIN = 512
GX = 64
ZS = 4
LANES = 128
SPAN = WIN // LANES + 1
CAP = 256
XR = 48
F32 = jnp.float32
BF16 = jnp.bfloat16
I32 = jnp.int32
MESH = pl.DeviceIdType.MESH
HIGHEST = lax.Precision.HIGHEST


def dot(a, b):
    return jnp.dot(a, b, preferred_element_type=F32)


def dot_nt(a, b):
    return lax.dot_general(a, b, (((1,), (1,)), ((), ())), preferred_element_type=F32)


def exact(a, b):
    return jnp.dot(a, b, preferred_element_type=F32, precision=HIGHEST)


def exact_nt(a, b):
    return lax.dot_general(a, b, (((1,), (1,)), ((), ())), preferred_element_type=F32, precision=HIGHEST)


def rows_of(shape):
    return lax.broadcasted_iota(I32, shape, 0)


def cols_of(shape):
    return lax.broadcasted_iota(I32, shape, 1)


def gelu_parts(x):
    z = jnp.abs(x) * (2.0**-0.5)
    t = 1.0 / (1.0 + 0.3275911 * z)
    e = jnp.exp(-0.5 * x * x)
    poly = ((((1.061405429 * t - 1.453152027) * t + 1.421413741) * t - 0.284496736) * t + 0.254829592) * t
    tail = 0.5 * poly * e
    cdf = jnp.where(x < 0, tail, 1.0 - tail)
    return x * cdf, cdf + x * e * ((2.0 * math.pi) ** -0.5)


def mask_of(cond):
    return jnp.where(cond, 1.0, 0.0).astype(BF16)


def split3(v):
    a = v.astype(BF16)
    r = v - a.astype(F32)
    b = r.astype(BF16)
    return a, b, (r - b.astype(F32)).astype(BF16)


def weights(win_ref, bin_ref, wout_ref, bout_ref, pad_ref, w1_ref, w2_ref, w2t_ref):
    hid, channels = win_ref.shape[1], wout_ref.shape[0]
    pad_ref[...] = jnp.zeros_like(pad_ref)
    pad_ref[: win_ref.shape[0], :hid] = win_ref[...]
    wide = pad_ref[...].T[:hid]
    w_hi = wide.astype(BF16)
    w_lo = (wide - w_hi.astype(F32)).astype(BF16)
    k, col = rows_of((LANES, LANES)), cols_of((LANES, LANES))
    s_hi = mask_of(((k < 3) & ((col == k) | (col == k + 8))) | ((k >= 3) & (k < 6) & (col == k + 13)))
    s_lo = mask_of(((k < 3) & (col == k + 24)) | ((k >= 3) & (k < 6) & (col == k + 29)))
    w1 = dot(w_hi, s_hi) + dot(w_lo, s_lo)
    pad_ref[0:1, :hid] = bin_ref[...]
    pad_ref[0:1, hid:] = jnp.zeros((1, LANES - hid), F32)
    diag = jnp.where(rows_of((hid, LANES)) == cols_of((hid, LANES)), pad_ref[0:1, :], 0.0)
    for i, part in enumerate(split3(diag)):
        w1 += dot(part, mask_of(col == 3 + i))
    w1_ref[...] = w1.astype(BF16)

    pad_ref[0:channels, :hid] = wout_ref[...].astype(F32)
    pad_ref[0:channels, hid:] = jnp.zeros((channels, LANES - hid), F32)
    w_out = pad_ref[0:channels, :].astype(BF16)
    w2 = dot(w_out, mask_of(k == col))
    eye = mask_of(rows_of((hid, LANES)) == cols_of((hid, LANES)))
    w2t_ref[...] = dot_nt(eye, w_out).astype(BF16)
    pad_ref[0:1, :channels] = bout_ref[...]
    diag = jnp.where(rows_of((channels, LANES)) == cols_of((channels, LANES)), pad_ref[0:1, :], 0.0)
    for i, part in enumerate(split3(diag)):
        w2 += dot(part, mask_of(col == hid + 3 + i))
    w2_ref[...] = w2.astype(BF16)


def order_parts(tiles, limit, offv_ref, table_ref):
    pairs = SPAN * tiles
    lanes = -(-pairs // LANES) * LANES
    base_row = jnp.minimum(lax.shift_right_logical(offv_ref[...], 7), limit)
    wide = jnp.concatenate([base_row, jnp.zeros((1, LANES - tiles), I32)], 1)
    pick = rows_of((tiles, LANES)) == cols_of((tiles, LANES))
    column = jnp.sum(jnp.where(pick, wide.astype(F32), 0.0), 1, keepdims=True)
    key = jnp.concatenate([column + float(j) for j in range(SPAN)], 0)
    key = jnp.broadcast_to(key, (pairs, lanes))
    p, q = rows_of((pairs, lanes)), cols_of((pairs, lanes))
    key_row = jnp.sum(jnp.where(p == q, key, 0.0), 0, keepdims=True)
    key_row = jnp.where(q[:1] < pairs, key_row, 1.0e6)
    ahead = (key_row == key) & (q < p)
    rank = jnp.sum(jnp.where((key_row < key) | ahead, 1.0, 0.0), 1, keepdims=True)
    again = jnp.sum(jnp.where(ahead, 1.0, 0.0), 1, keepdims=True)
    here = rank == q.astype(F32)
    order = jnp.sum(jnp.where(here, p.astype(F32), 0.0), 0, keepdims=True)
    keep = jnp.sum(jnp.where(here & (again > 0), 1.0, 0.0), 0, keepdims=True)
    upto = jnp.sum(jnp.where(key <= q.astype(F32), 1.0, 0.0), 0, keepdims=True)
    some = jnp.sum(jnp.where(key == q.astype(F32), 1.0, 0.0), 0, keepdims=True)
    some = jnp.minimum(some, 1.0)
    last = jnp.maximum(upto - 1.0, 0.0)
    rows = jnp.concatenate([order, keep, last, some, jnp.zeros((4, lanes), F32)], 0)
    table_ref[...] = rows.astype(I32)


def kernel(
    n_pb, n_ga,
    n_ins, latent_in, *rest,
):
    ins, rest = rest[:n_ins], rest[n_ins:]
    outs, rest = rest[:3], rest[3:]
    held, rest = rest[:n_ins], rest[n_ins:]
    ready, rest = rest[:3], rest[3:]
    body(n_pb, n_ga, latent_in, ins, outs, held, ready, *rest)


def body(
    n_pb, n_ga, latent_in, ins, outs, held, ready,
    pts_ref, pos_ref, from_ref, upto_ref, pad_ref, w1_ref, w2_ref, w2t_ref, tablev_ref, table_ref,
    cots_ref, hid_ref, slope_ref, x_ref, spot_ref, parts_ref, sums_ref, feats_ref,
    near_ref, nearin_ref, far_ref, farin_ref, half_ref, own_ref, acc_ref,
    ar_ref, arin_ref, gaall_ref, fin_ref,
    in_sem, latent_sem, out_sem, table_sem, gsend, grecv, fsend, nsend, nrecv, rsend, rrecv, hsend, hrecv, asend, arecv, bsend, brecv, csend, crecv,
):
    offs_ref, offv_ref, win_ref, bin_ref, wout_ref, bout_ref, ids_ref, qp_ref, rel_ref, cot_ref = held[:10]
    gridv_ref, final_ref, more_ref = ready
    me, slab = lax.axis_index("pb"), lax.axis_index("ga")
    chips = n_pb // 2
    chip, core = me // 2, me % 2
    sibling = chip * 2 + 1 - core
    tiles = cot_ref.shape[1] // TILE
    channels, hid = cot_ref.shape[0], win_ref.shape[1]
    blocks = latent_in.shape[2] // LANES
    limit = blocks * n_pb - SPAN
    group = math.gcd(tiles, 4)

    def send(src, dst, ssem, rsem, where):
        return pltpu.make_async_remote_copy(
            src_ref=src, dst_ref=dst, send_sem=ssem, recv_sem=rsem, device_id=where, device_id_type=MESH
        )

    square = chips == 4 and blocks % 2 == 0
    if square:
        beside = chip + 1 - 2 * (chip % 2)
        above = lax.rem(chip + 2, 4)
        others = [beside, above, lax.rem(beside + 2, 4)]
    else:
        others = [lax.rem(chip + m, chips) for m in range(1, chips)]
    peers = [o * 2 + core for o in others]
    twins = [o * 2 + 1 - core for o in others]
    near_chips = others + [chip]
    half = blocks // 2

    barrier = pltpu.get_barrier_semaphore()
    mine = me * blocks
    latent_copies = [
        pltpu.make_async_copy(latent_in.at[0, :, pl.ds(b * LANES, LANES)], feats_ref.at[mine + b], latent_sem.at[b])
        for b in range(blocks)
    ]
    loads = [pltpu.make_async_copy(src, dst, in_sem.at[i]) for i, (src, dst) in enumerate(zip(ins, held))]
    for copy in latent_copies + loads:
        copy.start()
    for m in range(1, n_pb):
        pl.semaphore_signal(barrier, inc=1, device_id={"pb": lax.rem(me + m, n_pb)}, device_id_type=MESH)
    for m in range(1, n_ga):
        pl.semaphore_signal(barrier, inc=1, device_id={"ga": lax.rem(slab + m, n_ga)}, device_id_type=MESH)

    def feats_of(d):
        return feats_ref.at[pl.ds(d * blocks, blocks)]

    for copy in latent_copies:
        copy.wait()
    pl.semaphore_wait(barrier, n_pb - 1 + n_ga - 1)
    def half_of(d, h):
        return feats_ref.at[pl.ds(d * blocks + h * half, half)]

    def piece(d, h, ssem, to):
        return send(half_of(d, h), half_of(d, h), ssem, grecv.at[d, h], {"pb": to})

    out = []
    if square:
        for i in range(2):
            out.append(piece(me, 1 - i, gsend.at[1 + i], peers[0]))
            out.append(piece(me, i, gsend.at[3 + i], peers[1]))
    else:
        for i, to in enumerate(peers):
            out.append(send(feats_of(me), feats_of(me), gsend.at[1 + i], grecv.at[me, 0], {"pb": to}))
    out.append(send(feats_of(me), feats_of(me), gsend.at[0], grecv.at[me, 0], {"pb": sibling}))
    for copy in out:
        copy.start()

    for copy in loads:
        copy.wait()
    pts_ref[...] = jnp.ones_like(pts_ref)
    pts_ref[0:3, :] = qp_ref[...]
    order_parts(tiles, limit, offv_ref, tablev_ref)
    weights(win_ref, bin_ref, wout_ref, bout_ref, pad_ref, w1_ref, w2_ref, w2t_ref)
    table_copy = pltpu.make_async_copy(tablev_ref, table_ref, table_sem)
    table_copy.start()

    lives = [jnp.where(ids_ref[:, t * TILE : (t + 1) * TILE] == slab, 1.0, 0.0) for t in range(tiles)]
    live = jnp.concatenate(lives, 0)
    rows = tiles * KN
    packed = live.astype(BF16)
    before = dot(packed, mask_of(rows_of((TILE, TILE)) < cols_of((TILE, TILE))))
    total = dot(packed, jnp.ones((TILE, TILE), BF16))
    r, c = rows_of((rows, rows)), cols_of((rows, rows))
    start = dot(mask_of((r // KN == c // KN) & (c < r)), total.astype(BF16))
    skip = (held[10][0] * CAP).astype(F32) if len(held) > 10 else 0.0
    pos_ref[...] = jnp.where(live > 0, before + start - skip, -1.0e6)
    from_ref[...] = start - skip
    upto_ref[...] = start + total - skip
    left = jnp.max(start + total - skip - float(CAP), axis=0, keepdims=True)
    left = jnp.max(left, axis=1, keepdims=True)

    def tile_base(t):
        return jnp.minimum(lax.shift_right_logical(offs_ref[0, t], 7), limit)

    def draw(t):
        cols = pl.ds(pl.multiple_of(t * TILE, TILE), TILE)
        lines = pl.ds(pl.multiple_of(t * KN, KN), KN)
        base = tile_base(t)
        pos = pos_ref[lines, :].astype(BF16)
        place = rows_of((CAP, TILE)).astype(F32).astype(BF16)
        pick = jnp.zeros((CAP, TILE), BF16)
        one = jnp.ones((CAP, TILE), BF16)
        for k in range(KN):
            pick = jnp.where(pos[k : k + 1, :] == place, one, pick)
        relp = rel_ref[:, cols] + (offs_ref[0, t] - base * LANES)
        low = (relp & (LANES - 1)).astype(F32)
        high = lax.shift_right_logical(relp, 7).astype(F32)
        points = pts_ref[:, cols]
        p_hi = points.astype(BF16).astype(F32)
        small = jnp.concatenate([p_hi, points - p_hi, low, high], 0).astype(BF16)
        data = jnp.concatenate([cot_ref[:, cols], small], 0)
        return dot_nt(data, pick)

    def place_inputs(t, drawn):
        lines = pl.ds(pl.multiple_of(t * KN, KN), KN)
        base = tile_base(t)
        head = drawn[channels : channels + 16]
        wide_from = jnp.concatenate([from_ref[lines, :]] * (CAP // TILE), 1)
        wide_upto = jnp.concatenate([upto_ref[lines, :]] * (CAP // TILE), 1)
        index = cols_of((KN, CAP)).astype(F32)
        which = (index >= wide_from) & (index < wide_upto)
        lo = jnp.sum(jnp.where(which, drawn[channels + 16 : channels + 24], 0.0), 0, keepdims=True)
        hi = jnp.sum(jnp.where(which, drawn[channels + 24 : channels + 32], 0.0), 0, keepdims=True)
        lo = jnp.broadcast_to(lo, (8, CAP))
        hi = jnp.broadcast_to(hi, (8, CAP))
        cell = (base + hi.astype(I32)) * LANES + lo.astype(I32)
        row = rows_of((8, CAP))
        along = jnp.where(
            row == 0,
            lax.shift_right_logical(cell, int(math.log2(GX * ZS))),
            jnp.where(
                row == 1,
                lax.shift_right_logical(cell, int(math.log2(ZS))) & (GX - 1),
                (cell & (ZS - 1)) + slab * ZS,
            ),
        )
        centre = jnp.where(row < 3, (along.astype(F32) + 0.5) / GX, 0.0)
        x = jnp.concatenate([head, centre, head[:8], centre, jnp.zeros((8, CAP), F32)], 0).astype(BF16)
        return x, lo, hi

    def lane_onehot(lo):
        row = jnp.broadcast_to(lo[:1], (LANES, CAP)).astype(BF16)
        return jnp.where(
            rows_of((LANES, CAP)).astype(F32).astype(BF16) == row, jnp.ones((LANES, CAP), BF16), jnp.zeros((LANES, CAP), BF16)
        )

    def spread(hi, grad):
        full = jnp.concatenate([hi, hi], 0)
        pieces = []
        for j in range(SPAN):
            on = jnp.where(full == float(j), 1.0, 0.0).astype(BF16)
            pieces.append(grad * jnp.concatenate([on] * (channels // 16), 0))
        return jnp.concatenate(pieces, 0)

    def first(i, carry):
        ts = [i * group + u for u in range(group)]
        drawn = [draw(t) for t in ts]
        placed = [place_inputs(t, d) for t, d in zip(ts, drawn)]
        cots = [d[:channels].astype(BF16) for d in drawn]
        pres = [dot(w1_ref[:, :XR], x) for x, _, _ in placed]
        kerns = []
        for t, pre, cot, (x, lo, hi) in zip(ts, pres, cots, placed):
            hidden, slope = gelu_parts(pre)
            hidden = hidden.astype(BF16)
            kerns.append(dot(w2_ref[...], jnp.concatenate([hidden, x], 0)))
            hid_ref[t] = hidden
            slope_ref[t] = slope
            cots_ref[t] = cot
            x_ref[t] = x
            spot_ref[t] = jnp.where(rows_of((8, CAP)) < 4, lo, hi)
        parts = []
        for kern, cot, (x, lo, hi) in zip(kerns, cots, placed):
            grad = (kern * cot.astype(F32)).astype(BF16)
            parts.append(dot_nt(spread(hi, grad), lane_onehot(lo)))
        for t, part in zip(ts, parts):
            for j in range(SPAN):
                parts_ref[j * tiles + t] = part[j * channels : (j + 1) * channels]
        return carry

    steps = tiles // group
    middle = steps // 2
    lax.fori_loop(0, middle, first, 0)
    forwards = []
    if square:
        piece(peers[0], 1, gsend.at[0], peers[0]).wait_recv()
        forwards.append(piece(peers[0], 1, hsend.at[2], peers[1]))
        piece(peers[1], 0, gsend.at[0], peers[1]).wait_recv()
        forwards.append(piece(peers[1], 0, hsend.at[3], peers[0]))
        for copy in forwards:
            copy.start()
    lax.fori_loop(middle, steps, first, 0)

    table_copy.wait()

    def pair_at(line, b):
        return jnp.clip(table_ref[line, b], 0, SPAN * tiles - 1)

    def run(i, acc):
        for u in range(group):
            at = i * group + u
            acc = acc * table_ref[1, at].astype(F32) + parts_ref[pair_at(0, at)]
            sums_ref[at] = acc
        return acc

    lax.fori_loop(0, SPAN * tiles // group, run, jnp.zeros((channels, LANES), F32))

    def block(b):
        return sums_ref[pair_at(2, b)] * table_ref[3, b].astype(F32)

    def near_copy(i):
        return send(near_ref.at[i], nearin_ref.at[i], nsend.at[i], nrecv.at[i], {"pb": sibling})

    def pass_on(i):
        d = peers[i]
        copy = send(feats_of(d), feats_of(d), fsend.at[i], grecv.at[d, 0], {"pb": sibling})
        copy.start()
        forwards.append(copy)

    pair = math.gcd(blocks, 4)
    order = list(range(chips - 2, -1, -1)) + [chips - 1]
    if square:
        piece(peers[0], 0, gsend.at[0], peers[0]).wait_recv()
        pass_on(0)
        piece(peers[1], 1, gsend.at[0], peers[1]).wait_recv()
        pass_on(1)
    for n, i in enumerate(order):
        owner = near_chips[i] * 2 + 1 - core

        def fill(b, carry, i=i, owner=owner):
            for u in range(pair):
                near_ref[i, b * pair + u] = block(owner * blocks + b * pair + u).astype(BF16)
            return carry

        lax.fori_loop(0, blocks // pair, fill, 0)
        if n > 0:
            near_copy(order[n - 1]).start()
    if square:
        piece(peers[2], 0, gsend.at[0], peers[2]).wait_recv()
        near_copy(order[-1]).start()
        piece(peers[2], 1, gsend.at[0], peers[2]).wait_recv()
        pass_on(2)
    else:
        for i, d in enumerate(peers):
            send(feats_of(d), feats_of(d), gsend.at[0], grecv.at[d, 0], {"pb": d}).wait_recv()
            pass_on(i)
        near_copy(order[-1]).start()

    if square:
        early = [(2, 0, 0, half_ref.at[0], 0), (2, 1, 1, half_ref.at[1], 1)]
        early += [(0, 0, 0, farin_ref.at[0, pl.ds(0, half)], 2), (1, 1, 1, farin_ref.at[1, pl.ds(half, half)], 5)]
        late = [(0, 1, 0, farin_ref.at[0, pl.ds(half, half)], 3), (1, 0, 1, farin_ref.at[1, pl.ds(0, half)], 4)]

        def far_half(slot, h, to, dst, n):
            return send(far_ref.at[slot, pl.ds(h * half, half)], dst, hsend.at[4 + n], hrecv.at[n], {"pb": peers[to]})

        early = [far_half(*e) for e in early]
        late = [far_half(*e) for e in late]
        slots = [(early[0], early[1]), (early[2],), (early[3],)]
    else:
        fars = [
            send(far_ref.at[i], farin_ref.at[i], rsend.at[i], rrecv.at[i], {"pb": to}) for i, to in enumerate(peers)
        ]
        slots = [(fars[i],) for i in order[:-1]]
    if square:
        order = [2, 0, 1, 3]
    for n, i in enumerate(order):
        owner = near_chips[i] * 2 + core
        near_copy(i).wait_recv()

        def join(b, carry, i=i, owner=owner):
            for u in range(pair):
                at = b * pair + u
                value = block(owner * blocks + at) + nearin_ref[i, at].astype(F32)
                if i < chips - 1:
                    far_ref[i, at] = value.astype(BF16)
                else:
                    own_ref[at] = value
            return carry

        lax.fori_loop(0, blocks // pair, join, 0)
        if n > 0:
            for copy in slots[n - 1]:
                copy.start()

    for d in twins + [sibling]:
        send(feats_of(d), feats_of(d), gsend.at[0], grecv.at[d, 0], {"pb": sibling}).wait_recv()

    acc_ref[...] = jnp.zeros_like(acc_ref)

    def draw_feats(t):
        window = feats_ref[pl.ds(tile_base(t), SPAN)].reshape(SPAN * channels, LANES)
        return dot(window, lane_onehot(spot_ref[t]))

    def feats_grad(t, drawn):
        tall = jnp.broadcast_to(spot_ref[t][4:5], (channels, CAP))
        feats = drawn[:channels]
        for j in range(1, SPAN):
            feats = jnp.where(tall == float(j), drawn[j * channels : (j + 1) * channels], feats)
        return (feats * cots_ref[t].astype(F32)).astype(BF16)

    def second(i, carry):
        ts = [i * group + u for u in range(group)]
        drawn = [draw_feats(t) for t in ts]
        grads = [feats_grad(t, d) for t, d in zip(ts, drawn)]
        pres = [dot(w2t_ref[...], g) for g in grads]
        sums = []
        for t, g, p in zip(ts, grads, pres):
            both = jnp.concatenate([g, (p * slope_ref[t]).astype(BF16)], 0)
            sums.append(dot_nt(both, jnp.concatenate([hid_ref[t], x_ref[t]], 0)))
        acc_ref[...] += functools.reduce(lambda a, b: a + b, sums)
        return carry

    lax.fori_loop(0, tiles // group, second, 0)

    k, l = rows_of((LANES, LANES)), cols_of((LANES, LANES))

    def gathered(shift):
        a = (l - shift >= 0) & (l - shift < 4) & ((k == hid + l - shift) | ((k == hid + 8 + l - shift) & (l - shift < 3)))
        b = (l - shift >= 4) & (l - shift < 7) & (k == hid + 16 + l - shift - 4)
        return jnp.where(a | b, 1.0, 0.0)

    top = jnp.where(cols_of((channels, LANES)) < 112, acc_ref[:channels], 0.0)
    tail = hid - channels
    top += exact(acc_ref[channels : 2 * channels], gathered(112))
    rest = exact(acc_ref[2 * channels : 2 * channels + tail], gathered(120))
    flag = jnp.where(left > 0, 1.0, 0.0)
    corner = (rows_of((tail, LANES)) == 0) & (cols_of((tail, LANES)) == 119)
    rest = jnp.where(corner, flag, rest)
    top = jnp.concatenate([top[:tail] + rest, top[tail:]], 0)
    slices = channels // n_pb
    ar_ref[...] = top.reshape(n_pb, slices, LANES)
    arin_ref[pl.ds(me, 1)] = ar_ref[pl.ds(me, 1)]
    first_hop = []
    for m in range(1, n_pb):
        to = lax.rem(me + m, n_pb)
        copy = send(ar_ref.at[to], arin_ref.at[me], asend.at[m - 1], arecv.at[me], {"pb": to})
        copy.start()
        first_hop.append(copy)
    if square:
        for i, copy in enumerate(early[:2]):
            copy.wait_recv()
            into = far_ref.at[1 - i, pl.ds(i * half, half)]
            into[...] = (into[...].astype(F32) + half_ref[i].astype(F32)).astype(BF16)
    for m in range(1, n_pb):
        d = lax.rem(me + m, n_pb)
        send(ar_ref.at[d], arin_ref.at[d], asend.at[m - 1], arecv.at[d], {"pb": d}).wait_recv()
    gaall_ref[pl.ds(slab, 1)] = jnp.sum(arin_ref[...], 0, keepdims=True)
    if square:
        for copy in late:
            copy.start()
    second_hop = []
    for m in range(1, n_ga):
        to = lax.rem(slab + m, n_ga)
        copy = send(gaall_ref.at[slab], gaall_ref.at[slab], bsend.at[m - 1], brecv.at[slab], {"ga": to})
        copy.start()
        second_hop.append(copy)
    for m in range(1, n_ga):
        d = lax.rem(slab + m, n_ga)
        send(gaall_ref.at[d], gaall_ref.at[d], bsend.at[m - 1], brecv.at[d], {"ga": d}).wait_recv()
    fin_ref[pl.ds(me, 1)] = jnp.sum(gaall_ref[...], 0, keepdims=True)
    third_hop = []
    for m in range(1, n_pb):
        to = lax.rem(me + m, n_pb)
        copy = send(fin_ref.at[me], fin_ref.at[me], csend.at[m - 1], crecv.at[me], {"pb": to})
        copy.start()
        third_hop.append(copy)

    for copy in early[2:] + late if square else fars:
        copy.wait_recv()
    for b in range(blocks):
        value = own_ref[b]
        for i in range(2 if square else chips - 1):
            value += farin_ref[i, b].astype(F32)
        gridv_ref[0, :, b * LANES : (b + 1) * LANES] = value
    stores = [pltpu.make_async_copy(src, dst, out_sem.at[i]) for i, (src, dst) in enumerate(zip(ready, outs))]
    stores[0].start()

    for m in range(1, n_pb):
        d = lax.rem(me + m, n_pb)
        send(fin_ref.at[d], fin_ref.at[d], csend.at[m - 1], crecv.at[d], {"pb": d}).wait_recv()
    final = fin_ref[...].reshape(channels, LANES)
    final_ref[...] = final
    flags = jnp.where(cols_of((1, LANES)) == 119, final[0:1], 0.0)
    more_ref[0] = jnp.sum(flags).astype(I32)
    for copy in stores[1:]:
        copy.start()
    for copy in stores:
        copy.wait()
    for copy in out + forwards + first_hop + second_hop + third_hop:
        copy.wait_send()
    for i in range(chips):
        near_copy(i).wait_send()
    for copy in early + late if square else fars:
        copy.wait_send()


def call(step, collective_id, query_points, cotangent, slab_ids, rel_cells, offsets, latent, w_in, b_in, w_out, b_out):
    n_pb, n_ga = lax.axis_size("pb"), lax.axis_size("ga")
    channels, owned = latent.shape[1], latent.shape[2]
    hid = w_in.shape[0]
    queries = query_points.shape[1]
    tiles = queries // TILE
    chips = n_pb // 2
    blocks = owned // LANES
    pairs = SPAN * tiles
    lanes = -(-pairs // LANES) * LANES
    hbm = pl.BlockSpec(memory_space=pltpu.HBM)
    dma = pltpu.SemaphoreType.DMA
    slices = channels // n_pb
    ins = (offsets, offsets, w_in.T, b_in[None], w_out, b_out[None], slab_ids, query_points, rel_cells, cotangent)
    ins += () if step is None else (step,)
    outs = [
        ((1, channels, owned), F32),
        ((channels, LANES), F32),
        ((1,), I32),
    ]
    return pl.pallas_call(
        functools.partial(kernel, n_pb, n_ga, len(ins)),
        out_shape=[jax.ShapeDtypeStruct(*o) for o in outs],
        in_specs=[hbm] * (1 + len(ins)),
        out_specs=[hbm] * len(outs),
        scratch_shapes=[(pltpu.SMEM if i in (0, 10) else pltpu.VMEM)(a.shape, a.dtype) for i, a in enumerate(ins)]
        + [pltpu.VMEM(*outs[0]), pltpu.VMEM(*outs[1]), pltpu.SMEM(*outs[2])]
        + [
            pltpu.VMEM((8, queries), F32),
            pltpu.VMEM((tiles * KN, TILE), F32),
            pltpu.VMEM((tiles * KN, TILE), F32),
            pltpu.VMEM((tiles * KN, TILE), F32),
            pltpu.VMEM((LANES, LANES), F32),
            pltpu.VMEM((hid, LANES), BF16),
            pltpu.VMEM((channels, LANES), BF16),
            pltpu.VMEM((hid, channels), BF16),
            pltpu.VMEM((8, lanes), I32),
            pltpu.SMEM((8, lanes), I32),
            pltpu.VMEM((tiles, channels, CAP), BF16),
            pltpu.VMEM((tiles, hid, CAP), BF16),
            pltpu.VMEM((tiles, hid, CAP), F32),
            pltpu.VMEM((tiles, XR, CAP), BF16),
            pltpu.VMEM((tiles, 8, CAP), F32),
            pltpu.VMEM((pairs, channels, LANES), F32),
            pltpu.VMEM((pairs, channels, LANES), F32),
            pltpu.VMEM((n_pb * blocks, channels, LANES), BF16),
            pltpu.VMEM((chips, blocks, channels, LANES), BF16),
            pltpu.VMEM((chips, blocks, channels, LANES), BF16),
            pltpu.VMEM((chips - 1, blocks, channels, LANES), BF16),
            pltpu.VMEM((chips - 1, blocks, channels, LANES), BF16),
            pltpu.VMEM((2, max(blocks // 2, 1), channels, LANES), BF16),
            pltpu.VMEM((blocks, channels, LANES), F32),
            pltpu.VMEM((channels + hid, LANES), F32),
            pltpu.VMEM((n_pb, slices, LANES), F32),
            pltpu.VMEM((n_pb, slices, LANES), F32),
            pltpu.VMEM((n_ga, slices, LANES), F32),
            pltpu.VMEM((n_pb, slices, LANES), F32),
            dma((len(ins),)),
            dma((blocks,)),
            dma((len(outs),)),
            dma,
            dma((max(chips + 1, 5),)),
            dma((n_pb, 2)),
            dma((chips,)),
            dma((chips,)),
            dma((chips,)),
            dma((chips,)),
            dma((chips,)),
            dma((10,)),
            dma((6,)),
            dma((n_pb,)),
            dma((n_pb,)),
            dma((n_ga,)),
            dma((n_ga,)),
            dma((n_pb,)),
            dma((n_pb,)),
        ],
        compiler_params=pltpu.CompilerParams(
            vmem_limit_bytes=67043328, collective_id=collective_id, has_side_effects=True
        ),
        name="whole",
    )(latent, *ins)


def settle(scale, grid_in, final_in, grid_ref, *rest):
    smalls, (final_ref, hold_ref), ready = rest[:4], rest[4:6], rest[6:10]
    load_sem, in_sem, out_sem, small_sem = rest[10:]
    gwin_ref, gbin_ref, gwout_ref, gbout_ref = ready
    load = pltpu.make_async_copy(final_in, final_ref, load_sem)
    load.start()
    parts = out_sem.shape[0]
    wide = grid_ref.shape[2] // parts
    arrive, leave = [], []
    for i in range(parts):
        at = (0, slice(None), pl.ds(i * wide, wide))
        arrive.append(pltpu.make_async_copy(grid_in.at[at], hold_ref.at[at], in_sem.at[i]))
        leave.append(pltpu.make_async_copy(hold_ref.at[at], grid_ref.at[at], out_sem.at[i]))
        arrive[-1].start()
    load.wait()
    channels, hid = gwout_ref.shape
    final = final_ref[...]
    k, l = rows_of((LANES, LANES)), cols_of((LANES, LANES))

    def chosen(shift):
        along = (l < 3) & (k == shift + l)
        cells = (l >= 3) & (l < 6) & (k == shift + 1 + l)
        return jnp.where(along | cells | ((l == 6) & (k == shift + 3)), scale, 0.0)

    gwout_ref[...] = final[:, :hid] * scale
    taken = jnp.concatenate([exact(final, chosen(112)), exact(final[: hid - channels], chosen(120))], 0)
    turned = exact_nt(jnp.where(rows_of((8, LANES)) == cols_of((8, LANES)), 1.0, 0.0), taken)
    gwin_ref[...] = turned[: gwin_ref.shape[0]]
    gbin_ref[...] = turned[6:7]
    gbout_ref[...] = exact_nt(jnp.where(cols_of((8, LANES)) == hid + 3, scale, 0.0), final)[0:1]
    for i in range(parts):
        arrive[i].wait()
        leave[i].start()
    stores = [pltpu.make_async_copy(src, dst, small_sem.at[i]) for i, (src, dst) in enumerate(zip(ready, smalls))]
    for copy in stores:
        copy.start()
    for copy in leave + stores:
        copy.wait()


def shards(*args):
    def again(state):
        step, _, sums = state
        grid, final, more = call(step, 1, *args)
        return step + 1, more, (sums[0] + grid, sums[1] + final)

    grid, final, more = call(None, 0, *args)
    first = (jnp.ones((1,), I32), more, (grid, final))
    grid, final = lax.while_loop(lambda state: state[1][0] > 0, again, first)[2]
    hid, channels = args[6].shape[0], args[8].shape[0]
    queries = args[0].shape[1] * lax.axis_size("pb")
    hbm = pl.BlockSpec(memory_space=pltpu.HBM)
    dma = pltpu.SemaphoreType.DMA
    parts = math.gcd(grid.shape[2] // LANES, 4)
    shapes = [args[6].shape[::-1], (1, hid), (channels, hid), (1, channels)]
    grid, gwin, gbin, gwout, gbout = pl.pallas_call(
        functools.partial(settle, float(queries) ** (-0.5)),
        out_shape=[jax.ShapeDtypeStruct(v, F32) for v in [grid.shape] + shapes],
        in_specs=[hbm] * 2,
        out_specs=[hbm] * 5,
        scratch_shapes=[pltpu.VMEM(v, F32) for v in [final.shape, grid.shape] + shapes]
        + [dma, dma((parts,)), dma((parts,)), dma((4,))],
        name="settle",
    )(grid, final)
    return grid, gwin.T, gbin[0], gwout, gbout[0]


def solution(mesh):
    return jax.shard_map(
        shards,
        mesh=mesh,
        in_specs=(
            P(None, "pb"),
            P(None, "pb"),
            P(None, "pb"),
            P(None, "pb"),
            P("ga", "pb"),
            P("ga", None, "pb"),
            P(),
            P(),
            P(),
            P(),
        ),
        out_specs=(P("ga", None, "pb"), P(), P(), P(), P()),
        check_vma=False,
    )
```

```python
import functools
import math

import jax
import jax.numpy as jnp
from jax import lax
from jax.experimental import pallas as pl
from jax.experimental.pallas import tpu as pltpu
from jax.sharding import PartitionSpec as P

KN = 8
TILE = 128
WIN = 512
GX = 64
ZS = 4
LANES = 128
SPAN = WIN // LANES + 1
CAP = 256
XR = 48
F32 = jnp.float32
BF16 = jnp.bfloat16
I32 = jnp.int32
MESH = pl.DeviceIdType.MESH
HIGHEST = lax.Precision.HIGHEST


def dot(a, b):
    return jnp.dot(a, b, preferred_element_type=F32)


def dot_nt(a, b):
    return lax.dot_general(a, b, (((1,), (1,)), ((), ())), preferred_element_type=F32)


def exact(a, b):
    return jnp.dot(a, b, preferred_element_type=F32, precision=HIGHEST)


def exact_nt(a, b):
    return lax.dot_general(a, b, (((1,), (1,)), ((), ())), preferred_element_type=F32, precision=HIGHEST)


def rows_of(shape):
    return lax.broadcasted_iota(I32, shape, 0)


def cols_of(shape):
    return lax.broadcasted_iota(I32, shape, 1)


def gelu_parts(x):
    z = jnp.abs(x) * (2.0**-0.5)
    t = 1.0 / (1.0 + 0.3275911 * z)
    e = jnp.exp(-0.5 * x * x)
    poly = ((((1.061405429 * t - 1.453152027) * t + 1.421413741) * t - 0.284496736) * t + 0.254829592) * t
    tail = 0.5 * poly * e
    cdf = jnp.where(x < 0, tail, 1.0 - tail)
    return x * cdf, cdf + x * e * ((2.0 * math.pi) ** -0.5)


def mask_of(cond):
    return jnp.where(cond, 1.0, 0.0).astype(BF16)


def split3(v):
    a = v.astype(BF16)
    r = v - a.astype(F32)
    b = r.astype(BF16)
    return a, b, (r - b.astype(F32)).astype(BF16)


def weights(win_ref, bin_ref, wout_ref, bout_ref, pad_ref, w1_ref, w2_ref, w2t_ref):
    hid, channels = win_ref.shape[1], wout_ref.shape[0]
    pad_ref[...] = jnp.zeros_like(pad_ref)
    pad_ref[: win_ref.shape[0], :hid] = win_ref[...]
    wide = pad_ref[...].T[:hid]
    w_hi = wide.astype(BF16)
    w_lo = (wide - w_hi.astype(F32)).astype(BF16)
    k, col = rows_of((LANES, LANES)), cols_of((LANES, LANES))
    s_hi = mask_of(((k < 3) & ((col == k) | (col == k + 8))) | ((k >= 3) & (k < 6) & (col == k + 13)))
    s_lo = mask_of(((k < 3) & (col == k + 24)) | ((k >= 3) & (k < 6) & (col == k + 29)))
    w1 = dot(w_hi, s_hi) + dot(w_lo, s_lo)
    pad_ref[0:1, :hid] = bin_ref[...]
    pad_ref[0:1, hid:] = jnp.zeros((1, LANES - hid), F32)
    diag = jnp.where(rows_of((hid, LANES)) == cols_of((hid, LANES)), pad_ref[0:1, :], 0.0)
    for i, part in enumerate(split3(diag)):
        w1 += dot(part, mask_of(col == 3 + i))
    w1_ref[...] = w1.astype(BF16)

    pad_ref[0:channels, :hid] = wout_ref[...].astype(F32)
    pad_ref[0:channels, hid:] = jnp.zeros((channels, LANES - hid), F32)
    w_out = pad_ref[0:channels, :].astype(BF16)
    w2 = dot(w_out, mask_of(k == col))
    eye = mask_of(rows_of((hid, LANES)) == cols_of((hid, LANES)))
    w2t_ref[...] = dot_nt(eye, w_out).astype(BF16)
    pad_ref[0:1, :channels] = bout_ref[...]
    diag = jnp.where(rows_of((channels, LANES)) == cols_of((channels, LANES)), pad_ref[0:1, :], 0.0)
    for i, part in enumerate(split3(diag)):
        w2 += dot(part, mask_of(col == hid + 3 + i))
    w2_ref[...] = w2.astype(BF16)


def order_parts(tiles, limit, offv_ref, table_ref):
    pairs = SPAN * tiles
    lanes = -(-pairs // LANES) * LANES
    base_row = jnp.minimum(lax.shift_right_logical(offv_ref[...], 7), limit)
    wide = jnp.concatenate([base_row, jnp.zeros((1, LANES - tiles), I32)], 1)
    pick = rows_of((tiles, LANES)) == cols_of((tiles, LANES))
    column = jnp.sum(jnp.where(pick, wide.astype(F32), 0.0), 1, keepdims=True)
    key = jnp.concatenate([column + float(j) for j in range(SPAN)], 0)
    key = jnp.broadcast_to(key, (pairs, lanes))
    p, q = rows_of((pairs, lanes)), cols_of((pairs, lanes))
    key_row = jnp.sum(jnp.where(p == q, key, 0.0), 0, keepdims=True)
    key_row = jnp.where(q[:1] < pairs, key_row, 1.0e6)
    ahead = (key_row == key) & (q < p)
    rank = jnp.sum(jnp.where((key_row < key) | ahead, 1.0, 0.0), 1, keepdims=True)
    again = jnp.sum(jnp.where(ahead, 1.0, 0.0), 1, keepdims=True)
    here = rank == q.astype(F32)
    order = jnp.sum(jnp.where(here, p.astype(F32), 0.0), 0, keepdims=True)
    keep = jnp.sum(jnp.where(here & (again > 0), 1.0, 0.0), 0, keepdims=True)
    upto = jnp.sum(jnp.where(key <= q.astype(F32), 1.0, 0.0), 0, keepdims=True)
    some = jnp.sum(jnp.where(key == q.astype(F32), 1.0, 0.0), 0, keepdims=True)
    some = jnp.minimum(some, 1.0)
    last = jnp.maximum(upto - 1.0, 0.0)
    rows = jnp.concatenate([order, keep, last, some, jnp.zeros((4, lanes), F32)], 0)
    table_ref[...] = rows.astype(I32)


def kernel(
    n_pb, n_ga,
    n_ins, latent_in, *rest,
):
    ins, rest = rest[:n_ins], rest[n_ins:]
    outs, rest = rest[:3], rest[3:]
    held, rest = rest[:n_ins], rest[n_ins:]
    body(n_pb, n_ga, latent_in, ins, outs, held, *rest)


def body(
    n_pb, n_ga, latent_in, ins, outs, held, more_ref,
    pts_ref, pos_ref, from_ref, upto_ref, pad_ref, w1_ref, w2_ref, w2t_ref, tablev_ref, table_ref,
    cots_ref, hid_ref, slope_ref, x_ref, spot_ref, parts_ref, sums_ref, feats_ref,
    near_ref, nearin_ref, far_ref, farin_ref, half_ref, own_ref, acc_ref,
    ar_ref, arin_ref, gaall_ref, fin_ref,
    in_sem, latent_sem, out_sem, table_sem, gsend, grecv, fsend, frecv, nsend, nrecv, rsend, rrecv, hsend, hrecv, asend, arecv, bsend, brecv, csend, crecv,
):
    offs_ref, offv_ref, win_ref, bin_ref, wout_ref, bout_ref, ids_ref, qp_ref, rel_ref, cot_ref = held[:10]
    grid_ref, final_ref, more_out = outs
    me, slab = lax.axis_index("pb"), lax.axis_index("ga")
    chips = n_pb // 2
    chip, core = me // 2, me % 2
    sibling = chip * 2 + 1 - core
    tiles = cot_ref.shape[1] // TILE
    channels, hid = cot_ref.shape[0], win_ref.shape[1]
    blocks = latent_in.shape[2] // LANES
    limit = blocks * n_pb - SPAN
    group = math.gcd(tiles, 4)

    def send(src, dst, ssem, rsem, where):
        return pltpu.make_async_remote_copy(
            src_ref=src, dst_ref=dst, send_sem=ssem, recv_sem=rsem, device_id=where, device_id_type=MESH
        )

    square = chips == 4 and blocks % 2 == 0
    if square:
        beside = chip + 1 - 2 * (chip % 2)
        above = lax.rem(chip + 2, 4)
        others = [beside, above, lax.rem(beside + 2, 4)]
    else:
        others = [lax.rem(chip + m, chips) for m in range(1, chips)]
    peers = [o * 2 + core for o in others]
    near_chips = others + [chip]
    half = blocks // 2

    barrier = pltpu.get_barrier_semaphore()
    mine = me * blocks
    latent_copies = [
        pltpu.make_async_copy(latent_in.at[0, :, pl.ds(b * LANES, LANES)], feats_ref.at[mine + b], latent_sem)
        for b in range(blocks)
    ]
    loads = [pltpu.make_async_copy(src, dst, in_sem.at[i]) for i, (src, dst) in enumerate(zip(ins, held))]
    for copy in latent_copies + loads:
        copy.start()
    for m in range(1, n_pb):
        pl.semaphore_signal(barrier, inc=1, device_id={"pb": lax.rem(me + m, n_pb)}, device_id_type=MESH)
    for m in range(1, n_ga):
        pl.semaphore_signal(barrier, inc=1, device_id={"ga": lax.rem(slab + m, n_ga)}, device_id_type=MESH)

    def feats_of(d):
        return feats_ref.at[pl.ds(d * blocks, blocks)]

    pltpu.make_async_copy(feats_of(me), feats_of(me), latent_sem).wait()
    pl.semaphore_wait(barrier, n_pb - 1 + n_ga - 1)
    def half_of(d, h):
        return feats_ref.at[pl.ds(d * blocks + h * half, half)]

    def piece(slot, d, h, ssem, to):
        return send(half_of(d, h), half_of(d, h), ssem, grecv.at[slot, h], {"pb": to})

    out = []
    if square:
        for i in range(2):
            out.append(piece(0, me, 1 - i, gsend, peers[0]))
            out.append(piece(1, me, i, gsend, peers[1]))
    else:
        for i, to in enumerate(peers):
            out.append(send(feats_of(me), feats_of(me), gsend, grecv.at[i, 0], {"pb": to}))
    out.append(send(feats_of(me), feats_of(me), gsend, frecv, {"pb": sibling}))
    for copy in out:
        copy.start()

    for copy in loads:
        copy.wait()
    pts_ref[...] = jnp.ones_like(pts_ref)
    pts_ref[0:3, :] = qp_ref[...]
    order_parts(tiles, limit, offv_ref, tablev_ref)
    weights(win_ref, bin_ref, wout_ref, bout_ref, pad_ref, w1_ref, w2_ref, w2t_ref)
    table_copy = pltpu.make_async_copy(tablev_ref, table_ref, table_sem)
    table_copy.start()

    lives = [jnp.where(ids_ref[:, t * TILE : (t + 1) * TILE] == slab, 1.0, 0.0) for t in range(tiles)]
    live = jnp.concatenate(lives, 0)
    rows = tiles * KN
    packed = live.astype(BF16)
    before = dot(packed, mask_of(rows_of((TILE, TILE)) < cols_of((TILE, TILE))))
    total = dot(packed, jnp.ones((TILE, TILE), BF16))
    r, c = rows_of((rows, rows)), cols_of((rows, rows))
    start = dot(mask_of((r // KN == c // KN) & (c < r)), total.astype(BF16))
    skip = (held[10][0] * CAP).astype(F32) if len(held) > 10 else 0.0
    pos_ref[...] = jnp.where(live > 0, before + start - skip, -1.0e6)
    from_ref[...] = start - skip
    upto_ref[...] = start + total - skip
    left = jnp.max(start + total - skip - float(CAP), axis=0, keepdims=True)
    left = jnp.max(left, axis=1, keepdims=True)

    def tile_base(t):
        return jnp.minimum(lax.shift_right_logical(offs_ref[0, t], 7), limit)

    def draw(t):
        cols = pl.ds(pl.multiple_of(t * TILE, TILE), TILE)
        lines = pl.ds(pl.multiple_of(t * KN, KN), KN)
        base = tile_base(t)
        pos = pos_ref[lines, :].astype(BF16)
        place = rows_of((CAP, TILE)).astype(F32).astype(BF16)
        pick = jnp.zeros((CAP, TILE), BF16)
        one = jnp.ones((CAP, TILE), BF16)
        for k in range(KN):
            pick = jnp.where(pos[k : k + 1, :] == place, one, pick)
        relp = rel_ref[:, cols] + (offs_ref[0, t] - base * LANES)
        low = (relp & (LANES - 1)).astype(F32)
        high = lax.shift_right_logical(relp, 7).astype(F32)
        points = pts_ref[:, cols]
        p_hi = points.astype(BF16).astype(F32)
        small = jnp.concatenate([p_hi, points - p_hi, low, high], 0).astype(BF16)
        data = jnp.concatenate([cot_ref[:, cols], small], 0)
        return dot_nt(data, pick)

    def place_inputs(t, drawn):
        lines = pl.ds(pl.multiple_of(t * KN, KN), KN)
        base = tile_base(t)
        head = drawn[channels : channels + 16]
        wide_from = jnp.concatenate([from_ref[lines, :]] * (CAP // TILE), 1)
        wide_upto = jnp.concatenate([upto_ref[lines, :]] * (CAP // TILE), 1)
        index = cols_of((KN, CAP)).astype(F32)
        which = (index >= wide_from) & (index < wide_upto)
        lo = jnp.sum(jnp.where(which, drawn[channels + 16 : channels + 24], 0.0), 0, keepdims=True)
        hi = jnp.sum(jnp.where(which, drawn[channels + 24 : channels + 32], 0.0), 0, keepdims=True)
        lo = jnp.broadcast_to(lo, (8, CAP))
        hi = jnp.broadcast_to(hi, (8, CAP))
        cell = (base + hi.astype(I32)) * LANES + lo.astype(I32)
        row = rows_of((8, CAP))
        along = jnp.where(
            row == 0,
            lax.shift_right_logical(cell, int(math.log2(GX * ZS))),
            jnp.where(
                row == 1,
                lax.shift_right_logical(cell, int(math.log2(ZS))) & (GX - 1),
                (cell & (ZS - 1)) + slab * ZS,
            ),
        )
        centre = jnp.where(row < 3, (along.astype(F32) + 0.5) / GX, 0.0)
        x = jnp.concatenate([head, centre, head[:8], centre, jnp.zeros((8, CAP), F32)], 0).astype(BF16)
        return x, lo, hi

    def lane_onehot(lo):
        row = jnp.broadcast_to(lo[:1], (LANES, CAP)).astype(BF16)
        return jnp.where(
            rows_of((LANES, CAP)).astype(F32).astype(BF16) == row, jnp.ones((LANES, CAP), BF16), jnp.zeros((LANES, CAP), BF16)
        )

    def spread(hi, grad):
        full = jnp.concatenate([hi, hi], 0)
        pieces = []
        for j in range(SPAN):
            on = jnp.where(full == float(j), 1.0, 0.0).astype(BF16)
            pieces.append(grad * jnp.concatenate([on] * (channels // 16), 0))
        return jnp.concatenate(pieces, 0)

    def first(i, carry):
        ts = [i * group + u for u in range(group)]
        drawn = [draw(t) for t in ts]
        placed = [place_inputs(t, d) for t, d in zip(ts, drawn)]
        cots = [d[:channels].astype(BF16) for d in drawn]
        pres = [dot(w1_ref[:, :XR], x) for x, _, _ in placed]
        kerns = []
        for t, pre, cot, (x, lo, hi) in zip(ts, pres, cots, placed):
            hidden, slope = gelu_parts(pre)
            hidden = hidden.astype(BF16)
            kerns.append(dot(w2_ref[...], jnp.concatenate([hidden, x], 0)))
            hid_ref[t] = hidden
            slope_ref[t] = slope
            cots_ref[t] = cot
            x_ref[t] = x
            spot_ref[t] = jnp.where(rows_of((8, CAP)) < 4, lo, hi)
        parts = []
        for kern, cot, (x, lo, hi) in zip(kerns, cots, placed):
            grad = (kern * cot.astype(F32)).astype(BF16)
            parts.append(dot_nt(spread(hi, grad), lane_onehot(lo)))
        for t, part in zip(ts, parts):
            for j in range(SPAN):
                parts_ref[j * tiles + t] = part[j * channels : (j + 1) * channels]
        return carry

    steps = tiles // group

    def pass_half(i, h):
        return send(half_of(peers[i], h), half_of(peers[i], h), fsend, frecv, {"pb": sibling})

    def come(i, h):
        piece(i, peers[i], h, gsend, peers[i]).wait_recv()

    middle, late_step, ahead = steps // 2, steps * 7 // 8, steps // 4
    lax.fori_loop(0, middle, first, 0)
    if square:
        come(0, 1)
        piece(2, peers[0], 1, hsend, peers[1]).start()
        come(1, 0)
        piece(2, peers[1], 0, hsend, peers[0]).start()
        pass_half(0, 1).start()
        pass_half(1, 0).start()
    lax.fori_loop(middle, late_step, first, 0)
    if square:
        for i in range(2):
            come(i, i)
            pass_half(i, i).start()
    lax.fori_loop(late_step, steps, first, 0)

    if square:
        for h in range(2):
            come(2, h)
            pass_half(2, h).start()
    table_copy.wait()

    def pair_at(line, b):
        return jnp.clip(table_ref[line, b], 0, SPAN * tiles - 1)

    def run(i, acc):
        for u in range(group):
            at = i * group + u
            acc = acc * table_ref[1, at].astype(F32) + parts_ref[pair_at(0, at)]
            sums_ref[at] = acc
        return acc

    lax.fori_loop(0, SPAN * tiles // group, run, jnp.zeros((channels, LANES), F32))

    def block(b):
        return sums_ref[pair_at(2, b)] * table_ref[3, b].astype(F32)

    def near_copy(i):
        return send(near_ref.at[i], nearin_ref.at[i], nsend, nrecv.at[i], {"pb": sibling})

    pair = math.gcd(blocks, 4)
    order = list(range(chips - 2, -1, -1)) + [chips - 1]
    for n, i in enumerate(order):
        owner = near_chips[i] * 2 + 1 - core

        def fill(b, carry, i=i, owner=owner):
            for u in range(pair):
                near_ref[i, b * pair + u] = block(owner * blocks + b * pair + u).astype(BF16)
            return carry

        lax.fori_loop(0, blocks // pair, fill, 0)
        if n > 0:
            near_copy(order[n - 1]).start()
    if not square:
        for i in range(chips - 1):
            d = lax.rem(chip + chips - 1 - i, chips) * 2 + core
            send(feats_of(d), feats_of(d), gsend, grecv.at[i, 0], {"pb": d}).wait_recv()
            send(feats_of(d), feats_of(d), fsend, frecv, {"pb": sibling}).start()

    all_twins = feats_ref.at[pl.ds(0, chips * blocks)]
    send(all_twins, all_twins, gsend, frecv, {"pb": sibling}).wait_recv()

    acc_ref[...] = jnp.zeros_like(acc_ref)

    def draw_feats(t):
        window = feats_ref[pl.ds(tile_base(t), SPAN)].reshape(SPAN * channels, LANES)
        return dot(window, lane_onehot(spot_ref[t]))

    def feats_grad(t, drawn):
        tall = jnp.broadcast_to(spot_ref[t][4:5], (channels, CAP))
        feats = drawn[:channels]
        for j in range(1, SPAN):
            feats = jnp.where(tall == float(j), drawn[j * channels : (j + 1) * channels], feats)
        return (feats * cots_ref[t].astype(F32)).astype(BF16)

    def second(i, carry):
        ts = [i * group + u for u in range(group)]
        drawn = [draw_feats(t) for t in ts]
        grads = [feats_grad(t, d) for t, d in zip(ts, drawn)]
        pres = [dot(w2t_ref[...], g) for g in grads]
        sums = []
        for t, g, p in zip(ts, grads, pres):
            both = jnp.concatenate([g, (p * slope_ref[t]).astype(BF16)], 0)
            sums.append(dot_nt(both, jnp.concatenate([hid_ref[t], x_ref[t]], 0)))
        acc_ref[...] += functools.reduce(lambda a, b: a + b, sums)
        return carry

    near_copy(order[-1]).start()
    lax.fori_loop(0, ahead, second, 0)
    if square:
        early = [(2, 0, 0, half_ref.at[0], 0), (2, 1, 1, half_ref.at[1], 1)]
        early += [(0, 0, 0, farin_ref.at[0, pl.ds(0, half)], 2), (1, 1, 1, farin_ref.at[1, pl.ds(half, half)], 2)]
        late = [(0, 1, 0, farin_ref.at[0, pl.ds(half, half)], 2), (1, 0, 1, farin_ref.at[1, pl.ds(0, half)], 2)]

        def far_half(slot, h, to, dst, n):
            return send(far_ref.at[slot, pl.ds(h * half, half)], dst, hsend, hrecv.at[n], {"pb": peers[to]})

        early = [far_half(*e) for e in early]
        late = [far_half(*e) for e in late]
        slots = [(early[0], early[1]), (early[2],), (early[3],)]
    else:
        fars = [
            send(far_ref.at[i], farin_ref.at[i], rsend.at[i], rrecv.at[i], {"pb": to}) for i, to in enumerate(peers)
        ]
        slots = [(fars[i],) for i in order[:-1]]
    if square:
        order = [2, 0, 1, 3]
    for n, i in enumerate(order):
        owner = near_chips[i] * 2 + core
        near_copy(i).wait_recv()

        def join(b, carry, i=i, owner=owner):
            for u in range(pair):
                at = b * pair + u
                value = block(owner * blocks + at) + nearin_ref[i, at].astype(F32)
                if i < chips - 1:
                    far_ref[i, at] = value.astype(BF16)
                else:
                    own_ref[at] = value
            return carry

        lax.fori_loop(0, blocks // pair, join, 0)
        if n > 0:
            for copy in slots[n - 1]:
                copy.start()

    lax.fori_loop(ahead, steps, second, 0)

    k, l = rows_of((LANES, LANES)), cols_of((LANES, LANES))

    def gathered(shift):
        a = (l - shift >= 0) & (l - shift < 4) & ((k == hid + l - shift) | ((k == hid + 8 + l - shift) & (l - shift < 3)))
        b = (l - shift >= 4) & (l - shift < 7) & (k == hid + 16 + l - shift - 4)
        return jnp.where(a | b, 1.0, 0.0)

    top = jnp.where(cols_of((channels, LANES)) < 112, acc_ref[:channels], 0.0)
    tail = hid - channels
    top += exact(acc_ref[channels : 2 * channels], gathered(112))
    rest = exact(acc_ref[2 * channels : 2 * channels + tail], gathered(120))
    flag = jnp.where(left > 0, 1.0, 0.0)
    slices = channels // n_pb
    top = jnp.concatenate([top[:tail] + rest, top[tail:]], 0)
    marked = (lax.rem(rows_of((channels, LANES)), slices) == 0) & (cols_of((channels, LANES)) == LANES - 1)
    top = jnp.where(marked, flag, top)
    ar_ref[...] = top.reshape(n_pb, slices, LANES)
    arin_ref[pl.ds(me, 1)] = ar_ref[pl.ds(me, 1)]
    for m in range(1, n_pb):
        to = lax.rem(me + m, n_pb)
        send(ar_ref.at[to], arin_ref.at[me], asend, arecv, {"pb": to}).start()
    if square:
        for i, copy in enumerate(early[:2]):
            copy.wait_recv()
            into = far_ref.at[1 - i, pl.ds(i * half, half)]
            into[...] = (into[...].astype(F32) + half_ref[i].astype(F32)).astype(BF16)
    most = pl.ds(0, n_pb - 1)
    all_in = send(ar_ref.at[most], arin_ref.at[most], asend, arecv, {"pb": sibling})
    all_in.wait_recv()
    gaall_ref[pl.ds(slab, 1)] = jnp.sum(arin_ref[...], 0, keepdims=True)
    for m in range(1, n_ga):
        to = lax.rem(slab + m, n_ga)
        send(gaall_ref.at[slab], gaall_ref.at[slab], bsend, brecv, {"ga": to}).start()
    if square:
        for copy in late:
            copy.start()
    less = gaall_ref.at[pl.ds(0, n_ga - 1)]
    all_slabs = send(less, less, bsend, brecv, {"pb": sibling})
    all_slabs.wait_recv()
    settled = jnp.sum(gaall_ref[...], 0, keepdims=True)
    fin_ref[pl.ds(me, 1)] = settled
    more_ref[0] = jnp.sum(jnp.where(cols_of((1, LANES)) == LANES - 1, settled[0, 0:1], 0.0)).astype(I32)
    for m in range(1, n_pb):
        to = lax.rem(me + m, n_pb)
        send(fin_ref.at[me], fin_ref.at[me], csend, crecv, {"pb": to}).start()
    tell = pltpu.make_async_copy(more_ref, more_out, out_sem)
    tell.start()

    if square:
        come_in = farin_ref.at[pl.ds(0, 2)]
        send(come_in, come_in, hsend, hrecv.at[2], {"pb": sibling}).wait_recv()
    else:
        for copy in fars:
            copy.wait_recv()
    for b in range(blocks):
        value = own_ref[b]
        for i in range(2 if square else chips - 1):
            value += farin_ref[i, b].astype(F32)
        grid_ref[0, :, b * LANES : (b + 1) * LANES] = value

    all_final = send(fin_ref.at[most], fin_ref.at[most], csend, crecv, {"pb": sibling})
    all_final.wait_recv()
    final = fin_ref[...].reshape(channels, LANES)
    final_ref[...] = final
    tell.wait()
    all_feats = feats_ref.at[pl.ds(0, (3 if square else chips) * blocks)]
    send(all_feats, all_feats, gsend, frecv, {"pb": sibling}).wait_send()
    passed = feats_ref.at[pl.ds(0, (chips - 1) * blocks)]
    send(passed, passed, fsend, frecv, {"pb": sibling}).wait_send()
    send(near_ref, nearin_ref, nsend, nrecv.at[0], {"pb": sibling}).wait_send()
    if square:
        send(all_twins, all_twins, hsend, frecv, {"pb": sibling}).wait_send()
    else:
        for copy in fars:
            copy.wait_send()
    for copy in (all_in, all_slabs, all_final):
        copy.wait_send()


def call(step, collective_id, query_points, cotangent, slab_ids, rel_cells, offsets, latent, w_in, b_in, w_out, b_out):
    n_pb, n_ga = lax.axis_size("pb"), lax.axis_size("ga")
    channels, owned = latent.shape[1], latent.shape[2]
    hid = w_in.shape[0]
    queries = query_points.shape[1]
    tiles = queries // TILE
    chips = n_pb // 2
    blocks = owned // LANES
    pairs = SPAN * tiles
    lanes = -(-pairs // LANES) * LANES
    hbm = pl.BlockSpec(memory_space=pltpu.HBM)
    vmem = pl.BlockSpec(memory_space=pltpu.VMEM)
    dma = pltpu.SemaphoreType.DMA
    slices = channels // n_pb
    ins = (offsets, offsets, w_in.T, b_in[None], w_out, b_out[None], slab_ids, query_points, rel_cells, cotangent)
    ins += () if step is None else (step,)
    outs = [
        ((1, channels, owned), F32),
        ((channels, LANES), F32),
        ((1,), I32),
    ]
    return pl.pallas_call(
        functools.partial(kernel, n_pb, n_ga, len(ins)),
        out_shape=[jax.ShapeDtypeStruct(*o) for o in outs],
        in_specs=[hbm] * (1 + len(ins)),
        out_specs=[vmem, vmem, hbm],
        scratch_shapes=[(pltpu.SMEM if i in (0, 10) else pltpu.VMEM)(a.shape, a.dtype) for i, a in enumerate(ins)]
        + [pltpu.SMEM(*outs[2])]
        + [
            pltpu.VMEM((8, queries), F32),
            pltpu.VMEM((tiles * KN, TILE), F32),
            pltpu.VMEM((tiles * KN, TILE), F32),
            pltpu.VMEM((tiles * KN, TILE), F32),
            pltpu.VMEM((LANES, LANES), F32),
            pltpu.VMEM((hid, LANES), BF16),
            pltpu.VMEM((channels, LANES), BF16),
            pltpu.VMEM((hid, channels), BF16),
            pltpu.VMEM((8, lanes), I32),
            pltpu.SMEM((8, lanes), I32),
            pltpu.VMEM((tiles, channels, CAP), BF16),
            pltpu.VMEM((tiles, hid, CAP), BF16),
            pltpu.VMEM((tiles, hid, CAP), F32),
            pltpu.VMEM((tiles, XR, CAP), BF16),
            pltpu.VMEM((tiles, 8, CAP), F32),
            pltpu.VMEM((pairs, channels, LANES), F32),
            pltpu.VMEM((pairs, channels, LANES), F32),
            pltpu.VMEM((n_pb * blocks, channels, LANES), BF16),
            pltpu.VMEM((chips, blocks, channels, LANES), BF16),
            pltpu.VMEM((chips, blocks, channels, LANES), BF16),
            pltpu.VMEM((chips - 1, blocks, channels, LANES), BF16),
            pltpu.VMEM((chips - 1, blocks, channels, LANES), BF16),
            pltpu.VMEM((2, max(blocks // 2, 1), channels, LANES), BF16),
            pltpu.VMEM((blocks, channels, LANES), F32),
            pltpu.VMEM((channels + hid, LANES), F32),
            pltpu.VMEM((n_pb, slices, LANES), F32),
            pltpu.VMEM((n_pb, slices, LANES), F32),
            pltpu.VMEM((n_ga, slices, LANES), F32),
            pltpu.VMEM((n_pb, slices, LANES), F32),
            dma((len(ins),)),
            dma,
            dma,
            dma,
            dma,
            dma((chips - 1, 2)),
            dma,
            dma,
            dma,
            dma((chips,)),
            dma((chips,)),
            dma((chips,)),
            dma,
            dma((3,)),
            dma,
            dma,
            dma,
            dma,
            dma,
            dma,
        ],
        compiler_params=pltpu.CompilerParams(
            vmem_limit_bytes=67043328 - 4 * channels * (owned + LANES) - 1024, collective_id=collective_id, has_side_effects=True
        ),
        name="whole",
    )(latent, *ins)


def settle(scale, grid_in, final_ref, grid_ref, *rest):
    smalls, ready = rest[:4], rest[4:8]
    grid_sem, small_sem = rest[8:]
    gwin_ref, gbin_ref, gwout_ref, gbout_ref = ready
    move = pltpu.make_async_copy(grid_in, grid_ref, grid_sem)
    move.start()
    channels, hid = gwout_ref.shape
    final = final_ref[...]
    k, l = rows_of((LANES, LANES)), cols_of((LANES, LANES))

    def chosen(shift):
        along = (l < 3) & (k == shift + l)
        cells = (l >= 3) & (l < 6) & (k == shift + 1 + l)
        return jnp.where(along | cells | ((l == 6) & (k == shift + 3)), scale, 0.0)

    gwout_ref[...] = final[:, :hid] * scale
    taken = jnp.concatenate([exact(final, chosen(112)), exact(final[: hid - channels], chosen(120))], 0)
    turned = exact_nt(jnp.where(rows_of((8, LANES)) == cols_of((8, LANES)), 1.0, 0.0), taken)
    gwin_ref[...] = turned[: gwin_ref.shape[0]]
    gbin_ref[...] = turned[6:7]
    gbout_ref[...] = exact_nt(jnp.where(cols_of((8, LANES)) == hid + 3, scale, 0.0), final)[0:1]
    stores = [pltpu.make_async_copy(src, dst, small_sem.at[i]) for i, (src, dst) in enumerate(zip(ready, smalls))]
    for copy in stores:
        copy.start()
    for copy in stores:
        copy.wait()
    move.wait()


def shards(*args):
    def again(state):
        step, _, sums = state
        grid, final, more = call(step, 1, *args)
        return step + 1, more, (sums[0] + grid, sums[1] + final)

    grid, final, more = call(None, 0, *args)
    first = (jnp.ones((1,), I32), more, (grid, final))
    grid, final = lax.while_loop(lambda state: state[1][0] > 0, again, first)[2]
    hid, channels = args[6].shape[0], args[8].shape[0]
    queries = args[0].shape[1] * lax.axis_size("pb")
    hbm = pl.BlockSpec(memory_space=pltpu.HBM)
    dma = pltpu.SemaphoreType.DMA
    shapes = [args[6].shape[::-1], (1, hid), (channels, hid), (1, channels)]
    grid, gwin, gbin, gwout, gbout = pl.pallas_call(
        functools.partial(settle, float(queries) ** (-0.5)),
        out_shape=[jax.ShapeDtypeStruct(v, F32) for v in [grid.shape] + shapes],
        in_specs=[hbm, pl.BlockSpec(memory_space=pltpu.VMEM)],
        out_specs=[hbm] * 5,
        scratch_shapes=[pltpu.VMEM(v, F32) for v in shapes] + [dma, dma((4,))],
        name="settle",
    )(grid, final)
    return grid, gwin.T, gbin[0], gwout, gbout[0]


def solution(mesh):
    return jax.shard_map(
        shards,
        mesh=mesh,
        in_specs=(
            P(None, "pb"),
            P(None, "pb"),
            P(None, "pb"),
            P(None, "pb"),
            P("ga", "pb"),
            P("ga", None, "pb"),
            P(),
            P(),
            P(),
            P(),
        ),
        out_specs=(P("ga", None, "pb"), P(), P(), P(), P()),
        check_vma=False,
    )
```

```python
import functools
import math

import jax
import jax.numpy as jnp
from jax import lax
from jax.experimental import pallas as pl
from jax.experimental.pallas import tpu as pltpu
from jax.sharding import PartitionSpec as P

KN = 8
TILE = 128
WIN = 512
GX = 64
ZS = 4
LANES = 128
SPAN = WIN // LANES + 1
CAP = 256
XR = 48
F32 = jnp.float32
BF16 = jnp.bfloat16
I32 = jnp.int32
MESH = pl.DeviceIdType.MESH
HIGHEST = lax.Precision.HIGHEST


def dot(a, b):
    return jnp.dot(a, b, preferred_element_type=F32)


def dot_nt(a, b):
    return lax.dot_general(a, b, (((1,), (1,)), ((), ())), preferred_element_type=F32)


def exact(a, b):
    return jnp.dot(a, b, preferred_element_type=F32, precision=HIGHEST)


def exact_nt(a, b):
    return lax.dot_general(a, b, (((1,), (1,)), ((), ())), preferred_element_type=F32, precision=HIGHEST)


def rows_of(shape):
    return lax.broadcasted_iota(I32, shape, 0)


def cols_of(shape):
    return lax.broadcasted_iota(I32, shape, 1)


def gelu_parts(x):
    z = jnp.abs(x) * (2.0**-0.5)
    t = 1.0 / (1.0 + 0.3275911 * z)
    e = jnp.exp(-0.5 * x * x)
    poly = ((((1.061405429 * t - 1.453152027) * t + 1.421413741) * t - 0.284496736) * t + 0.254829592) * t
    tail = 0.5 * poly * e
    cdf = jnp.where(x < 0, tail, 1.0 - tail)
    return x * cdf, cdf + x * e * ((2.0 * math.pi) ** -0.5)


def mask_of(cond):
    return jnp.where(cond, 1.0, 0.0).astype(BF16)


def split3(v):
    a = v.astype(BF16)
    r = v - a.astype(F32)
    b = r.astype(BF16)
    return a, b, (r - b.astype(F32)).astype(BF16)


def weights(win_ref, bin_ref, wout_ref, bout_ref, pad_ref, w1_ref, w2_ref, w2t_ref):
    hid, channels = win_ref.shape[1], wout_ref.shape[0]
    pad_ref[...] = jnp.zeros_like(pad_ref)
    pad_ref[: win_ref.shape[0], :hid] = win_ref[...]
    wide = pad_ref[...].T[:hid]
    w_hi = wide.astype(BF16)
    w_lo = (wide - w_hi.astype(F32)).astype(BF16)
    k, col = rows_of((LANES, LANES)), cols_of((LANES, LANES))
    s_hi = mask_of(((k < 3) & ((col == k) | (col == k + 8))) | ((k >= 3) & (k < 6) & (col == k + 13)))
    s_lo = mask_of(((k < 3) & (col == k + 24)) | ((k >= 3) & (k < 6) & (col == k + 29)))
    w1 = dot(w_hi, s_hi) + dot(w_lo, s_lo)
    pad_ref[0:1, :hid] = bin_ref[...]
    pad_ref[0:1, hid:] = jnp.zeros((1, LANES - hid), F32)
    diag = jnp.where(rows_of((hid, LANES)) == cols_of((hid, LANES)), pad_ref[0:1, :], 0.0)
    for i, part in enumerate(split3(diag)):
        w1 += dot(part, mask_of(col == 3 + i))
    w1_ref[...] = w1.astype(BF16)

    pad_ref[0:channels, :hid] = wout_ref[...].astype(F32)
    pad_ref[0:channels, hid:] = jnp.zeros((channels, LANES - hid), F32)
    w_out = pad_ref[0:channels, :].astype(BF16)
    w2 = dot(w_out, mask_of(k == col))
    eye = mask_of(rows_of((hid, LANES)) == cols_of((hid, LANES)))
    w2t_ref[...] = dot_nt(eye, w_out).astype(BF16)
    pad_ref[0:1, :channels] = bout_ref[...]
    diag = jnp.where(rows_of((channels, LANES)) == cols_of((channels, LANES)), pad_ref[0:1, :], 0.0)
    for i, part in enumerate(split3(diag)):
        w2 += dot(part, mask_of(col == hid + 3 + i))
    w2_ref[...] = w2.astype(BF16)


def order_parts(tiles, limit, offv_ref, table_ref):
    pairs = SPAN * tiles
    lanes = -(-pairs // LANES) * LANES
    base_row = jnp.minimum(lax.shift_right_logical(offv_ref[...], 7), limit)
    wide = jnp.concatenate([base_row, jnp.zeros((1, LANES - tiles), I32)], 1)
    pick = rows_of((tiles, LANES)) == cols_of((tiles, LANES))
    column = jnp.sum(jnp.where(pick, wide.astype(F32), 0.0), 1, keepdims=True)
    key = jnp.concatenate([column + float(j) for j in range(SPAN)], 0)
    key = jnp.broadcast_to(key, (pairs, lanes))
    p, q = rows_of((pairs, lanes)), cols_of((pairs, lanes))
    key_row = jnp.sum(jnp.where(p == q, key, 0.0), 0, keepdims=True)
    key_row = jnp.where(q[:1] < pairs, key_row, 1.0e6)
    ahead = (key_row == key) & (q < p)
    rank = jnp.sum(jnp.where((key_row < key) | ahead, 1.0, 0.0), 1, keepdims=True)
    again = jnp.sum(jnp.where(ahead, 1.0, 0.0), 1, keepdims=True)
    here = rank == q.astype(F32)
    order = jnp.sum(jnp.where(here, p.astype(F32), 0.0), 0, keepdims=True)
    keep = jnp.sum(jnp.where(here & (again > 0), 1.0, 0.0), 0, keepdims=True)
    upto = jnp.sum(jnp.where(key <= q.astype(F32), 1.0, 0.0), 0, keepdims=True)
    some = jnp.sum(jnp.where(key == q.astype(F32), 1.0, 0.0), 0, keepdims=True)
    some = jnp.minimum(some, 1.0)
    last = jnp.maximum(upto - 1.0, 0.0)
    rows = jnp.concatenate([order, keep, last, some, jnp.zeros((4, lanes), F32)], 0)
    table_ref[...] = rows.astype(I32)


def kernel(
    n_pb, n_ga,
    n_ins, latent_in, *rest,
):
    ins, rest = rest[:n_ins], rest[n_ins:]
    outs, rest = rest[:3], rest[3:]
    held, rest = rest[:n_ins], rest[n_ins:]
    body(n_pb, n_ga, latent_in, ins, outs, held, *rest)


def body(
    n_pb, n_ga, latent_in, ins, outs, held, more_ref,
    pts_ref, pos_ref, from_ref, upto_ref, pad_ref, w1_ref, w2_ref, w2t_ref, tablev_ref, table_ref,
    cots_ref, hid_ref, slope_ref, x_ref, spot_ref, parts_ref, sums_ref, feats_ref,
    near_ref, nearin_ref, far_ref, farin_ref, half_ref, own_ref, acc_ref,
    ar_ref, arin_ref, gaall_ref, fin_ref,
    in_sem, latent_sem, out_sem, table_sem, gsend, grecv, fsend, frecv, nsend, nrecv, rsend, rrecv, hsend, hrecv, asend, arecv, bsend, brecv, csend, crecv,
):
    offs_ref, offv_ref, win_ref, bin_ref, wout_ref, bout_ref, ids_ref, qp_ref, rel_ref, cot_ref = held[:10]
    grid_ref, final_ref, more_out = outs
    me, slab = lax.axis_index("pb"), lax.axis_index("ga")
    chips = n_pb // 2
    chip, core = me // 2, me % 2
    sibling = chip * 2 + 1 - core
    tiles = cot_ref.shape[1] // TILE
    channels, hid = cot_ref.shape[0], win_ref.shape[1]
    blocks = latent_in.shape[2] // LANES
    limit = blocks * n_pb - SPAN
    group = math.gcd(tiles, 4)

    def send(src, dst, ssem, rsem, where):
        return pltpu.make_async_remote_copy(
            src_ref=src, dst_ref=dst, send_sem=ssem, recv_sem=rsem, device_id=where, device_id_type=MESH
        )

    square = chips == 4 and blocks % 2 == 0
    if square:
        beside = chip + 1 - 2 * (chip % 2)
        above = lax.rem(chip + 2, 4)
        others = [beside, above, lax.rem(beside + 2, 4)]
    else:
        others = [lax.rem(chip + m, chips) for m in range(1, chips)]
    peers = [o * 2 + core for o in others]
    near_chips = others + [chip]
    half = blocks // 2

    barrier = pltpu.get_barrier_semaphore()
    for m in range(1, n_pb):
        pl.semaphore_signal(barrier, inc=1, device_id={"pb": lax.rem(me + m, n_pb)}, device_id_type=MESH)
    for m in range(1, n_ga):
        pl.semaphore_signal(barrier, inc=1, device_id={"ga": lax.rem(slab + m, n_ga)}, device_id_type=MESH)
    mine = me * blocks
    latent_copies = [
        pltpu.make_async_copy(latent_in.at[0, :, pl.ds(b * LANES, LANES)], feats_ref.at[mine + b], latent_sem)
        for b in range(blocks)
    ]
    loads = [pltpu.make_async_copy(src, dst, in_sem.at[i]) for i, (src, dst) in enumerate(zip(ins, held))]
    for copy in latent_copies + loads:
        copy.start()
    def feats_of(d):
        return feats_ref.at[pl.ds(d * blocks, blocks)]

    pltpu.make_async_copy(feats_of(me), feats_of(me), latent_sem).wait()
    pl.semaphore_wait(barrier, n_pb - 1 + n_ga - 1)
    def half_of(d, h):
        return feats_ref.at[pl.ds(d * blocks + h * half, half)]

    def piece(slot, d, h, ssem, to):
        return send(half_of(d, h), half_of(d, h), ssem, grecv.at[slot, h], {"pb": to})

    out = []
    if square:
        for i in range(2):
            out.append(piece(0, me, 1 - i, gsend, peers[0]))
            out.append(piece(1, me, i, gsend, peers[1]))
    else:
        for i, to in enumerate(peers):
            out.append(send(feats_of(me), feats_of(me), gsend, grecv.at[i, 0], {"pb": to}))
    out.append(send(feats_of(me), feats_of(me), gsend, frecv, {"pb": sibling}))
    for copy in out:
        copy.start()

    for copy in loads:
        copy.wait()
    pts_ref[...] = jnp.ones_like(pts_ref)
    pts_ref[0:3, :] = qp_ref[...]
    order_parts(tiles, limit, offv_ref, tablev_ref)
    weights(win_ref, bin_ref, wout_ref, bout_ref, pad_ref, w1_ref, w2_ref, w2t_ref)
    table_copy = pltpu.make_async_copy(tablev_ref, table_ref, table_sem)
    table_copy.start()

    lives = [jnp.where(ids_ref[:, t * TILE : (t + 1) * TILE] == slab, 1.0, 0.0) for t in range(tiles)]
    live = jnp.concatenate(lives, 0)
    rows = tiles * KN
    packed = live.astype(BF16)
    before = dot(packed, mask_of(rows_of((TILE, TILE)) < cols_of((TILE, TILE))))
    total = dot(packed, jnp.ones((TILE, TILE), BF16))
    r, c = rows_of((rows, rows)), cols_of((rows, rows))
    start = dot(mask_of((r // KN == c // KN) & (c < r)), total.astype(BF16))
    skip = (held[10][0] * CAP).astype(F32) if len(held) > 10 else 0.0
    pos_ref[...] = jnp.where(live > 0, before + start - skip, -1.0e6)
    from_ref[...] = start - skip
    upto_ref[...] = start + total - skip
    left = jnp.max(start + total - skip - float(CAP), axis=0, keepdims=True)
    left = jnp.max(left, axis=1, keepdims=True)

    def tile_base(t):
        return jnp.minimum(lax.shift_right_logical(offs_ref[0, t], 7), limit)

    def draw(t):
        cols = pl.ds(pl.multiple_of(t * TILE, TILE), TILE)
        lines = pl.ds(pl.multiple_of(t * KN, KN), KN)
        base = tile_base(t)
        pos = pos_ref[lines, :].astype(BF16)
        place = rows_of((CAP, TILE)).astype(F32).astype(BF16)
        pick = jnp.zeros((CAP, TILE), BF16)
        one = jnp.ones((CAP, TILE), BF16)
        for k in range(KN):
            pick = jnp.where(pos[k : k + 1, :] == place, one, pick)
        relp = rel_ref[:, cols] + (offs_ref[0, t] - base * LANES)
        low = (relp & (LANES - 1)).astype(F32)
        high = lax.shift_right_logical(relp, 7).astype(F32)
        points = pts_ref[:, cols]
        p_hi = points.astype(BF16).astype(F32)
        small = jnp.concatenate([p_hi, points - p_hi, low, high], 0).astype(BF16)
        data = jnp.concatenate([cot_ref[:, cols], small], 0)
        return dot_nt(data, pick)

    def place_inputs(t, drawn):
        lines = pl.ds(pl.multiple_of(t * KN, KN), KN)
        base = tile_base(t)
        head = drawn[channels : channels + 16]
        wide_from = jnp.concatenate([from_ref[lines, :]] * (CAP // TILE), 1)
        wide_upto = jnp.concatenate([upto_ref[lines, :]] * (CAP // TILE), 1)
        index = cols_of((KN, CAP)).astype(F32)
        which = (index >= wide_from) & (index < wide_upto)
        lo = jnp.sum(jnp.where(which, drawn[channels + 16 : channels + 24], 0.0), 0, keepdims=True)
        hi = jnp.sum(jnp.where(which, drawn[channels + 24 : channels + 32], 0.0), 0, keepdims=True)
        lo = jnp.broadcast_to(lo, (8, CAP))
        hi = jnp.broadcast_to(hi, (8, CAP))
        cell = (base + hi.astype(I32)) * LANES + lo.astype(I32)
        row = rows_of((8, CAP))
        along = jnp.where(
            row == 0,
            lax.shift_right_logical(cell, int(math.log2(GX * ZS))),
            jnp.where(
                row == 1,
                lax.shift_right_logical(cell, int(math.log2(ZS))) & (GX - 1),
                (cell & (ZS - 1)) + slab * ZS,
            ),
        )
        centre = jnp.where(row < 3, (along.astype(F32) + 0.5) / GX, 0.0)
        x = jnp.concatenate([head, centre, head[:8], centre, jnp.zeros((8, CAP), F32)], 0).astype(BF16)
        return x, lo, hi

    def lane_onehot(lo):
        row = jnp.broadcast_to(lo[:1], (LANES, CAP)).astype(BF16)
        return jnp.where(
            rows_of((LANES, CAP)).astype(F32).astype(BF16) == row, jnp.ones((LANES, CAP), BF16), jnp.zeros((LANES, CAP), BF16)
        )

    def spread(hi, grad):
        full = jnp.concatenate([hi, hi], 0)
        pieces = []
        for j in range(SPAN):
            on = jnp.where(full == float(j), 1.0, 0.0).astype(BF16)
            pieces.append(grad * jnp.concatenate([on] * (channels // 16), 0))
        return jnp.concatenate(pieces, 0)

    def first(i, carry):
        ts = [i * group + u for u in range(group)]
        drawn = [draw(t) for t in ts]
        placed = [place_inputs(t, d) for t, d in zip(ts, drawn)]
        cots = [d[:channels].astype(BF16) for d in drawn]
        pres = [dot(w1_ref[:, :XR], x) for x, _, _ in placed]
        kerns = []
        for t, pre, cot, (x, lo, hi) in zip(ts, pres, cots, placed):
            hidden, slope = gelu_parts(pre)
            hidden = hidden.astype(BF16)
            kerns.append(dot(w2_ref[...], jnp.concatenate([hidden, x], 0)))
            hid_ref[t] = hidden
            slope_ref[t] = slope
            cots_ref[t] = cot
            x_ref[t] = x
            spot_ref[t] = jnp.where(rows_of((8, CAP)) < 4, lo, hi)
        parts = []
        for kern, cot, (x, lo, hi) in zip(kerns, cots, placed):
            grad = (kern * cot.astype(F32)).astype(BF16)
            parts.append(dot_nt(spread(hi, grad), lane_onehot(lo)))
        for t, part in zip(ts, parts):
            for j in range(SPAN):
                parts_ref[j * tiles + t] = part[j * channels : (j + 1) * channels]
        return carry

    steps = tiles // group

    def pass_half(i, h):
        return send(half_of(peers[i], h), half_of(peers[i], h), fsend, frecv, {"pb": sibling})

    def come(i, h):
        piece(i, peers[i], h, gsend, peers[i]).wait_recv()

    middle, late_step = steps // 2, steps * 7 // 8
    lax.fori_loop(0, middle, first, 0)
    if square:
        come(0, 1)
        piece(2, peers[0], 1, hsend, peers[1]).start()
        come(1, 0)
        piece(2, peers[1], 0, hsend, peers[0]).start()
        pass_half(0, 1).start()
        pass_half(1, 0).start()
    lax.fori_loop(middle, late_step, first, 0)
    if square:
        for i in range(2):
            come(i, i)
            pass_half(i, i).start()
    lax.fori_loop(late_step, steps, first, 0)

    if square:
        for h in range(2):
            come(2, h)
            pass_half(2, h).start()
    table_copy.wait()

    def pair_at(line, b):
        return jnp.clip(table_ref[line, b], 0, SPAN * tiles - 1)

    def run(i, acc):
        for u in range(group):
            at = i * group + u
            acc = acc * table_ref[1, at].astype(F32) + parts_ref[pair_at(0, at)]
            sums_ref[at] = acc
        return acc

    lax.fori_loop(0, SPAN * tiles // group, run, jnp.zeros((channels, LANES), F32))

    def block(b):
        return sums_ref[pair_at(2, b)] * table_ref[3, b].astype(F32)

    def near_copy(i):
        return send(near_ref.at[i], nearin_ref.at[i], nsend, nrecv.at[i], {"pb": sibling})

    pair = math.gcd(blocks, 4)
    order = list(range(chips - 2, -1, -1)) + [chips - 1]
    for n, i in enumerate(order):
        owner = near_chips[i] * 2 + 1 - core

        def fill(b, carry, i=i, owner=owner):
            for u in range(pair):
                near_ref[i, b * pair + u] = block(owner * blocks + b * pair + u).astype(BF16)
            return carry

        lax.fori_loop(0, blocks // pair, fill, 0)
        if n > 0:
            near_copy(order[n - 1]).start()
    if not square:
        for i in range(chips - 1):
            d = lax.rem(chip + chips - 1 - i, chips) * 2 + core
            send(feats_of(d), feats_of(d), gsend, grecv.at[i, 0], {"pb": d}).wait_recv()
            send(feats_of(d), feats_of(d), fsend, frecv, {"pb": sibling}).start()

    all_twins = feats_ref.at[pl.ds(0, chips * blocks)]
    send(all_twins, all_twins, gsend, frecv, {"pb": sibling}).wait_recv()

    acc_ref[...] = jnp.zeros_like(acc_ref)

    def draw_feats(t):
        window = feats_ref[pl.ds(tile_base(t), SPAN)].reshape(SPAN * channels, LANES)
        return dot(window, lane_onehot(spot_ref[t]))

    def feats_grad(t, drawn):
        tall = jnp.broadcast_to(spot_ref[t][4:5], (channels, CAP))
        feats = drawn[:channels]
        for j in range(1, SPAN):
            feats = jnp.where(tall == float(j), drawn[j * channels : (j + 1) * channels], feats)
        return (feats * cots_ref[t].astype(F32)).astype(BF16)

    wide = math.gcd(tiles, 8)

    def second(i, carry):
        ts = [i * wide + u for u in range(wide)]
        drawn = [draw_feats(t) for t in ts]
        grads = [feats_grad(t, d) for t, d in zip(ts, drawn)]
        pres = [dot(w2t_ref[...], g) for g in grads]
        sums = []
        for t, g, p in zip(ts, grads, pres):
            both = jnp.concatenate([g, (p * slope_ref[t]).astype(BF16)], 0)
            sums.append(dot_nt(both, jnp.concatenate([hid_ref[t], x_ref[t]], 0)))
        acc_ref[...] += functools.reduce(lambda a, b: a + b, sums)
        return carry

    near_copy(order[-1]).start()
    ahead = tiles // wide // 2
    lax.fori_loop(0, ahead, second, 0)
    if square:
        early = [(2, 0, 0, half_ref.at[0], 0), (2, 1, 1, half_ref.at[1], 1)]
        early += [(0, 0, 0, farin_ref.at[0, pl.ds(0, half)], 2), (1, 1, 1, farin_ref.at[1, pl.ds(half, half)], 2)]
        late = [(0, 1, 0, farin_ref.at[0, pl.ds(half, half)], 2), (1, 0, 1, farin_ref.at[1, pl.ds(0, half)], 2)]

        def far_half(slot, h, to, dst, n):
            return send(far_ref.at[slot, pl.ds(h * half, half)], dst, hsend, hrecv.at[n], {"pb": peers[to]})

        early = [far_half(*e) for e in early]
        late = [far_half(*e) for e in late]
        slots = [early[:2], [], []]
    else:
        fars = [
            send(far_ref.at[i], farin_ref.at[i], rsend.at[i], rrecv.at[i], {"pb": to}) for i, to in enumerate(peers)
        ]
        slots = [(fars[i],) for i in order[:-1]]
    if square:
        order = [2, 0, 1, 3]
    for n, i in enumerate(order):
        owner = near_chips[i] * 2 + core
        near_copy(i).wait_recv()

        def join(b, carry, i=i, owner=owner):
            for u in range(pair):
                at = b * pair + u
                value = block(owner * blocks + at) + nearin_ref[i, at].astype(F32)
                if i < chips - 1:
                    far_ref[i, at] = value.astype(BF16)
                else:
                    own_ref[at] = value
            return carry

        lax.fori_loop(0, blocks // pair, join, 0)
        if n > 0:
            for copy in slots[n - 1]:
                copy.start()

    lax.fori_loop(ahead, tiles // wide, second, 0)

    k, l = rows_of((LANES, LANES)), cols_of((LANES, LANES))

    def gathered(shift):
        a = (l - shift >= 0) & (l - shift < 4) & ((k == hid + l - shift) | ((k == hid + 8 + l - shift) & (l - shift < 3)))
        b = (l - shift >= 4) & (l - shift < 7) & (k == hid + 16 + l - shift - 4)
        return jnp.where(a | b, 1.0, 0.0)

    top = jnp.where(cols_of((channels, LANES)) < 112, acc_ref[:channels], 0.0)
    tail = hid - channels
    top += exact(acc_ref[channels : 2 * channels], gathered(112))
    rest = exact(acc_ref[2 * channels : 2 * channels + tail], gathered(120))
    flag = jnp.where(left > 0, 1.0, 0.0)
    slices = channels // n_pb
    top = jnp.concatenate([top[:tail] + rest, top[tail:]], 0)
    marked = (lax.rem(rows_of((channels, LANES)), slices) == 0) & (cols_of((channels, LANES)) == LANES - 1)
    top = jnp.where(marked, flag, top)
    ar_ref[...] = top.reshape(n_pb, slices, LANES)
    arin_ref[pl.ds(me, 1)] = ar_ref[pl.ds(me, 1)]
    for m in range(1, n_pb):
        to = lax.rem(me + m, n_pb)
        send(ar_ref.at[to], arin_ref.at[me], asend, arecv, {"pb": to}).start()
    if square:
        for copy in early[2:]:
            copy.start()
        for i, copy in enumerate(early[:2]):
            copy.wait_recv()
            into = far_ref.at[1 - i, pl.ds(i * half, half)]
            into[...] = (into[...].astype(F32) + half_ref[i].astype(F32)).astype(BF16)
    most = pl.ds(0, n_pb - 1)
    all_in = send(ar_ref.at[most], arin_ref.at[most], asend, arecv, {"pb": sibling})
    all_in.wait_recv()
    gaall_ref[pl.ds(slab, 1)] = jnp.sum(arin_ref[...], 0, keepdims=True)
    for m in range(1, n_ga):
        to = lax.rem(slab + m, n_ga)
        send(gaall_ref.at[slab], gaall_ref.at[slab], bsend, brecv, {"ga": to}).start()
    if square:
        for copy in late:
            copy.start()
    less = gaall_ref.at[pl.ds(0, n_ga - 1)]
    all_slabs = send(less, less, bsend, brecv, {"pb": sibling})
    all_slabs.wait_recv()
    settled = jnp.sum(gaall_ref[...], 0, keepdims=True)
    fin_ref[pl.ds(me, 1)] = settled
    more_ref[0] = jnp.sum(jnp.where(cols_of((1, LANES)) == LANES - 1, settled[0, 0:1], 0.0)).astype(I32)
    for m in range(1, n_pb):
        to = lax.rem(me + m, n_pb)
        send(fin_ref.at[me], fin_ref.at[me], csend, crecv, {"pb": to}).start()
    tell = pltpu.make_async_copy(more_ref, more_out, out_sem)
    tell.start()

    if square:
        come_in = farin_ref.at[pl.ds(0, 2)]
        send(come_in, come_in, hsend, hrecv.at[2], {"pb": sibling}).wait_recv()
    else:
        for copy in fars:
            copy.wait_recv()
    for b in range(blocks):
        value = own_ref[b]
        for i in range(2 if square else chips - 1):
            value += farin_ref[i, b].astype(F32)
        grid_ref[0, :, b * LANES : (b + 1) * LANES] = value

    all_final = send(fin_ref.at[most], fin_ref.at[most], csend, crecv, {"pb": sibling})
    all_final.wait_recv()
    final = fin_ref[...].reshape(channels, LANES)
    final_ref[...] = final
    tell.wait()
    all_feats = feats_ref.at[pl.ds(0, (3 if square else chips) * blocks)]
    send(all_feats, all_feats, gsend, frecv, {"pb": sibling}).wait_send()
    passed = feats_ref.at[pl.ds(0, (chips - 1) * blocks)]
    send(passed, passed, fsend, frecv, {"pb": sibling}).wait_send()
    send(near_ref, nearin_ref, nsend, nrecv.at[0], {"pb": sibling}).wait_send()
    if square:
        send(all_twins, all_twins, hsend, frecv, {"pb": sibling}).wait_send()
    else:
        for copy in fars:
            copy.wait_send()
    for copy in (all_in, all_slabs, all_final):
        copy.wait_send()


def call(step, collective_id, query_points, cotangent, slab_ids, rel_cells, offsets, latent, w_in, b_in, w_out, b_out):
    n_pb, n_ga = lax.axis_size("pb"), lax.axis_size("ga")
    channels, owned = latent.shape[1], latent.shape[2]
    hid = w_in.shape[0]
    queries = query_points.shape[1]
    tiles = queries // TILE
    chips = n_pb // 2
    blocks = owned // LANES
    pairs = SPAN * tiles
    lanes = -(-pairs // LANES) * LANES
    hbm = pl.BlockSpec(memory_space=pltpu.HBM)
    vmem = pl.BlockSpec(memory_space=pltpu.VMEM)
    dma = pltpu.SemaphoreType.DMA
    slices = channels // n_pb
    ins = (offsets, offsets, w_in.T, b_in[None], w_out, b_out[None], slab_ids, query_points, rel_cells, cotangent)
    ins += () if step is None else (step,)
    outs = [
        ((1, channels, owned), F32),
        ((channels, LANES), F32),
        ((1,), I32),
    ]
    return pl.pallas_call(
        functools.partial(kernel, n_pb, n_ga, len(ins)),
        out_shape=[jax.ShapeDtypeStruct(*o) for o in outs],
        in_specs=[hbm] * (1 + len(ins)),
        out_specs=[vmem, vmem, hbm],
        scratch_shapes=[(pltpu.SMEM if i in (0, 10) else pltpu.VMEM)(a.shape, a.dtype) for i, a in enumerate(ins)]
        + [pltpu.SMEM(*outs[2])]
        + [
            pltpu.VMEM((8, queries), F32),
            pltpu.VMEM((tiles * KN, TILE), F32),
            pltpu.VMEM((tiles * KN, TILE), F32),
            pltpu.VMEM((tiles * KN, TILE), F32),
            pltpu.VMEM((LANES, LANES), F32),
            pltpu.VMEM((hid, LANES), BF16),
            pltpu.VMEM((channels, LANES), BF16),
            pltpu.VMEM((hid, channels), BF16),
            pltpu.VMEM((8, lanes), I32),
            pltpu.SMEM((8, lanes), I32),
            pltpu.VMEM((tiles, channels, CAP), BF16),
            pltpu.VMEM((tiles, hid, CAP), BF16),
            pltpu.VMEM((tiles, hid, CAP), F32),
            pltpu.VMEM((tiles, XR, CAP), BF16),
            pltpu.VMEM((tiles, 8, CAP), F32),
            pltpu.VMEM((pairs, channels, LANES), F32),
            pltpu.VMEM((pairs, channels, LANES), F32),
            pltpu.VMEM((n_pb * blocks, channels, LANES), BF16),
            pltpu.VMEM((chips, blocks, channels, LANES), BF16),
            pltpu.VMEM((chips, blocks, channels, LANES), BF16),
            pltpu.VMEM((chips - 1, blocks, channels, LANES), BF16),
            pltpu.VMEM((chips - 1, blocks, channels, LANES), BF16),
            pltpu.VMEM((2, max(blocks // 2, 1), channels, LANES), BF16),
            pltpu.VMEM((blocks, channels, LANES), F32),
            pltpu.VMEM((channels + hid, LANES), F32),
            pltpu.VMEM((n_pb, slices, LANES), F32),
            pltpu.VMEM((n_pb, slices, LANES), F32),
            pltpu.VMEM((n_ga, slices, LANES), F32),
            pltpu.VMEM((n_pb, slices, LANES), F32),
            dma((len(ins),)),
            dma,
            dma,
            dma,
            dma,
            dma((chips - 1, 2)),
            dma,
            dma,
            dma,
            dma((chips,)),
            dma((chips,)),
            dma((chips,)),
            dma,
            dma((3,)),
            dma,
            dma,
            dma,
            dma,
            dma,
            dma,
        ],
        compiler_params=pltpu.CompilerParams(
            vmem_limit_bytes=67043328 - 4 * channels * (owned + LANES) - 1024, collective_id=collective_id, has_side_effects=True
        ),
        name="whole",
    )(latent, *ins)


def settle(scale, grid_in, final_ref, grid_ref, *rest):
    smalls, ready = rest[:4], rest[4:8]
    grid_sem, small_sem = rest[8:]
    gwin_ref, gbin_ref, gwout_ref, gbout_ref = ready
    move = pltpu.make_async_copy(grid_in, grid_ref, grid_sem)
    move.start()
    channels, hid = gwout_ref.shape
    final = final_ref[...]
    k, l = rows_of((LANES, LANES)), cols_of((LANES, LANES))

    def chosen(shift):
        along = (l < 3) & (k == shift + l)
        cells = (l >= 3) & (l < 6) & (k == shift + 1 + l)
        return jnp.where(along | cells | ((l == 6) & (k == shift + 3)), scale, 0.0)

    gwout_ref[...] = final[:, :hid] * scale
    taken = jnp.concatenate([exact(final, chosen(112)), exact(final[: hid - channels], chosen(120))], 0)
    turned = exact_nt(jnp.where(rows_of((8, LANES)) == cols_of((8, LANES)), 1.0, 0.0), taken)
    gwin_ref[...] = turned[: gwin_ref.shape[0]]
    gbin_ref[...] = turned[6:7]
    gbout_ref[...] = exact_nt(jnp.where(cols_of((8, LANES)) == hid + 3, scale, 0.0), final)[0:1]
    stores = [pltpu.make_async_copy(src, dst, small_sem.at[i]) for i, (src, dst) in enumerate(zip(ready, smalls))]
    for copy in stores:
        copy.start()
    for copy in stores:
        copy.wait()
    move.wait()


def shards(*args):
    def again(state):
        step, _, sums = state
        grid, final, more = call(step, 1, *args)
        return step + 1, more, (sums[0] + grid, sums[1] + final)

    grid, final, more = call(None, 0, *args)
    first = (jnp.ones((1,), I32), more, (grid, final))
    grid, final = lax.while_loop(lambda state: state[1][0] > 0, again, first)[2]
    hid, channels = args[6].shape[0], args[8].shape[0]
    queries = args[0].shape[1] * lax.axis_size("pb")
    hbm = pl.BlockSpec(memory_space=pltpu.HBM)
    dma = pltpu.SemaphoreType.DMA
    shapes = [args[6].shape[::-1], (1, hid), (channels, hid), (1, channels)]
    grid, gwin, gbin, gwout, gbout = pl.pallas_call(
        functools.partial(settle, float(queries) ** (-0.5)),
        out_shape=[jax.ShapeDtypeStruct(v, F32) for v in [grid.shape] + shapes],
        in_specs=[hbm, pl.BlockSpec(memory_space=pltpu.VMEM)],
        out_specs=[hbm] * 5,
        scratch_shapes=[pltpu.VMEM(v, F32) for v in shapes] + [dma, dma((4,))],
        name="settle",
    )(grid, final)
    return grid, gwin.T, gbin[0], gwout, gbout[0]


def solution(mesh):
    return jax.shard_map(
        shards,
        mesh=mesh,
        in_specs=(
            P(None, "pb"),
            P(None, "pb"),
            P(None, "pb"),
            P(None, "pb"),
            P("ga", "pb"),
            P("ga", None, "pb"),
            P(),
            P(),
            P(),
            P(),
        ),
        out_specs=(P("ga", None, "pb"), P(), P(), P(), P()),
        check_vma=False,
    )
```

```python
import functools
import math

import jax
import jax.numpy as jnp
from jax import lax
from jax.experimental import pallas as pl
from jax.experimental.pallas import tpu as pltpu
from jax.sharding import PartitionSpec as P

KN = 8
TILE = 128
WIN = 512
GX = 64
ZS = 4
LANES = 128
SPAN = WIN // LANES + 1
CAP = 256
XR = 48
F32 = jnp.float32
BF16 = jnp.bfloat16
I32 = jnp.int32
MESH = pl.DeviceIdType.MESH
HIGHEST = lax.Precision.HIGHEST


def dot(a, b):
    return jnp.dot(a, b, preferred_element_type=F32)


def dot_nt(a, b):
    return lax.dot_general(a, b, (((1,), (1,)), ((), ())), preferred_element_type=F32)


def exact(a, b):
    return jnp.dot(a, b, preferred_element_type=F32, precision=HIGHEST)


def exact_nt(a, b):
    return lax.dot_general(a, b, (((1,), (1,)), ((), ())), preferred_element_type=F32, precision=HIGHEST)


def rows_of(shape):
    return lax.broadcasted_iota(I32, shape, 0)


def cols_of(shape):
    return lax.broadcasted_iota(I32, shape, 1)


def gelu_parts(x):
    z = jnp.abs(x) * (2.0**-0.5)
    t = 1.0 / (1.0 + 0.3275911 * z)
    e = jnp.exp(-0.5 * x * x)
    poly = ((((1.061405429 * t - 1.453152027) * t + 1.421413741) * t - 0.284496736) * t + 0.254829592) * t
    tail = 0.5 * poly * e
    cdf = jnp.where(x < 0, tail, 1.0 - tail)
    return x * cdf, cdf + x * e * ((2.0 * math.pi) ** -0.5)


def mask_of(cond):
    return jnp.where(cond, 1.0, 0.0).astype(BF16)


def split3(v):
    a = v.astype(BF16)
    r = v - a.astype(F32)
    b = r.astype(BF16)
    return a, b, (r - b.astype(F32)).astype(BF16)


def weights(win_ref, bin_ref, wout_ref, bout_ref, pad_ref, w1_ref, w2_ref, w2t_ref):
    hid, channels = win_ref.shape[1], wout_ref.shape[0]
    pad_ref[...] = jnp.zeros_like(pad_ref)
    pad_ref[: win_ref.shape[0], :hid] = win_ref[...]
    wide = pad_ref[...].T[:hid]
    w_hi = wide.astype(BF16)
    w_lo = (wide - w_hi.astype(F32)).astype(BF16)
    k, col = rows_of((LANES, LANES)), cols_of((LANES, LANES))
    s_hi = mask_of(((k < 3) & ((col == k) | (col == k + 8))) | ((k >= 3) & (k < 6) & (col == k + 13)))
    s_lo = mask_of(((k < 3) & (col == k + 24)) | ((k >= 3) & (k < 6) & (col == k + 29)))
    w1 = dot(w_hi, s_hi) + dot(w_lo, s_lo)
    pad_ref[0:1, :hid] = bin_ref[...]
    pad_ref[0:1, hid:] = jnp.zeros((1, LANES - hid), F32)
    diag = jnp.where(rows_of((hid, LANES)) == cols_of((hid, LANES)), pad_ref[0:1, :], 0.0)
    for i, part in enumerate(split3(diag)):
        w1 += dot(part, mask_of(col == 3 + i))
    w1_ref[...] = w1.astype(BF16)

    pad_ref[0:channels, :hid] = wout_ref[...].astype(F32)
    pad_ref[0:channels, hid:] = jnp.zeros((channels, LANES - hid), F32)
    w_out = pad_ref[0:channels, :].astype(BF16)
    w2 = dot(w_out, mask_of(k == col))
    eye = mask_of(rows_of((hid, LANES)) == cols_of((hid, LANES)))
    w2t_ref[...] = dot_nt(eye, w_out).astype(BF16)
    pad_ref[0:1, :channels] = bout_ref[...]
    diag = jnp.where(rows_of((channels, LANES)) == cols_of((channels, LANES)), pad_ref[0:1, :], 0.0)
    for i, part in enumerate(split3(diag)):
        w2 += dot(part, mask_of(col == hid + 3 + i))
    w2_ref[...] = w2.astype(BF16)


def order_parts(tiles, limit, offv_ref, table_ref):
    pairs = SPAN * tiles
    lanes = -(-pairs // LANES) * LANES
    base_row = jnp.minimum(lax.shift_right_logical(offv_ref[...], 7), limit)
    wide = jnp.concatenate([base_row, jnp.zeros((1, LANES - tiles), I32)], 1)
    pick = rows_of((tiles, LANES)) == cols_of((tiles, LANES))
    column = jnp.sum(jnp.where(pick, wide.astype(F32), 0.0), 1, keepdims=True)
    key = jnp.concatenate([column + float(j) for j in range(SPAN)], 0)
    key = jnp.broadcast_to(key, (pairs, lanes))
    p, q = rows_of((pairs, lanes)), cols_of((pairs, lanes))
    key_row = jnp.sum(jnp.where(p == q, key, 0.0), 0, keepdims=True)
    key_row = jnp.where(q[:1] < pairs, key_row, 1.0e6)
    ahead = (key_row == key) & (q < p)
    rank = jnp.sum(jnp.where((key_row < key) | ahead, 1.0, 0.0), 1, keepdims=True)
    again = jnp.sum(jnp.where(ahead, 1.0, 0.0), 1, keepdims=True)
    here = rank == q.astype(F32)
    order = jnp.sum(jnp.where(here, p.astype(F32), 0.0), 0, keepdims=True)
    keep = jnp.sum(jnp.where(here & (again > 0), 1.0, 0.0), 0, keepdims=True)
    upto = jnp.sum(jnp.where(key <= q.astype(F32), 1.0, 0.0), 0, keepdims=True)
    some = jnp.sum(jnp.where(key == q.astype(F32), 1.0, 0.0), 0, keepdims=True)
    some = jnp.minimum(some, 1.0)
    last = jnp.maximum(upto - 1.0, 0.0)
    rows = jnp.concatenate([order, keep, last, some, jnp.zeros((4, lanes), F32)], 0)
    table_ref[...] = rows.astype(I32)


def kernel(
    n_pb, n_ga,
    n_ins, latent_in, *rest,
):
    ins, rest = rest[:n_ins], rest[n_ins:]
    outs, rest = rest[:3], rest[3:]
    held, rest = rest[:n_ins], rest[n_ins:]
    body(n_pb, n_ga, latent_in, ins, outs, held, *rest)


def body(
    n_pb, n_ga, latent_in, ins, outs, held, more_ref,
    pts_ref, pos_ref, from_ref, upto_ref, pad_ref, w1_ref, w2_ref, w2t_ref, tablev_ref, table_ref,
    cots_ref, hid_ref, slope_ref, x_ref, spot_ref, parts_ref, sums_ref, feats_ref,
    near_ref, nearin_ref, far_ref, farin_ref, half_ref, own_ref, acc_ref,
    ar_ref, arin_ref, gaall_ref, fin_ref, marks_ref, markz_ref,
    in_sem, latent_sem, out_sem, table_sem, gsend, grecv, fsend, frecv, nsend, nrecv, rsend, rrecv, hsend, hrecv, asend, arecv, bsend, brecv, csend, crecv, msend, mrecv, zsend, zrecv,
):
    offs_ref, offv_ref, win_ref, bin_ref, wout_ref, bout_ref, ids_ref, qp_ref, rel_ref, cot_ref = held[:10]
    grid_ref, final_ref, more_out = outs
    me, slab = lax.axis_index("pb"), lax.axis_index("ga")
    chips = n_pb // 2
    chip, core = me // 2, me % 2
    sibling = chip * 2 + 1 - core
    tiles = cot_ref.shape[1] // TILE
    channels, hid = cot_ref.shape[0], win_ref.shape[1]
    blocks = latent_in.shape[2] // LANES
    limit = blocks * n_pb - SPAN
    group = math.gcd(tiles, 4)

    def send(src, dst, ssem, rsem, where):
        return pltpu.make_async_remote_copy(
            src_ref=src, dst_ref=dst, send_sem=ssem, recv_sem=rsem, device_id=where, device_id_type=MESH
        )

    square = chips == 4 and blocks % 2 == 0
    if square:
        beside = chip + 1 - 2 * (chip % 2)
        above = lax.rem(chip + 2, 4)
        others = [beside, above, lax.rem(beside + 2, 4)]
    else:
        others = [lax.rem(chip + m, chips) for m in range(1, chips)]
    peers = [o * 2 + core for o in others]
    near_chips = others + [chip]
    half = blocks // 2

    barrier = pltpu.get_barrier_semaphore()
    for m in range(1, n_pb):
        pl.semaphore_signal(barrier, inc=1, device_id={"pb": lax.rem(me + m, n_pb)}, device_id_type=MESH)
    for m in range(1, n_ga):
        pl.semaphore_signal(barrier, inc=1, device_id={"ga": lax.rem(slab + m, n_ga)}, device_id_type=MESH)
    mine = me * blocks
    latent_copies = [
        pltpu.make_async_copy(latent_in.at[0, :, pl.ds(b * LANES, LANES)], feats_ref.at[mine + b], latent_sem)
        for b in range(blocks)
    ]
    loads = [pltpu.make_async_copy(src, dst, in_sem.at[i]) for i, (src, dst) in enumerate(zip(ins, held))]
    for copy in latent_copies + loads:
        copy.start()
    def feats_of(d):
        return feats_ref.at[pl.ds(d * blocks, blocks)]

    pltpu.make_async_copy(feats_of(me), feats_of(me), latent_sem).wait()
    pl.semaphore_wait(barrier, n_pb - 1 + n_ga - 1)
    def half_of(d, h):
        return feats_ref.at[pl.ds(d * blocks + h * half, half)]

    def piece(slot, d, h, ssem, to):
        return send(half_of(d, h), half_of(d, h), ssem, grecv.at[slot, h], {"pb": to})

    out = []
    if square:
        for i in range(2):
            out.append(piece(0, me, 1 - i, gsend, peers[0]))
            out.append(piece(1, me, i, gsend, peers[1]))
    else:
        for i, to in enumerate(peers):
            out.append(send(feats_of(me), feats_of(me), gsend, grecv.at[i, 0], {"pb": to}))
    out.append(send(feats_of(me), feats_of(me), gsend, frecv, {"pb": sibling}))
    for copy in out:
        copy.start()

    for copy in loads:
        copy.wait()
    pts_ref[...] = jnp.ones_like(pts_ref)
    pts_ref[0:3, :] = qp_ref[...]
    order_parts(tiles, limit, offv_ref, tablev_ref)
    weights(win_ref, bin_ref, wout_ref, bout_ref, pad_ref, w1_ref, w2_ref, w2t_ref)
    table_copy = pltpu.make_async_copy(tablev_ref, table_ref, table_sem)
    table_copy.start()

    lives = [jnp.where(ids_ref[:, t * TILE : (t + 1) * TILE] == slab, 1.0, 0.0) for t in range(tiles)]
    live = jnp.concatenate(lives, 0)
    rows = tiles * KN
    packed = live.astype(BF16)
    before = dot(packed, mask_of(rows_of((TILE, TILE)) < cols_of((TILE, TILE))))
    total = dot(packed, jnp.ones((TILE, TILE), BF16))
    r, c = rows_of((rows, rows)), cols_of((rows, rows))
    start = dot(mask_of((r // KN == c // KN) & (c < r)), total.astype(BF16))
    skip = (held[10][0] * CAP).astype(F32) if len(held) > 10 else 0.0
    pos_ref[...] = jnp.where(live > 0, before + start - skip, -1.0e6)
    from_ref[...] = start - skip
    upto_ref[...] = start + total - skip
    left = jnp.max(start + total - skip - float(CAP), axis=0, keepdims=True)
    left = jnp.max(left, axis=1, keepdims=True)
    marks_ref[pl.ds(me, 1)] = jnp.broadcast_to(jnp.where(left > 0, 1.0, 0.0)[None], (1, 8, LANES))

    def tile_base(t):
        return jnp.minimum(lax.shift_right_logical(offs_ref[0, t], 7), limit)

    def draw(t):
        cols = pl.ds(pl.multiple_of(t * TILE, TILE), TILE)
        lines = pl.ds(pl.multiple_of(t * KN, KN), KN)
        base = tile_base(t)
        pos = pos_ref[lines, :].astype(BF16)
        place = rows_of((CAP, TILE)).astype(F32).astype(BF16)
        pick = jnp.zeros((CAP, TILE), BF16)
        one = jnp.ones((CAP, TILE), BF16)
        for k in range(KN):
            pick = jnp.where(pos[k : k + 1, :] == place, one, pick)
        relp = rel_ref[:, cols] + (offs_ref[0, t] - base * LANES)
        low = (relp & (LANES - 1)).astype(F32)
        high = lax.shift_right_logical(relp, 7).astype(F32)
        points = pts_ref[:, cols]
        p_hi = points.astype(BF16).astype(F32)
        small = jnp.concatenate([p_hi, points - p_hi, low, high], 0).astype(BF16)
        data = jnp.concatenate([cot_ref[:, cols], small], 0)
        return dot_nt(data, pick)

    def place_inputs(t, drawn):
        lines = pl.ds(pl.multiple_of(t * KN, KN), KN)
        base = tile_base(t)
        head = drawn[channels : channels + 16]
        wide_from = jnp.concatenate([from_ref[lines, :]] * (CAP // TILE), 1)
        wide_upto = jnp.concatenate([upto_ref[lines, :]] * (CAP // TILE), 1)
        index = cols_of((KN, CAP)).astype(F32)
        which = (index >= wide_from) & (index < wide_upto)
        lo = jnp.sum(jnp.where(which, drawn[channels + 16 : channels + 24], 0.0), 0, keepdims=True)
        hi = jnp.sum(jnp.where(which, drawn[channels + 24 : channels + 32], 0.0), 0, keepdims=True)
        lo = jnp.broadcast_to(lo, (8, CAP))
        hi = jnp.broadcast_to(hi, (8, CAP))
        cell = (base + hi.astype(I32)) * LANES + lo.astype(I32)
        row = rows_of((8, CAP))
        along = jnp.where(
            row == 0,
            lax.shift_right_logical(cell, int(math.log2(GX * ZS))),
            jnp.where(
                row == 1,
                lax.shift_right_logical(cell, int(math.log2(ZS))) & (GX - 1),
                (cell & (ZS - 1)) + slab * ZS,
            ),
        )
        centre = jnp.where(row < 3, (along.astype(F32) + 0.5) / GX, 0.0)
        x = jnp.concatenate([head, centre, head[:8], centre, jnp.zeros((8, CAP), F32)], 0).astype(BF16)
        return x, lo, hi

    def lane_onehot(lo):
        row = jnp.broadcast_to(lo[:1], (LANES, CAP)).astype(BF16)
        return jnp.where(
            rows_of((LANES, CAP)).astype(F32).astype(BF16) == row, jnp.ones((LANES, CAP), BF16), jnp.zeros((LANES, CAP), BF16)
        )

    def spread(hi, grad):
        full = jnp.concatenate([hi, hi], 0)
        pieces = []
        for j in range(SPAN):
            on = jnp.where(full == float(j), 1.0, 0.0).astype(BF16)
            pieces.append(grad * jnp.concatenate([on] * (channels // 16), 0))
        return jnp.concatenate(pieces, 0)

    def first(i, carry):
        ts = [i * group + u for u in range(group)]
        drawn = [draw(t) for t in ts]
        placed = [place_inputs(t, d) for t, d in zip(ts, drawn)]
        cots = [d[:channels].astype(BF16) for d in drawn]
        pres = [dot(w1_ref[:, :XR], x) for x, _, _ in placed]
        kerns = []
        for t, pre, cot, (x, lo, hi) in zip(ts, pres, cots, placed):
            hidden, slope = gelu_parts(pre)
            hidden = hidden.astype(BF16)
            kerns.append(dot(w2_ref[...], jnp.concatenate([hidden, x], 0)))
            hid_ref[t] = hidden
            slope_ref[t] = slope
            cots_ref[t] = cot
            x_ref[t] = x
            spot_ref[t] = jnp.where(rows_of((8, CAP)) < 4, lo, hi)
        parts = []
        for kern, cot, (x, lo, hi) in zip(kerns, cots, placed):
            grad = (kern * cot.astype(F32)).astype(BF16)
            parts.append(dot_nt(spread(hi, grad), lane_onehot(lo)))
        for t, part in zip(ts, parts):
            for j in range(SPAN):
                parts_ref[j * tiles + t] = part[j * channels : (j + 1) * channels]
        return carry

    steps = tiles // group

    def pass_half(i, h):
        return send(half_of(peers[i], h), half_of(peers[i], h), fsend, frecv, {"pb": sibling})

    def come(i, h):
        piece(i, peers[i], h, gsend, peers[i]).wait_recv()

    middle, late_step = steps // 2, steps * 7 // 8
    lax.fori_loop(0, 1, first, 0)
    for m in range(1, n_pb):
        to = lax.rem(me + m, n_pb)
        send(marks_ref.at[me], marks_ref.at[me], msend, mrecv, {"pb": to}).start()
    lax.fori_loop(1, middle, first, 0)
    if square:
        come(0, 1)
        piece(2, peers[0], 1, hsend, peers[1]).start()
        come(1, 0)
        piece(2, peers[1], 0, hsend, peers[0]).start()
        pass_half(0, 1).start()
        pass_half(1, 0).start()
    lax.fori_loop(middle, late_step, first, 0)
    if square:
        for i in range(2):
            come(i, i)
            pass_half(i, i).start()
    lax.fori_loop(late_step, steps, first, 0)

    if square:
        for h in range(2):
            come(2, h)
            pass_half(2, h).start()
    some = marks_ref.at[pl.ds(0, n_pb - 1)]
    send(some, some, msend, mrecv, {"pb": sibling}).wait_recv()
    markz_ref[pl.ds(slab, 1)] = jnp.sum(marks_ref[...], 0, keepdims=True)
    table_copy.wait()

    def pair_at(line, b):
        return jnp.clip(table_ref[line, b], 0, SPAN * tiles - 1)

    def run(i, acc):
        for u in range(group):
            at = i * group + u
            acc = acc * table_ref[1, at].astype(F32) + parts_ref[pair_at(0, at)]
            sums_ref[at] = acc
        return acc

    lax.fori_loop(0, SPAN * tiles // group, run, jnp.zeros((channels, LANES), F32))

    def block(b):
        return sums_ref[pair_at(2, b)] * table_ref[3, b].astype(F32)

    def near_copy(i):
        return send(near_ref.at[i], nearin_ref.at[i], nsend, nrecv.at[i], {"pb": sibling})

    for m in range(1, n_ga):
        to = lax.rem(slab + m, n_ga)
        send(markz_ref.at[slab], markz_ref.at[slab], zsend, zrecv, {"ga": to}).start()
    pair = math.gcd(blocks, 4)
    order = list(range(chips - 2, -1, -1)) + [chips - 1]
    for n, i in enumerate(order):
        owner = near_chips[i] * 2 + 1 - core

        def fill(b, carry, i=i, owner=owner):
            for u in range(pair):
                near_ref[i, b * pair + u] = block(owner * blocks + b * pair + u).astype(BF16)
            return carry

        lax.fori_loop(0, blocks // pair, fill, 0)
        if n > 0:
            near_copy(order[n - 1]).start()
    if not square:
        for i in range(chips - 1):
            d = lax.rem(chip + chips - 1 - i, chips) * 2 + core
            send(feats_of(d), feats_of(d), gsend, grecv.at[i, 0], {"pb": d}).wait_recv()
            send(feats_of(d), feats_of(d), fsend, frecv, {"pb": sibling}).start()

    all_twins = feats_ref.at[pl.ds(0, chips * blocks)]
    send(all_twins, all_twins, gsend, frecv, {"pb": sibling}).wait_recv()

    acc_ref[...] = jnp.zeros_like(acc_ref)

    def draw_feats(t):
        window = feats_ref[pl.ds(tile_base(t), SPAN)].reshape(SPAN * channels, LANES)
        return dot(window, lane_onehot(spot_ref[t]))

    def feats_grad(t, drawn):
        tall = jnp.broadcast_to(spot_ref[t][4:5], (channels, CAP))
        feats = drawn[:channels]
        for j in range(1, SPAN):
            feats = jnp.where(tall == float(j), drawn[j * channels : (j + 1) * channels], feats)
        return (feats * cots_ref[t].astype(F32)).astype(BF16)

    wide = math.gcd(tiles, 8)

    def second(i, carry):
        ts = [i * wide + u for u in range(wide)]
        drawn = [draw_feats(t) for t in ts]
        grads = [feats_grad(t, d) for t, d in zip(ts, drawn)]
        pres = [dot(w2t_ref[...], g) for g in grads]
        sums = []
        for t, g, p in zip(ts, grads, pres):
            both = jnp.concatenate([g, (p * slope_ref[t]).astype(BF16)], 0)
            sums.append(dot_nt(both, jnp.concatenate([hid_ref[t], x_ref[t]], 0)))
        acc_ref[...] += functools.reduce(lambda a, b: a + b, sums)
        return carry

    near_copy(order[-1]).start()
    ahead = tiles // wide // 2
    lax.fori_loop(0, ahead, second, 0)
    if square:
        early = [(2, 0, 0, half_ref.at[0], 0), (2, 1, 1, half_ref.at[1], 1)]
        early += [(0, 0, 0, farin_ref.at[0, pl.ds(0, half)], 2), (1, 1, 1, farin_ref.at[1, pl.ds(half, half)], 2)]
        late = [(0, 1, 0, farin_ref.at[0, pl.ds(half, half)], 2), (1, 0, 1, farin_ref.at[1, pl.ds(0, half)], 2)]

        def far_half(slot, h, to, dst, n):
            return send(far_ref.at[slot, pl.ds(h * half, half)], dst, hsend, hrecv.at[n], {"pb": peers[to]})

        early = [far_half(*e) for e in early]
        late = [far_half(*e) for e in late]
        slots = [early[:2], [], []]
    else:
        fars = [
            send(far_ref.at[i], farin_ref.at[i], rsend.at[i], rrecv.at[i], {"pb": to}) for i, to in enumerate(peers)
        ]
        slots = [(fars[i],) for i in order[:-1]]
    if square:
        order = [2, 0, 1, 3]
    for n, i in enumerate(order):
        owner = near_chips[i] * 2 + core
        near_copy(i).wait_recv()

        def join(b, carry, i=i, owner=owner):
            for u in range(pair):
                at = b * pair + u
                value = block(owner * blocks + at) + nearin_ref[i, at].astype(F32)
                if i < chips - 1:
                    far_ref[i, at] = value.astype(BF16)
                else:
                    own_ref[at] = value
            return carry

        lax.fori_loop(0, blocks // pair, join, 0)
        if n > 0:
            for copy in slots[n - 1]:
                copy.start()

    lax.fori_loop(ahead, tiles // wide, second, 0)

    k, l = rows_of((LANES, LANES)), cols_of((LANES, LANES))

    def gathered(shift):
        a = (l - shift >= 0) & (l - shift < 4) & ((k == hid + l - shift) | ((k == hid + 8 + l - shift) & (l - shift < 3)))
        b = (l - shift >= 4) & (l - shift < 7) & (k == hid + 16 + l - shift - 4)
        return jnp.where(a | b, 1.0, 0.0)

    top = jnp.where(cols_of((channels, LANES)) < 112, acc_ref[:channels], 0.0)
    tail = hid - channels
    top += exact(acc_ref[channels : 2 * channels], gathered(112))
    rest = exact(acc_ref[2 * channels : 2 * channels + tail], gathered(120))
    top = jnp.concatenate([top[:tail] + rest, top[tail:]], 0)
    slices = channels // chips
    ar_ref[...] = top.reshape(chips, slices, LANES)

    def counted(n, ssem, rsem):
        some = arin_ref.at[pl.ds(0, n)]
        return send(some, some, ssem, rsem, {"pb": sibling})

    for m in range(1, chips):
        to = lax.rem(chip + m, chips)
        send(ar_ref.at[to], arin_ref.at[me], asend, arecv, {"pb": to * 2 + 1}).start()

    @pl.when(core == 0)
    def _():
        send(ar_ref.at[chip], arin_ref.at[me], asend, arecv, {"pb": sibling}).start()

    some = markz_ref.at[pl.ds(0, n_ga - 1)]
    send(some, some, zsend, zrecv, {"pb": sibling}).wait_recv()
    more_ref[0] = jnp.max(jnp.sum(markz_ref[...], 0)).astype(I32)
    tell = pltpu.make_async_copy(more_ref, more_out, out_sem)
    tell.start()
    if square:
        for copy in early[2:]:
            copy.start()
        for i, copy in enumerate(early[:2]):
            copy.wait_recv()
            into = far_ref.at[1 - i, pl.ds(i * half, half)]
            into[...] = (into[...].astype(F32) + half_ref[i].astype(F32)).astype(BF16)

    @pl.when(core == 0)
    def _():
        counted(chips, asend, arecv).wait_send()

    @pl.when(core == 1)
    def _():
        arin_ref[pl.ds(me, 1)] = ar_ref[pl.ds(chip, 1)]
        counted(n_pb - 1, asend, arecv).wait_recv()
        gaall_ref[pl.ds(slab, 1)] = jnp.sum(arin_ref[...], 0, keepdims=True)
        for m in range(1, n_ga):
            to = lax.rem(slab + m, n_ga)
            send(gaall_ref.at[slab], gaall_ref.at[slab], bsend, brecv, {"ga": to}).start()

    if square:
        for copy in late:
            copy.start()

    @pl.when(core == 1)
    def _():
        counted(n_ga - 1, bsend, brecv).wait_recv()
        fin_ref[pl.ds(chip, 1)] = jnp.sum(gaall_ref[...], 0, keepdims=True)
        for m in range(1, n_pb):
            to = lax.rem(me + m, n_pb)
            send(fin_ref.at[chip], fin_ref.at[chip], csend, crecv, {"pb": to}).start()

    if square:
        come_in = farin_ref.at[pl.ds(0, 2)]
        send(come_in, come_in, hsend, hrecv.at[2], {"pb": sibling}).wait_recv()
    else:
        for copy in fars:
            copy.wait_recv()
    for b in range(blocks):
        value = own_ref[b]
        for i in range(2 if square else chips - 1):
            value += farin_ref[i, b].astype(F32)
        grid_ref[0, :, b * LANES : (b + 1) * LANES] = value

    @pl.when(core == 0)
    def _():
        counted(chips, csend, crecv).wait_recv()

    @pl.when(core == 1)
    def _():
        counted(chips - 1, csend, crecv).wait_recv()

    final = fin_ref[...].reshape(channels, LANES)
    final_ref[...] = final
    tell.wait()
    all_feats = feats_ref.at[pl.ds(0, (3 if square else chips) * blocks)]
    send(all_feats, all_feats, gsend, frecv, {"pb": sibling}).wait_send()
    passed = feats_ref.at[pl.ds(0, (chips - 1) * blocks)]
    send(passed, passed, fsend, frecv, {"pb": sibling}).wait_send()
    send(near_ref, nearin_ref, nsend, nrecv.at[0], {"pb": sibling}).wait_send()
    if square:
        send(all_twins, all_twins, hsend, frecv, {"pb": sibling}).wait_send()
    else:
        for copy in fars:
            copy.wait_send()

    @pl.when(core == 1)
    def _():
        counted(chips - 1, asend, arecv).wait_send()
        counted(n_ga - 1, bsend, brecv).wait_send()
        counted(n_pb - 1, csend, crecv).wait_send()

    marks_in = marks_ref.at[pl.ds(0, n_pb - 1)]
    send(marks_in, marks_in, msend, mrecv, {"pb": sibling}).wait_send()
    marks_in = markz_ref.at[pl.ds(0, n_ga - 1)]
    send(marks_in, marks_in, zsend, zrecv, {"pb": sibling}).wait_send()


def call(step, collective_id, query_points, cotangent, slab_ids, rel_cells, offsets, latent, w_in, b_in, w_out, b_out):
    n_pb, n_ga = lax.axis_size("pb"), lax.axis_size("ga")
    channels, owned = latent.shape[1], latent.shape[2]
    hid = w_in.shape[0]
    queries = query_points.shape[1]
    tiles = queries // TILE
    chips = n_pb // 2
    blocks = owned // LANES
    pairs = SPAN * tiles
    lanes = -(-pairs // LANES) * LANES
    hbm = pl.BlockSpec(memory_space=pltpu.HBM)
    vmem = pl.BlockSpec(memory_space=pltpu.VMEM)
    dma = pltpu.SemaphoreType.DMA
    slices = channels // chips
    ins = (offsets, offsets, w_in.T, b_in[None], w_out, b_out[None], slab_ids, query_points, rel_cells, cotangent)
    ins += () if step is None else (step,)
    outs = [
        ((1, channels, owned), F32),
        ((channels, LANES), F32),
        ((1,), I32),
    ]
    return pl.pallas_call(
        functools.partial(kernel, n_pb, n_ga, len(ins)),
        out_shape=[jax.ShapeDtypeStruct(*o) for o in outs],
        in_specs=[hbm] * (1 + len(ins)),
        out_specs=[vmem, vmem, hbm],
        scratch_shapes=[(pltpu.SMEM if i in (0, 10) else pltpu.VMEM)(a.shape, a.dtype) for i, a in enumerate(ins)]
        + [pltpu.SMEM(*outs[2])]
        + [
            pltpu.VMEM((8, queries), F32),
            pltpu.VMEM((tiles * KN, TILE), F32),
            pltpu.VMEM((tiles * KN, TILE), F32),
            pltpu.VMEM((tiles * KN, TILE), F32),
            pltpu.VMEM((LANES, LANES), F32),
            pltpu.VMEM((hid, LANES), BF16),
            pltpu.VMEM((channels, LANES), BF16),
            pltpu.VMEM((hid, channels), BF16),
            pltpu.VMEM((8, lanes), I32),
            pltpu.SMEM((8, lanes), I32),
            pltpu.VMEM((tiles, channels, CAP), BF16),
            pltpu.VMEM((tiles, hid, CAP), BF16),
            pltpu.VMEM((tiles, hid, CAP), F32),
            pltpu.VMEM((tiles, XR, CAP), BF16),
            pltpu.VMEM((tiles, 8, CAP), F32),
            pltpu.VMEM((pairs, channels, LANES), F32),
            pltpu.VMEM((pairs, channels, LANES), F32),
            pltpu.VMEM((n_pb * blocks, channels, LANES), BF16),
            pltpu.VMEM((chips, blocks, channels, LANES), BF16),
            pltpu.VMEM((chips, blocks, channels, LANES), BF16),
            pltpu.VMEM((chips - 1, blocks, channels, LANES), BF16),
            pltpu.VMEM((chips - 1, blocks, channels, LANES), BF16),
            pltpu.VMEM((2, max(blocks // 2, 1), channels, LANES), BF16),
            pltpu.VMEM((blocks, channels, LANES), F32),
            pltpu.VMEM((channels + hid, LANES), F32),
            pltpu.VMEM((chips, slices, LANES), F32),
            pltpu.VMEM((n_pb, slices, LANES), F32),
            pltpu.VMEM((n_ga, slices, LANES), F32),
            pltpu.VMEM((chips, slices, LANES), F32),
            pltpu.VMEM((n_pb, 8, LANES), F32),
            pltpu.VMEM((n_ga, 8, LANES), F32),
            dma((len(ins),)),
            dma,
            dma,
            dma,
            dma,
            dma((chips - 1, 2)),
            dma,
            dma,
            dma,
            dma((chips,)),
            dma((chips,)),
            dma((chips,)),
            dma,
            dma((3,)),
            dma,
            dma,
            dma,
            dma,
            dma,
            dma,
            dma,
            dma,
            dma,
            dma,
        ],
        compiler_params=pltpu.CompilerParams(
            vmem_limit_bytes=67043328 - 4 * channels * (owned + LANES) - 1024, collective_id=collective_id, has_side_effects=True
        ),
        name="whole",
    )(latent, *ins)


def settle(scale, grid_in, final_ref, grid_ref, *rest):
    smalls, ready = rest[:4], rest[4:8]
    grid_sem, small_sem = rest[8:]
    gwin_ref, gbin_ref, gwout_ref, gbout_ref = ready
    move = pltpu.make_async_copy(grid_in, grid_ref, grid_sem)
    move.start()
    channels, hid = gwout_ref.shape
    final = final_ref[...]
    k, l = rows_of((LANES, LANES)), cols_of((LANES, LANES))

    def chosen(shift):
        along = (l < 3) & (k == shift + l)
        cells = (l >= 3) & (l < 6) & (k == shift + 1 + l)
        return jnp.where(along | cells | ((l == 6) & (k == shift + 3)), scale, 0.0)

    gwout_ref[...] = final[:, :hid] * scale
    taken = jnp.concatenate([exact(final, chosen(112)), exact(final[: hid - channels], chosen(120))], 0)
    turned = exact_nt(jnp.where(rows_of((8, LANES)) == cols_of((8, LANES)), 1.0, 0.0), taken)
    gwin_ref[...] = turned[: gwin_ref.shape[0]]
    gbin_ref[...] = turned[6:7]
    gbout_ref[...] = exact_nt(jnp.where(cols_of((8, LANES)) == hid + 3, scale, 0.0), final)[0:1]
    stores = [pltpu.make_async_copy(src, dst, small_sem.at[i]) for i, (src, dst) in enumerate(zip(ready, smalls))]
    for copy in stores:
        copy.start()
    for copy in stores:
        copy.wait()
    move.wait()


def shards(*args):
    def again(state):
        step, _, sums = state
        grid, final, more = call(step, 1, *args)
        return step + 1, more, (sums[0] + grid, sums[1] + final)

    grid, final, more = call(None, 0, *args)
    first = (jnp.ones((1,), I32), more, (grid, final))
    grid, final = lax.while_loop(lambda state: state[1][0] > 0, again, first)[2]
    hid, channels = args[6].shape[0], args[8].shape[0]
    queries = args[0].shape[1] * lax.axis_size("pb")
    hbm = pl.BlockSpec(memory_space=pltpu.HBM)
    dma = pltpu.SemaphoreType.DMA
    shapes = [args[6].shape[::-1], (1, hid), (channels, hid), (1, channels)]
    grid, gwin, gbin, gwout, gbout = pl.pallas_call(
        functools.partial(settle, float(queries) ** (-0.5)),
        out_shape=[jax.ShapeDtypeStruct(v, F32) for v in [grid.shape] + shapes],
        in_specs=[hbm, pl.BlockSpec(memory_space=pltpu.VMEM)],
        out_specs=[hbm] * 5,
        scratch_shapes=[pltpu.VMEM(v, F32) for v in shapes] + [dma, dma((4,))],
        name="settle",
    )(grid, final)
    return grid, gwin.T, gbin[0], gwout, gbout[0]


def solution(mesh):
    return jax.shard_map(
        shards,
        mesh=mesh,
        in_specs=(
            P(None, "pb"),
            P(None, "pb"),
            P(None, "pb"),
            P(None, "pb"),
            P("ga", "pb"),
            P("ga", None, "pb"),
            P(),
            P(),
            P(),
            P(),
        ),
        out_specs=(P("ga", None, "pb"), P(), P(), P(), P()),
        check_vma=False,
    )
```
